32 devices in a mesh: cp: 32 (over z, y, x, core).
Axes of the slice: x: 2, y: 2, z: 4, core: 2. Of those that a mesh axis runs over, the one named last changes fastest.
Arguments:
- queries: bfloat16 [4096, 16, 192], P('cp')
- latent: bfloat16 [4096, 512], P('cp')
- key_rope: bfloat16 [4096, 64], P('cp')
- w_uk: bfloat16 [512, 16, 128], replicated
- w_uv: bfloat16 [512, 16, 128], replicated
- d_out: bfloat16 [4096, 16, 128], P('cp')
Outputs:
- output 1: bfloat16 [4096, 16, 128], P('cp')
- output 2: bfloat16 [4096, 16, 192], P('cp')
- output 3: bfloat16 [4096, 512], P('cp')
- output 4: bfloat16 [4096, 64], P('cp')
- output 5: float32 [512, 16, 128], replicated
- output 6: float32 [512, 16, 128], replicated
All inputs are finite; a program needn't handle non-finite values.
Results may differ from the reference program's by a relative error of at most 0.02.
Values are sent between devices in bfloat16 or wider.
A program may use at most 1 GiB of HBM per device.

```python
import math
import jax
import jax.numpy as jnp
from jax import lax

TOK_DEV = 128
N_DEV = 32
N_HEADS = 16
LATENT = 512
NOPE_DIM = 128
ROPE_DIM = 64
V_DIM = 128

SEQ_LEN = TOK_DEV * N_DEV
QK_DIM = NOPE_DIM + ROPE_DIM
SOFT_SCALE = 1.0 / math.sqrt(QK_DIM)
Q_SPREAD = math.sqrt(0.75 * math.log(SEQ_LEN))


def setup_inputs(seed: int = 0) -> dict:
    rng_keys = jax.random.split(jax.random.key(seed), 6)
    queries = jax.random.normal(rng_keys[0], (SEQ_LEN, N_HEADS, QK_DIM), jnp.float32) * Q_SPREAD
    latent = jax.random.normal(rng_keys[1], (SEQ_LEN, LATENT), jnp.float32)
    key_rope = jax.random.normal(rng_keys[2], (SEQ_LEN, ROPE_DIM), jnp.float32)
    w_uk = jax.random.normal(rng_keys[3], (LATENT, N_HEADS, NOPE_DIM), jnp.float32) * LATENT ** -0.5
    w_uv = jax.random.normal(rng_keys[4], (LATENT, N_HEADS, V_DIM), jnp.float32) * LATENT ** -0.5
    d_out = jax.random.normal(rng_keys[5], (SEQ_LEN, N_HEADS, V_DIM), jnp.float32)
    return {
        "queries": queries.astype(jnp.bfloat16),
        "latent": latent.astype(jnp.bfloat16),
        "key_rope": key_rope.astype(jnp.bfloat16),
        "w_uk": w_uk.astype(jnp.bfloat16),
        "w_uv": w_uv.astype(jnp.bfloat16),
        "d_out": d_out.astype(jnp.bfloat16),
    }


def decompress(latent, w_uk, w_uv):
    lat_f = latent.astype(jnp.float32)
    k_nope = jnp.einsum("tl,lhd->thd", lat_f, w_uk.astype(jnp.float32)).astype(jnp.bfloat16)
    values = jnp.einsum("tl,lhd->thd", lat_f, w_uv.astype(jnp.float32)).astype(jnp.bfloat16)
    return k_nope, values


def attend(queries, latent, key_rope, w_uk, w_uv):
    k_nope, values = decompress(latent, w_uk, w_uv)
    k_f = k_nope.astype(jnp.float32)
    v_f = values.astype(jnp.float32)
    r_f = key_rope.astype(jnp.float32)
    key_pos = jnp.arange(SEQ_LEN)

    def block_rows(blk_pair):
        q_blk, q_start = blk_pair
        q_f = q_blk.astype(jnp.float32)
        scores = (jnp.einsum("qhd,khd->hqk", q_f[:, :, :NOPE_DIM], k_f)
                  + jnp.einsum("qhd,kd->hqk", q_f[:, :, NOPE_DIM:], r_f)) * SOFT_SCALE
        q_pos = q_start + jnp.arange(TOK_DEV)
        visible = key_pos[None, :] <= q_pos[:, None]
        scores = jnp.where(visible[None], scores, -1e30)
        attn_prob = jax.nn.softmax(scores, axis=-1)
        return jnp.einsum("hqk,khd->qhd", attn_prob, v_f)

    q_blocks = queries.reshape(N_DEV, TOK_DEV, N_HEADS, QK_DIM)
    q_starts = jnp.arange(N_DEV) * TOK_DEV
    out_rows = lax.map(jax.checkpoint(block_rows), (q_blocks, q_starts))
    return out_rows.reshape(SEQ_LEN, N_HEADS, V_DIM).astype(jnp.bfloat16)


def reference(queries, latent, key_rope, w_uk, w_uv, d_out):
    attn_out, pull_back = jax.vjp(attend, queries, latent, key_rope, w_uk.astype(jnp.float32), w_uv.astype(jnp.float32))
    d_query, d_latent, d_key_rope, d_w_uk, d_w_uv = pull_back(d_out)
    return (attn_out, d_query.astype(jnp.bfloat16), d_latent.astype(jnp.bfloat16), d_key_rope.astype(jnp.bfloat16), d_w_uk, d_w_uv)
```

```python
import functools
import math

import jax
import jax.numpy as jnp
from jax import lax
from jax.experimental import pallas as pl
from jax.experimental.pallas import tpu as pltpu
from jax.sharding import PartitionSpec as P

MESH = pl.DeviceIdType.MESH
NX, NY = 2, 2
BLK = 128
SUP = 256
CH = 1024
MSG = 320
CMSG = 576
NEG = -1e30
NT = (((1,), (1,)), ((), ()))
NN = (((1,), (0,)), ((), ()))


def mm(a, b, dims=NN):
    return lax.dot_general(a, b, dims, preferred_element_type=jnp.float32)


def unpack_rope(x):
    return jnp.concatenate([x[:, :64], x[:, 64:]], axis=0)


def pack_rope(x):
    return jnp.concatenate([x[:64], x[64:]], axis=1)


def kernel(nz, qk_dim, qd_ref, cr_ref, w_ref, wt_ref, od_recv, dkv_recv, dw_all,
           qd_recv, c_all, kr, v, kt, vt, s_buf, p_buf, ds_buf, dkr, dv, qf, dof, dot_, ot, dqt,
           od_send, dkv_out, dkv_part, dwt, dw_out, dw_part,
           q_send, q_rec, od_ssem, od_rsem, dkv_ssem, dkv_rsem, pair_sem,
           cg_rz, cg_rp, cg_sz, cg_sx, cg_sp, wg_rz, wg_rp, wg_sz, wg_sx, wg_sp):
    n_chip = NX * NY * nz
    n_dev = 2 * n_chip
    n_sup = n_chip // 2
    me = lax.axis_index("cp")
    chip, par = me // 2, me % 2
    partner = 2 * chip + (1 - par)
    x, y, z = chip % NX, (chip // NX) % NY, chip // (NX * NY)
    scale = 1.0 / math.sqrt(qk_dim)
    c1 = scale * math.log2(math.e)

    def chip_at(zq, yq, xq):
        return (zq * NY + yq) * NX + xq

    def col_chip(col, zq):
        return chip_at(zq, 1 - y if col >= 2 else y, 1 - x if col % 2 else x)

    def remote(src, dst, ssem, rsem, dev):
        return pltpu.make_async_remote_copy(src_ref=src, dst_ref=dst, send_sem=ssem, recv_sem=rsem,
                                            device_id=(dev,), device_id_type=MESH)

    def start(src, dst, ssem, rsem, dev):
        @pl.when(dev == me)
        def _():
            pltpu.make_async_copy(src, dst, rsem).start()

        @pl.when(dev != me)
        def _():
            remote(src, dst, ssem, rsem, dev).start()

    def sent(src, dst, ssem, rsem, dev):
        @pl.when(dev != me)
        def _():
            remote(src, dst, ssem, rsem, dev).wait_send()

    def arrived(dst, rsem):
        pltpu.make_async_copy(dst, dst, rsem).wait()

    barrier = pltpu.get_barrier_semaphore()

    def sig(i, carry):
        pl.semaphore_signal(barrier, inc=1, device_id=(lax.rem(me + i, n_dev),), device_id_type=MESH)
        return carry

    lax.fori_loop(1, n_dev, sig, 0)
    pl.semaphore_wait(barrier, n_dev - 1)

    def gather(buf, rows, rz, rp, sz, sx, sp, background):
        half = rows // 2
        dev_z = lambda zq: 2 * chip_at(zq, y, x) + par
        dev_x = 2 * chip_at(z, y, 1 - x) + par
        dev_y = 2 * chip_at(z, 1 - y, x) + par

        def blk(col, zq):
            return buf.at[par, col_chip(col, zq)]

        def up(zq):
            return remote(blk(0, zq), blk(0, zq), sz.at[0, zq], rz.at[0, zq, 0], dev_z(jnp.minimum(z + 1, nz - 1)))

        def down(zq):
            return remote(blk(0, zq), blk(0, zq), sz.at[1, zq], rz.at[0, zq, 0], dev_z(jnp.maximum(z - 1, 0)))

        def to_x(zq):
            return remote(blk(0, zq), blk(0, zq), sx.at[0, zq], rz.at[1, zq, 0], dev_x)

        def to_y(zq):
            return remote(blk(0, zq), blk(0, zq), sx.at[1, zq], rz.at[2, zq, 0], dev_y)

        def half_y(zq):
            b = blk(1, zq).at[pl.ds(0, half)]
            return remote(b, b, sx.at[2, zq], rz.at[3, zq, 0], dev_y)

        def half_x(zq):
            b = blk(2, zq).at[pl.ds(half, half)]
            return remote(b, b, sx.at[3, zq], rz.at[3, zq, 1], dev_x)

        def pair(col, zq):
            return remote(blk(col, zq), blk(col, zq), sp.at[col, zq], rp.at[col, zq], partner)

        def own_col(zq):
            to_x(zq).start()
            to_y(zq).start()
            pair(0, zq).start()

        def xy_wait1(zq):
            remote(blk(1, zq), blk(1, zq), sx.at[0, zq], rz.at[1, zq, 0], dev_x).wait_recv()
            half_y(zq).start()
            pair(1, zq).start()
            remote(blk(2, zq), blk(2, zq), sx.at[1, zq], rz.at[2, zq, 0], dev_y).wait_recv()
            half_x(zq).start()
            pair(2, zq).start()

        def diag(zq):
            b0 = blk(3, zq).at[pl.ds(0, half)]
            b1 = blk(3, zq).at[pl.ds(half, half)]
            remote(b0, b0, sx.at[2, zq], rz.at[3, zq, 0], dev_y).wait_recv()
            remote(b1, b1, sx.at[3, zq], rz.at[3, zq, 1], dev_x).wait_recv()
            pair(3, zq).start()

        def dist(d, f):
            if d == 0:
                f(z)
                return

            @pl.when(z - d >= 0)
            def _():
                f(z - d)

            @pl.when(z + d < nz)
            def _():
                f(z + d)

        @pl.when(z + 1 < nz)
        def _():
            up(z).start()

        @pl.when(z > 0)
        def _():
            down(z).start()

        own_col(z)
        background(0)
        for d in range(1, nz):
            @pl.when(z - d >= 0)
            def _():
                remote(blk(0, z - d), blk(0, z - d), sz.at[0, z - d], rz.at[0, z - d, 0], partner).wait_recv()

                @pl.when(z + 1 < nz)
                def _():
                    up(z - d).start()

                own_col(z - d)

            @pl.when(z + d < nz)
            def _():
                remote(blk(0, z + d), blk(0, z + d), sz.at[1, z + d], rz.at[0, z + d, 0], partner).wait_recv()

                @pl.when(z > 0)
                def _():
                    down(z + d).start()

                own_col(z + d)

            dist(d - 1, xy_wait1)
            background(d)
            if d >= 2:
                dist(d - 2, diag)
        dist(nz - 1, xy_wait1)
        background(nz)
        for d in range(max(nz - 2, 0), nz):
            dist(d, diag)

        def finish():
            for zq in range(nz):
                for col in range(4):
                    pair(col, zq).wait()
                for c in (to_x, to_y, half_y, half_x):
                    c(zq).wait_send()

                @pl.when(jnp.logical_and(z >= zq, z + 1 < nz))
                def _():
                    up(zq).wait_send()

                @pl.when(jnp.logical_and(z <= zq, z > 0))
                def _():
                    down(zq).wait_send()

        return finish

    owner_core = lax.rem((chip + 1) // 2, 2)
    q_slot = 2 * (chip // 2) + par

    def q_copy(i):
        head = lax.rem(chip + i, n_chip)
        return qd_ref.at[head], qd_recv.at[q_slot], q_send.at[i], q_rec.at[q_slot], 2 * head + owner_core

    def run_parts(copy, parts):
        per = -(-n_chip // parts)

        def background(step):
            def go(i, carry):
                start(*copy(i))
                return carry

            lax.fori_loop(min(step * per, n_chip), min((step + 1) * per, n_chip), go, 0)

        return background

    c_all[par, chip] = cr_ref[...]
    finish_c = gather(c_all, CMSG, cg_rz, cg_rp, cg_sz, cg_sx, cg_sp, run_parts(q_copy, nz + 1))

    dkr[...] = jnp.zeros_like(dkr)
    dv[...] = jnp.zeros_like(dv)
    finish_c()

    def latent_of(ch):
        rows = []
        for q in range(2):
            rows.append(jnp.concatenate([c_all[q, ch, pl.ds(BLK * i, BLK), :] for i in range(4)], axis=1))
        return jnp.concatenate(rows, axis=0)

    def up_project(ch, carry):
        base = pl.multiple_of(ch * SUP, SUP)
        lat = latent_of(ch)
        kv = mm(lat, w_ref[...]).astype(jnp.bfloat16)
        kvt = mm(wt_ref[...], lat, NT).astype(jnp.bfloat16)
        kr[pl.ds(base, SUP), pl.ds(0, 128)] = kv[:, :128]
        v[pl.ds(base, SUP), :] = kv[:, 128:]
        kt[pl.ds(0, 128), pl.ds(base, SUP)] = kvt[:128]
        vt[:, pl.ds(base, SUP)] = kvt[128:]
        for q in range(2):
            rp = c_all[q, ch, pl.ds(4 * BLK, 64), :].astype(jnp.float32)
            r = unpack_rope(rp)
            kr[pl.ds(base + q * BLK, BLK), pl.ds(128, 128)] = jnp.concatenate(
                [r, jnp.zeros_like(r)], axis=1).astype(jnp.bfloat16)
            rt = jnp.transpose(r)
            kt[pl.ds(128, 64), pl.ds(base + q * BLK, BLK)] = rt.astype(jnp.bfloat16)
        return carry

    lax.fori_loop(0, n_chip, up_project, 0)

    k_iota = lax.broadcasted_iota(jnp.int32, (SUP, SUP), 0)
    q_iota = lax.broadcasted_iota(jnp.int32, (SUP, SUP), 1)
    diff = k_iota - q_iota

    def od_copy(s, i):
        ch = 2 * s + lax.rem(s + par, 2)
        return od_send.at[2 * s + i], od_recv.at[chip], od_ssem.at[2 * s + i], od_rsem.at[chip], 2 * ch + i

    def superblock(s, carry):
        ch = 2 * s + lax.rem(s + par, 2)
        for i in range(2):
            slot = 2 * s + i
            arrived(qd_recv.at[slot], q_rec.at[slot])
            rows = pl.ds(i * BLK, BLK)
            qf[rows, pl.ds(0, 128)] = qd_recv[slot, pl.ds(0, BLK), :]
            qr = unpack_rope(qd_recv[slot, pl.ds(2 * BLK, 64), :].astype(jnp.float32))
            qf[rows, pl.ds(128, 128)] = jnp.concatenate([qr, jnp.zeros_like(qr)], axis=1).astype(jnp.bfloat16)
            do = qd_recv[slot, pl.ds(BLK, BLK), :]
            dof[rows, :] = do
            dot_[:, rows] = jnp.transpose(do.astype(jnp.float32))
        n_ch = s // (CH // (2 * SUP)) + 1

        def score(j, m8):
            for t in range(CH // SUP):
                r0 = pl.multiple_of(j * CH + t * SUP, SUP)
                st = mm(kr[pl.ds(r0, SUP), :], qf[...], NT)
                st = jnp.where(diff <= ch * SUP - r0, st, NEG)
                s_buf[pl.ds(r0, SUP), :] = st
                m8 = jnp.maximum(m8, jnp.max(st.reshape(SUP // 8, 8, SUP), axis=0))
            return m8

        m8 = lax.fori_loop(0, n_ch, score, jnp.full((8, SUP), NEG, jnp.float32))
        m2 = jnp.max(m8, axis=0, keepdims=True) * c1
        ot[...] = jnp.zeros_like(ot)

        def forward(j, l8):
            base = pl.multiple_of(j * CH, CH)
            for t in range(CH // SUP):
                p = jnp.exp2(s_buf[pl.ds(base + t * SUP, SUP), :] * c1 - m2)
                l8 = l8 + jnp.sum(p.reshape(SUP // 8, 8, SUP), axis=0)
                p_buf[pl.ds(t * SUP, SUP), :] = p.astype(jnp.bfloat16)
            ot[...] += mm(vt[:, pl.ds(base, CH)], p_buf[...])
            return l8

        l8 = lax.fori_loop(0, n_ch, forward, jnp.zeros((8, SUP), jnp.float32))
        l = jnp.sum(l8, axis=0, keepdims=True)
        o = ot[...] / l
        lse2 = m2 + jnp.log2(l)
        delta = jnp.sum(o * dot_[...], axis=0, keepdims=True)
        o_rows = jnp.transpose(o)
        for i in range(2):
            od_send[2 * s + i, pl.ds(0, BLK), :] = o_rows[i * BLK:(i + 1) * BLK].astype(jnp.bfloat16)
        dqt[...] = jnp.zeros_like(dqt)

        def backward(j, carry):
            base = pl.multiple_of(j * CH, CH)
            for t in range(CH // SUP):
                rows = pl.ds(base + t * SUP, SUP)
                dp = mm(v[rows, :], dof[...], NT)
                p = jnp.exp2(s_buf[rows, :] * c1 - lse2)
                p_buf[pl.ds(t * SUP, SUP), :] = p.astype(jnp.bfloat16)
                ds_buf[pl.ds(t * SUP, SUP), :] = (p * (dp - delta) * scale).astype(jnp.bfloat16)
            for t in range(CH // SUP):
                rows = pl.ds(base + t * SUP, SUP)
                dkr[rows, :] += mm(ds_buf[pl.ds(t * SUP, SUP), :], qf[...])
                dv[rows, :] += mm(p_buf[pl.ds(t * SUP, SUP), :], dof[...])
            dqt[...] += mm(kt[:, pl.ds(base, CH)], ds_buf[...])
            return carry

        lax.fori_loop(0, n_ch, backward, 0)
        dq_n = jnp.transpose(dqt[pl.ds(0, 128), :])
        dq_r = jnp.transpose(dqt[pl.ds(128, 64), :])
        for i in range(2):
            od_send[2 * s + i, pl.ds(BLK, BLK), :] = dq_n[i * BLK:(i + 1) * BLK].astype(jnp.bfloat16)
            od_send[2 * s + i, pl.ds(2 * BLK, 64), :] = pack_rope(dq_r[i * BLK:(i + 1) * BLK]).astype(jnp.bfloat16)
        for i in range(2):
            start(*od_copy(s, i))
        return carry

    lax.fori_loop(0, n_sup, superblock, 0)

    dwt[...] = jnp.zeros_like(dwt)

    def finish_keys(ch, carry):
        base = pl.multiple_of(ch * SUP, SUP)
        for q in range(2):
            rows = pl.ds(base + q * BLK, BLK)
            dkv_out[q, ch, pl.ds(0, BLK), :] = dkr[rows, pl.ds(0, 128)].astype(jnp.bfloat16)
            dkv_out[q, ch, pl.ds(BLK, BLK), :] = dv[rows, :].astype(jnp.bfloat16)
            dkv_out[q, ch, pl.ds(2 * BLK, 64), :] = pack_rope(dkr[rows, pl.ds(128, 128)][:, :64]).astype(jnp.bfloat16)
        dk_t = jnp.transpose(dkr[pl.ds(base, SUP), pl.ds(0, 128)])
        dv_t = jnp.transpose(dv[pl.ds(base, SUP), :])
        dkv_t = jnp.concatenate([dk_t, dv_t], axis=0).astype(jnp.bfloat16)
        dwt[...] += mm(dkv_t, latent_of(ch))
        return carry

    lax.fori_loop(0, n_chip, finish_keys, 0)
    pair_dkv = remote(dkv_out.at[1 - par], dkv_part, pair_sem.at[0], pair_sem.at[1], partner)
    pair_dkv.start()
    for q in range(2):
        dw_out[q] = jnp.transpose(dwt[pl.ds(q * 128, 128), :])
    pair_dw = remote(dw_out.at[1 - par], dw_part, pair_sem.at[2], pair_sem.at[3], partner)
    pair_dw.start()
    pair_dkv.wait()

    def add_pair(ch, carry):
        dkv_out[par, ch] = (dkv_out[par, ch].astype(jnp.float32) + dkv_part[ch].astype(jnp.float32)).astype(jnp.bfloat16)
        return carry

    lax.fori_loop(0, n_chip, add_pair, 0)
    pair_dw.wait()
    dw_all[par, chip] = dw_out[par] + dw_part[...]

    def dkv_copy(i):
        ch = lax.rem(chip + i, n_chip)
        return dkv_out.at[par, ch], dkv_recv.at[chip], dkv_ssem.at[i], dkv_rsem.at[chip], 2 * ch + par

    finish_w = gather(dw_all, 512, wg_rz, wg_rp, wg_sz, wg_sx, wg_sp, run_parts(dkv_copy, nz + 1))
    finish_w()

    def drain(i, carry):
        sent(*q_copy(i))
        sent(*dkv_copy(i))
        sent(*od_copy(i // 2, i % 2))
        arrived(od_recv.at[i], od_rsem.at[i])
        arrived(dkv_recv.at[i], dkv_rsem.at[i])
        return carry

    lax.fori_loop(0, n_chip, drain, 0)


def solution(mesh):
    n_dev = mesh.shape["cp"]
    n_chip = n_dev // 2
    nz = n_chip // (NX * NY)
    seq = n_dev * BLK
    seq_spec = P("cp")

    def local_step(queries, latent, key_rope, w_uk, w_uv, d_out):
        head = lax.axis_index("cp") // 2
        q_n = queries[:, :, :128].transpose(1, 0, 2)
        q_r = queries[:, :, 128:].transpose(1, 0, 2)
        q_r = jnp.concatenate([q_r[:, :64], q_r[:, 64:]], axis=2)
        qd = jnp.concatenate([q_n, d_out.transpose(1, 0, 2), q_r], axis=1)
        r2 = jnp.concatenate([key_rope[:64], key_rope[64:]], axis=1)
        cr = jnp.concatenate([latent[:, 128 * i:128 * (i + 1)] for i in range(4)] + [r2], axis=0)
        wk = lax.dynamic_index_in_dim(w_uk, head, 1, keepdims=False)
        wv = lax.dynamic_index_in_dim(w_uv, head, 1, keepdims=False)
        w = jnp.concatenate([wk, wv], axis=1)
        bf, f32 = jnp.bfloat16, jnp.float32
        vm = pl.BlockSpec(memory_space=pltpu.VMEM)
        dma = pltpu.SemaphoreType.DMA
        gather_sems = [dma((4, nz, 2)), dma((4, nz)), dma((2, nz)), dma((4, nz)), dma((4, nz))]
        od, dkv, dw = pl.pallas_call(
            functools.partial(kernel, nz, queries.shape[-1]),
            out_shape=(jax.ShapeDtypeStruct((n_chip, MSG, 128), bf),
                       jax.ShapeDtypeStruct((n_chip, MSG, 128), bf),
                       jax.ShapeDtypeStruct((2, n_chip, 512, 128), f32)),
            in_specs=[vm] * 4,
            out_specs=(vm, vm, vm),
            scratch_shapes=[
                pltpu.VMEM((n_chip, MSG, 128), bf),
                pltpu.VMEM((2, n_chip, CMSG, 128), bf),
                pltpu.VMEM((seq, 256), bf),
                pltpu.VMEM((seq, 128), bf),
                pltpu.VMEM((192, seq), bf),
                pltpu.VMEM((128, seq), bf),
                pltpu.VMEM((seq, SUP), f32),
                pltpu.VMEM((CH, SUP), bf),
                pltpu.VMEM((CH, SUP), bf),
                pltpu.VMEM((seq, 256), f32),
                pltpu.VMEM((seq, 128), f32),
                pltpu.VMEM((SUP, 256), bf),
                pltpu.VMEM((SUP, 128), bf),
                pltpu.VMEM((128, SUP), f32),
                pltpu.VMEM((128, SUP), f32),
                pltpu.VMEM((192, SUP), f32),
                pltpu.VMEM((n_chip, MSG, 128), bf),
                pltpu.VMEM((2, n_chip, MSG, 128), bf),
                pltpu.VMEM((n_chip, MSG, 128), bf),
                pltpu.VMEM((256, 512), f32),
                pltpu.VMEM((2, 512, 128), f32),
                pltpu.VMEM((512, 128), f32),
                dma((n_chip,)), dma((n_chip,)), dma((n_chip,)), dma((n_chip,)), dma((n_chip,)), dma((n_chip,)),
                dma((4,)),
            ] + gather_sems + gather_sems,
            compiler_params=pltpu.CompilerParams(
                collective_id=0, has_side_effects=True, vmem_limit_bytes=60 * 1024 * 1024),
        )(qd, cr, w, w.T)
        attn_out = od[:, :BLK].transpose(1, 0, 2)
        dq_r = od[:, 2 * BLK:]
        dq_r = jnp.concatenate([dq_r[:, :, :64], dq_r[:, :, 64:]], axis=1)
        d_query = jnp.concatenate([od[:, BLK:2 * BLK], dq_r], axis=2).transpose(1, 0, 2)
        d_latent = (jnp.einsum("htd,lhd->tl", dkv[:, :BLK], w_uk, preferred_element_type=f32)
                    + jnp.einsum("htd,lhd->tl", dkv[:, BLK:2 * BLK], w_uv, preferred_element_type=f32)).astype(bf)
        dr = jnp.sum(dkv[:, 2 * BLK:].astype(f32), axis=0)
        d_key_rope = jnp.concatenate([dr[:, :64], dr[:, 64:]], axis=0).astype(bf)
        return (attn_out, d_query, d_latent, d_key_rope,
                dw[0].transpose(1, 0, 2), dw[1].transpose(1, 0, 2))

    return jax.shard_map(local_step, mesh=mesh,
                         in_specs=(seq_spec, seq_spec, seq_spec, P(), P(), seq_spec),
                         out_specs=(seq_spec, seq_spec, seq_spec, seq_spec, P(), P()),
                         check_vma=False)
```

```python
import functools
import math

import jax
import jax.numpy as jnp
from jax import lax
from jax.experimental import pallas as pl
from jax.experimental.pallas import tpu as pltpu
from jax.sharding import PartitionSpec as P

MESH = pl.DeviceIdType.MESH
NX, NY = 2, 2
BLK = 128
SUP = 256
CH = 1024
MSG = 320
CMSG = 576
NEG = -1e30
NT = (((1,), (1,)), ((), ()))
NN = (((1,), (0,)), ((), ()))


def mm(a, b, dims=NN):
    return lax.dot_general(a, b, dims, preferred_element_type=jnp.float32)


def unpack_rope(x):
    return jnp.concatenate([x[:, :64], x[:, 64:]], axis=0)


def pack_rope(x):
    return jnp.concatenate([x[:64], x[64:]], axis=1)


def kernel(nz, qk_dim, qd_ref, cr_ref, wk_ref, wv_ref, o_out, dq_out, dkv_recv, dwk_out, dwv_out,
           od_recv, dw_all, w_cat, wt_cat, qd_recv, c_all, kr, v, kt, vt, s_buf, p_buf, ds_buf, dkr, dv, qt, dof, dot_, ot, dqt,
           od_send, dkv_out, dkv_part, dwt, dw_out, dw_part,
           q_send, q_rec, od_ssem, od_rsem, dkv_ssem, dkv_rsem, pair_sem, dw_sem,
           cg_rz, cg_rp, cg_sz, cg_sx, cg_sp, wg_rz, wg_rp, wg_sz, wg_sx, wg_sp):
    n_chip = NX * NY * nz
    n_dev = 2 * n_chip
    n_sup = n_chip // 2
    me = lax.axis_index("cp")
    chip, par = me // 2, me % 2
    partner = 2 * chip + (1 - par)
    x, y, z = chip % NX, (chip // NX) % NY, chip // (NX * NY)
    scale = 1.0 / math.sqrt(qk_dim)
    c1 = scale * math.log2(math.e)

    def chip_at(zq, yq, xq):
        return (zq * NY + yq) * NX + xq

    def col_chip(col, zq):
        return chip_at(zq, 1 - y if col >= 2 else y, 1 - x if col % 2 else x)

    def remote(src, dst, ssem, rsem, dev):
        return pltpu.make_async_remote_copy(src_ref=src, dst_ref=dst, send_sem=ssem, recv_sem=rsem,
                                            device_id=(dev,), device_id_type=MESH)

    def start(src, dst, ssem, rsem, dev):
        @pl.when(dev == me)
        def _():
            pltpu.make_async_copy(src, dst, rsem).start()

        @pl.when(dev != me)
        def _():
            remote(src, dst, ssem, rsem, dev).start()

    def sent(src, dst, ssem, rsem, dev):
        @pl.when(dev != me)
        def _():
            remote(src, dst, ssem, rsem, dev).wait_send()

    def arrived(dst, rsem):
        pltpu.make_async_copy(dst, dst, rsem).wait()

    barrier = pltpu.get_barrier_semaphore()

    def sig(i, carry):
        pl.semaphore_signal(barrier, inc=1, device_id=(lax.rem(me + i, n_dev),), device_id_type=MESH)
        return carry

    lax.fori_loop(1, n_dev, sig, 0)
    pl.semaphore_wait(barrier, n_dev - 1)

    def gather(buf, rows, chain, rz, rp, sz, sx, sp, background, ready):
        half = rows // 2
        dev_z = lambda zq: 2 * chip_at(zq, y, x) + par
        dev_x = 2 * chip_at(z, y, 1 - x) + par
        dev_y = 2 * chip_at(z, 1 - y, x) + par

        def blk(col, zq):
            return buf.at[par, col_chip(col, zq)]

        def along_z(zq, to, k):
            return remote(blk(0, zq), blk(0, zq), sz.at[k, zq], rz.at[0, zq, 0], dev_z(to))

        def to_x(col, zq):
            return remote(blk(col, zq), blk(col, zq), sx.at[0, zq], rz.at[1, zq, 0], dev_x)

        def to_y(col, zq):
            return remote(blk(col, zq), blk(col, zq), sx.at[1, zq], rz.at[2, zq, 0], dev_y)

        def half_y(col, zq):
            b = blk(col, zq).at[pl.ds(0, half)]
            return remote(b, b, sx.at[2, zq], rz.at[3, zq, 0], dev_y)

        def half_x(col, zq):
            b = blk(col, zq).at[pl.ds(half, half)]
            return remote(b, b, sx.at[3, zq], rz.at[3, zq, 1], dev_x)

        def pair(col, zq):
            return remote(blk(col, zq), blk(col, zq), sp.at[col, zq], rp.at[col, zq], partner)

        def own_col(zq):
            to_x(0, zq).start()
            to_y(0, zq).start()
            pair(0, zq).start()

        def xy(zq):
            to_x(1, zq).wait_recv()
            half_y(1, zq).start()
            pair(1, zq).start()
            to_y(2, zq).wait_recv()
            half_x(2, zq).start()
            pair(2, zq).start()

        def diag(zq):
            half_y(3, zq).wait_recv()
            half_x(3, zq).wait_recv()
            pair(3, zq).start()
            for col in range(4):
                pair(col, zq).wait_recv()
            ready(zq)

        def dist(d, f):
            if d == 0:
                f(z)
                return

            @pl.when(z - d >= 0)
            def _():
                f(z - d)

            @pl.when(z + d < nz)
            def _():
                f(z + d)

        def z_sends(go):
            if chain:
                for zq in range(nz):
                    @pl.when(jnp.logical_and(z >= zq, z + 1 < nz))
                    def _():
                        go(along_z(zq, z + 1, 0))

                    @pl.when(jnp.logical_and(z <= zq, z > 0))
                    def _():
                        go(along_z(zq, z - 1, 1))
            else:
                for d in range(1, nz):
                    @pl.when(z + d < nz)
                    def _():
                        go(along_z(z, z + d, d - 1))

                    @pl.when(z - d >= 0)
                    def _():
                        go(along_z(z, z - d, nz - 2 + d))

        if chain:
            @pl.when(z + 1 < nz)
            def _():
                along_z(z, z + 1, 0).start()

            @pl.when(z > 0)
            def _():
                along_z(z, z - 1, 1).start()
        else:
            z_sends(lambda c: c.start())

        own_col(z)
        background(0)
        for d in range(1, nz):
            @pl.when(z - d >= 0)
            def _():
                along_z(z - d, z, 0).wait_recv()
                if chain:
                    @pl.when(z + 1 < nz)
                    def _():
                        along_z(z - d, z + 1, 0).start()

                own_col(z - d)

            @pl.when(z + d < nz)
            def _():
                along_z(z + d, z, 1).wait_recv()
                if chain:
                    @pl.when(z > 0)
                    def _():
                        along_z(z + d, z - 1, 1).start()

                own_col(z + d)

            dist(d - 1, xy)
            background(d)
            if d >= 2:
                dist(d - 2, diag)
        dist(nz - 1, xy)
        background(nz)
        for d in range(max(nz - 2, 0), nz):
            dist(d, diag)

        def finish():
            z_sends(lambda c: c.wait_send())
            for zq in range(nz):
                for col in range(4):
                    pair(col, zq).wait_send()
                to_x(0, zq).wait_send()
                to_y(0, zq).wait_send()
                half_y(1, zq).wait_send()
                half_x(2, zq).wait_send()

        return finish

    owner_core = lax.rem((chip + 1) // 2, 2)
    q_slot = 2 * (chip // 2) + par

    def q_copy(i):
        head = lax.rem(chip + i, n_chip)
        return qd_ref.at[head], qd_recv.at[q_slot], q_send.at[i], q_rec.at[q_slot], 2 * head + owner_core

    def latent_of(ch):
        rows = []
        for q in range(2):
            rows.append(jnp.concatenate([c_all[q, ch, pl.ds(BLK * i, BLK), :] for i in range(4)], axis=1))
        return jnp.concatenate(rows, axis=0)

    def up_project(ch, carry):
        base = pl.multiple_of(ch * SUP, SUP)
        lat = latent_of(ch)
        kv = mm(lat, w_cat[...]).astype(jnp.bfloat16)
        kvt = mm(wt_cat[...], lat, NT).astype(jnp.bfloat16)
        kr[pl.ds(base, SUP), pl.ds(0, 128)] = kv[:, :128]
        v[pl.ds(base, SUP), :] = kv[:, 128:]
        kt[pl.ds(0, 128), pl.ds(base, SUP)] = kvt[:128]
        vt[:, pl.ds(base, SUP)] = kvt[128:]
        for q in range(2):
            rt = c_all[q, ch, pl.ds(4 * BLK, 64), :]
            kt[pl.ds(128, 64), pl.ds(base + q * BLK, BLK)] = rt
            r = jnp.transpose(rt.astype(jnp.float32))
            kr[pl.ds(base + q * BLK, BLK), pl.ds(128, 128)] = jnp.concatenate(
                [r, jnp.zeros_like(r)], axis=1).astype(jnp.bfloat16)
        return carry

    def up_column(zq):
        lax.fori_loop(0, 4, lambda i, carry: up_project(zq * 4 + i, carry), 0)

    def send_q(step):
        if step == 0:
            def go(i, carry):
                start(*q_copy(i))
                return carry

            lax.fori_loop(0, n_chip, go, 0)
            dkr[...] = jnp.zeros_like(dkr)
            dv[...] = jnp.zeros_like(dv)
            w_cat[...] = jnp.concatenate([wk_ref[...], wv_ref[...]], axis=1)
            for i, w in enumerate((wk_ref, wv_ref)):
                wt_cat[pl.ds(i * 128, 128), :] = jnp.transpose(w[...].astype(jnp.float32)).astype(jnp.bfloat16)
            qt[pl.ds(192, 64), :] = jnp.zeros((64, SUP), jnp.bfloat16)

    c_all[par, chip] = cr_ref[...]
    finish_c = gather(c_all, CMSG, False, cg_rz, cg_rp, cg_sz, cg_sx, cg_sp, send_q, up_column)


    k_iota = lax.broadcasted_iota(jnp.int32, (SUP, SUP), 0)
    q_iota = lax.broadcasted_iota(jnp.int32, (SUP, SUP), 1)
    diff = k_iota - q_iota

    def od_copy(s, i):
        ch = 2 * s + lax.rem(s + par, 2)
        return od_send.at[2 * s + i], od_recv.at[chip], od_ssem.at[2 * s + i], od_rsem.at[chip], 2 * ch + i

    def superblock(s, carry):
        ch = 2 * s + lax.rem(s + par, 2)
        for i in range(2):
            slot = 2 * s + i
            arrived(qd_recv.at[slot], q_rec.at[slot])
            rows = pl.ds(i * BLK, BLK)
            qt[pl.ds(0, 192), rows] = qd_recv[slot, pl.ds(0, 192), :]
            do = qd_recv[slot, pl.ds(192, BLK), :]
            dof[rows, :] = do
            dot_[:, rows] = jnp.transpose(do.astype(jnp.float32))
        n_ch = s // (CH // (2 * SUP)) + 1

        def score(j, m8):
            for t in range(CH // SUP):
                r0 = pl.multiple_of(j * CH + t * SUP, SUP)
                st = mm(kr[pl.ds(r0, SUP), :], qt[...])
                st = jnp.where(diff <= ch * SUP - r0, st, NEG)
                s_buf[pl.ds(r0, SUP), :] = st
                m8 = jnp.maximum(m8, jnp.max(st.reshape(SUP // 8, 8, SUP), axis=0))
            return m8

        m8 = lax.fori_loop(0, n_ch, score, jnp.full((8, SUP), NEG, jnp.float32))
        m2 = jnp.max(m8, axis=0, keepdims=True) * c1
        ot[...] = jnp.zeros_like(ot)

        def forward(j, l8):
            base = pl.multiple_of(j * CH, CH)
            for t in range(CH // SUP):
                p = jnp.exp2(s_buf[pl.ds(base + t * SUP, SUP), :] * c1 - m2)
                l8 = l8 + jnp.sum(p.reshape(SUP // 8, 8, SUP), axis=0)
                p_buf[pl.ds(t * SUP, SUP), :] = p.astype(jnp.bfloat16)
            ot[...] += mm(vt[:, pl.ds(base, CH)], p_buf[...])
            return l8

        l8 = lax.fori_loop(0, n_ch, forward, jnp.zeros((8, SUP), jnp.float32))
        l = jnp.sum(l8, axis=0, keepdims=True)
        o = ot[...] / l
        lse2 = m2 + jnp.log2(l)
        delta = jnp.sum(o * dot_[...], axis=0, keepdims=True)
        o_rows = jnp.transpose(o)
        for i in range(2):
            od_send[2 * s + i, pl.ds(0, BLK), :] = o_rows[i * BLK:(i + 1) * BLK].astype(jnp.bfloat16)
        dqt[...] = jnp.zeros_like(dqt)

        def backward(j, carry):
            base = pl.multiple_of(j * CH, CH)
            for t in range(CH // SUP):
                rows = pl.ds(base + t * SUP, SUP)
                dp = mm(v[rows, :], dof[...], NT)
                p = jnp.exp2(s_buf[rows, :] * c1 - lse2)
                p_buf[pl.ds(t * SUP, SUP), :] = p.astype(jnp.bfloat16)
                ds_buf[pl.ds(t * SUP, SUP), :] = (p * (dp - delta) * scale).astype(jnp.bfloat16)
            for t in range(CH // SUP):
                rows = pl.ds(base + t * SUP, SUP)
                dkr[rows, :] += mm(ds_buf[pl.ds(t * SUP, SUP), :], qt[...], NT)
                dv[rows, :] += mm(p_buf[pl.ds(t * SUP, SUP), :], dof[...])
            dqt[...] += mm(kt[:, pl.ds(base, CH)], ds_buf[...])
            return carry

        lax.fori_loop(0, n_ch, backward, 0)
        for i in range(2):
            od_send[2 * s + i, pl.ds(BLK, 192), :] = dqt[:, pl.ds(i * BLK, BLK)].astype(jnp.bfloat16)
        for i in range(2):
            start(*od_copy(s, i))
        return carry

    lax.fori_loop(0, n_sup, superblock, 0)

    dwt[...] = jnp.zeros_like(dwt)

    def finish_keys(ch, carry):
        base = pl.multiple_of(ch * SUP, SUP)
        for q in range(2):
            rows = pl.ds(base + q * BLK, BLK)
            dkv_out[q, ch, pl.ds(0, BLK), :] = dkr[rows, pl.ds(0, 128)].astype(jnp.bfloat16)
            dkv_out[q, ch, pl.ds(BLK, BLK), :] = dv[rows, :].astype(jnp.bfloat16)
            dkv_out[q, ch, pl.ds(2 * BLK, 64), :] = pack_rope(dkr[rows, pl.ds(128, 128)][:, :64]).astype(jnp.bfloat16)
        dk_t = jnp.transpose(dkr[pl.ds(base, SUP), pl.ds(0, 128)])
        dv_t = jnp.transpose(dv[pl.ds(base, SUP), :])
        dkv_t = jnp.concatenate([dk_t, dv_t], axis=0).astype(jnp.bfloat16)
        dwt[...] += mm(dkv_t, latent_of(ch))
        return carry

    lax.fori_loop(0, n_chip, finish_keys, 0)
    pair_dkv = remote(dkv_out.at[1 - par], dkv_part, pair_sem.at[0], pair_sem.at[1], partner)
    pair_dkv.start()
    for q in range(2):
        dw_out[q] = jnp.transpose(dwt[pl.ds(q * 128, 128), :])
    pair_dw = remote(dw_out.at[1 - par], dw_part, pair_sem.at[2], pair_sem.at[3], partner)
    pair_dw.start()
    pair_dkv.wait()

    def add_pair(ch, carry):
        dkv_out[par, ch] = (dkv_out[par, ch].astype(jnp.float32) + dkv_part[ch].astype(jnp.float32)).astype(jnp.bfloat16)
        return carry

    lax.fori_loop(0, n_chip, add_pair, 0)
    pair_dw.wait()
    dw_all[par, chip] = dw_out[par] + dw_part[...]

    def dkv_copy(i):
        ch = lax.rem(chip + i, n_chip)
        return dkv_out.at[par, ch], dkv_recv.at[chip], dkv_ssem.at[i], dkv_rsem.at[chip], 2 * ch + par

    def deliver(h, carry):
        arrived(od_recv.at[h], od_rsem.at[h])
        o_out[h] = od_recv[h, pl.ds(0, BLK), :]
        dq_out[h] = od_recv[h, pl.ds(BLK, 192), :]
        return carry

    def send_dkv(step):
        per = -(-n_chip // nz)
        if step < nz:
            def go(i, carry):
                start(*dkv_copy(i))
                return carry

            lax.fori_loop(step * per, min((step + 1) * per, n_chip), go, 0)
        else:
            lax.fori_loop(0, n_chip, deliver, 0)

    def dw_copy(q, h):
        dst = dwk_out if q == 0 else dwv_out
        return pltpu.make_async_copy(dw_all.at[q, h], dst.at[:, h, 0], dw_sem.at[q, h])

    def put_dw(zq):
        for q in range(2):
            def go(i, carry):
                dw_copy(q, zq * 4 + i).start()
                return carry

            lax.fori_loop(0, 4, go, 0)

    finish_w = gather(dw_all, 512, True, wg_rz, wg_rp, wg_sz, wg_sx, wg_sp, send_dkv, put_dw)

    finish_c()
    finish_w()

    def drain(i, carry):
        sent(*q_copy(i))
        sent(*dkv_copy(i))
        sent(*od_copy(i // 2, i % 2))
        arrived(dkv_recv.at[i], dkv_rsem.at[i])
        for q in range(2):
            dw_copy(q, i).wait()
        return carry

    lax.fori_loop(0, n_chip, drain, 0)


def solution(mesh):
    n_dev = mesh.shape["cp"]
    n_chip = n_dev // 2
    nz = n_chip // (NX * NY)
    seq = n_dev * BLK
    seq_spec = P("cp")

    def local_step(queries, latent, key_rope, w_uk, w_uv, d_out):
        head = lax.axis_index("cp") // 2
        qd = jnp.concatenate([queries.transpose(1, 2, 0), d_out.transpose(1, 0, 2)], axis=1)
        cr = jnp.concatenate([latent[:, 128 * i:128 * (i + 1)] for i in range(4)] + [key_rope.T], axis=0)
        wk = lax.dynamic_index_in_dim(w_uk, head, 1, keepdims=False)
        wv = lax.dynamic_index_in_dim(w_uv, head, 1, keepdims=False)
        bf, f32 = jnp.bfloat16, jnp.float32
        vm = pl.BlockSpec(memory_space=pltpu.VMEM)
        dma = pltpu.SemaphoreType.DMA
        gather_sems = [dma((4, nz, 2)), dma((4, nz)), dma((max(2 * nz - 2, 2), nz)), dma((4, nz)), dma((4, nz))]
        o, dq, dkv, dwk, dwv = pl.pallas_call(
            functools.partial(kernel, nz, queries.shape[-1]),
            out_shape=(jax.ShapeDtypeStruct((n_chip, BLK, 128), bf),
                       jax.ShapeDtypeStruct((n_chip, 192, BLK), bf),
                       jax.ShapeDtypeStruct((n_chip, MSG, 128), bf),
                       jax.ShapeDtypeStruct((512, n_chip, 1, 128), f32),
                       jax.ShapeDtypeStruct((512, n_chip, 1, 128), f32)),
            in_specs=[vm] * 4,
            out_specs=(vm, vm, vm, pl.BlockSpec(memory_space=pl.ANY), pl.BlockSpec(memory_space=pl.ANY)),
            scratch_shapes=[
                pltpu.VMEM((n_chip, MSG, 128), bf),
                pltpu.VMEM((2, n_chip, 512, 128), f32),
                pltpu.VMEM((512, 256), bf),
                pltpu.VMEM((256, 512), bf),
                pltpu.VMEM((n_chip, MSG, 128), bf),
                pltpu.VMEM((2, n_chip, CMSG, 128), bf),
                pltpu.VMEM((seq, 256), bf),
                pltpu.VMEM((seq, 128), bf),
                pltpu.VMEM((192, seq), bf),
                pltpu.VMEM((128, seq), bf),
                pltpu.VMEM((seq, SUP), f32),
                pltpu.VMEM((CH, SUP), bf),
                pltpu.VMEM((CH, SUP), bf),
                pltpu.VMEM((seq, 256), f32),
                pltpu.VMEM((seq, 128), f32),
                pltpu.VMEM((256, SUP), bf),
                pltpu.VMEM((SUP, 128), bf),
                pltpu.VMEM((128, SUP), f32),
                pltpu.VMEM((128, SUP), f32),
                pltpu.VMEM((192, SUP), f32),
                pltpu.VMEM((n_chip, MSG, 128), bf),
                pltpu.VMEM((2, n_chip, MSG, 128), bf),
                pltpu.VMEM((n_chip, MSG, 128), bf),
                pltpu.VMEM((256, 512), f32),
                pltpu.VMEM((2, 512, 128), f32),
                pltpu.VMEM((512, 128), f32),
                dma((n_chip,)), dma((n_chip,)), dma((n_chip,)), dma((n_chip,)), dma((n_chip,)), dma((n_chip,)),
                dma((4,)), dma((2, n_chip)),
            ] + gather_sems + gather_sems,
            compiler_params=pltpu.CompilerParams(
                collective_id=0, has_side_effects=True, vmem_limit_bytes=60 * 1024 * 1024),
        )(qd, cr, wk, wv)
        attn_out = o.transpose(1, 0, 2)
        d_query = dq.transpose(2, 0, 1)
        d_latent = (jnp.einsum("htd,lhd->tl", dkv[:, :BLK], w_uk, preferred_element_type=f32)
                    + jnp.einsum("htd,lhd->tl", dkv[:, BLK:2 * BLK], w_uv, preferred_element_type=f32)).astype(bf)
        dr = jnp.sum(dkv[:, 2 * BLK:].astype(f32), axis=0)
        d_key_rope = jnp.concatenate([dr[:, :64], dr[:, 64:]], axis=0).astype(bf)
        return (attn_out, d_query, d_latent, d_key_rope,
                dwk.reshape(512, n_chip, 128), dwv.reshape(512, n_chip, 128))

    return jax.shard_map(local_step, mesh=mesh,
                         in_specs=(seq_spec, seq_spec, seq_spec, P(), P(), seq_spec),
                         out_specs=(seq_spec, seq_spec, seq_spec, seq_spec, P(), P()),
                         check_vma=False)
```

```python
import functools
import math

import jax
import jax.numpy as jnp
from jax import lax
from jax.experimental import pallas as pl
from jax.experimental.pallas import tpu as pltpu
from jax.sharding import PartitionSpec as P

MESH = pl.DeviceIdType.MESH
NX, NY = 2, 2
PLANE = NX * NY
BLK = 128
SUP = 256
CH = SUP * PLANE
NEG = -1e30
NT = (((1,), (1,)), ((), ()))
NN = (((1,), (0,)), ((), ()))
BF, F32 = jnp.bfloat16, jnp.float32


def mm(a, b, dims=NN):
    return lax.dot_general(a, b, dims, preferred_element_type=F32)


def pack_rope(x):
    return jnp.concatenate([x[:64], x[64:]], axis=1)


def kernel(nz, qk_dim, q_ref, do_ref, c_ref, rt_ref, wk_ref, wv_ref,
           o_out, dq_out, dv_recv, dk_recv, dwk_out, dwv_out,
           w_cat, wt_cat, q_recv, do_recv, c_all, kr, v, kt, vt, s_buf, p_buf, p_store, ds_buf, dkr, dv,
           qt, dof, dot_, ot, dqt, lse, delta_s, o_send, dq_send, dv_msg, dv_part, dk_msg, dk_part,
           dwt, dw_msg, dw_part, dw_all,
           q_ss, q_rs, do_ss, do_rs, o_ss, o_rs, dq_ss, dq_rs, dv_ss, dv_rs, dk_ss, dk_rs, pair_s, pair_r, dw_sem,
           cg_rz, cg_rp, cg_sz, cg_sx, cg_sp, v_rz, v_rp, v_sz, v_sx, v_sp, k_rz, k_rp, k_sz, k_sx, k_sp):
    n_chip = PLANE * nz
    n_dev = 2 * n_chip
    n_sup = n_chip // 2
    me = lax.axis_index("cp")
    chip, par = me // 2, me % 2
    partner = 2 * chip + (1 - par)
    x, y, z = chip % NX, (chip // NX) % NY, chip // PLANE
    scale = 1.0 / math.sqrt(qk_dim)
    c1 = scale * math.log2(math.e)
    scope = jax.named_scope

    def chip_at(zq, yq, xq):
        return (zq * NY + yq) * NX + xq

    def col_chip(col, zq):
        return chip_at(zq, 1 - y if col >= 2 else y, 1 - x if col % 2 else x)

    def remote(src, dst, ssem, rsem, dev):
        return pltpu.make_async_remote_copy(src_ref=src, dst_ref=dst, send_sem=ssem, recv_sem=rsem,
                                            device_id=(dev,), device_id_type=MESH)

    def start(src, dst, ssem, rsem, dev):
        @pl.when(dev == me)
        def _():
            pltpu.make_async_copy(src, dst, rsem).start()

        @pl.when(dev != me)
        def _():
            remote(src, dst, ssem, rsem, dev).start()

    def sent(src, dst, ssem, rsem, dev):
        @pl.when(dev != me)
        def _():
            remote(src, dst, ssem, rsem, dev).wait_send()

    def arrived(dst, rsem):
        pltpu.make_async_copy(dst, dst, rsem).wait()

    def loop(lo, hi, f):
        def body(i, carry):
            f(i)
            return carry

        lax.fori_loop(lo, hi, body, 0)

    with scope("barrier"):
        barrier = pltpu.get_barrier_semaphore()
        loop(1, n_dev, lambda i: pl.semaphore_signal(
            barrier, inc=1, device_id=(lax.rem(me + i, n_dev),), device_id_type=MESH))
        pl.semaphore_wait(barrier, n_dev - 1)

    class Gather:
        def __init__(self, buf, rows, split, chain, rz, rp, sz, sx, sp):
            self.buf, self.rows, self.split, self.chain = buf, rows, split, chain
            self.rz, self.rp, self.sz, self.sx, self.sp = rz, rp, sz, sx, sp
            self.dev_x = 2 * chip_at(z, y, 1 - x) + par
            self.dev_y = 2 * chip_at(z, 1 - y, x) + par

        def blk(self, col, zq):
            return self.buf.at[par, col_chip(col, zq)]

        def along_z(self, zq, to, k):
            b = self.blk(0, zq)
            return remote(b, b, self.sz.at[k, zq], self.rz.at[0, zq, 0], 2 * chip_at(to, y, x) + par)

        def to_x(self, col, zq):
            b = self.blk(col, zq)
            return remote(b, b, self.sx.at[0, zq], self.rz.at[1, zq, 0], self.dev_x)

        def to_y(self, col, zq):
            b = self.blk(col, zq)
            return remote(b, b, self.sx.at[1, zq], self.rz.at[2, zq, 0], self.dev_y)

        def part_y(self, col, zq):
            b = self.blk(col, zq).at[pl.ds(0, self.split)]
            return remote(b, b, self.sx.at[2, zq], self.rz.at[3, zq, 0], self.dev_y)

        def part_x(self, col, zq):
            b = self.blk(col, zq).at[pl.ds(self.split, self.rows - self.split)]
            return remote(b, b, self.sx.at[3, zq], self.rz.at[3, zq, 1], self.dev_x)

        def pair(self, col, zq):
            b = self.blk(col, zq)
            return remote(b, b, self.sp.at[col, zq], self.rp.at[col, zq], partner)

        def own_col(self, zq):
            self.to_x(0, zq).start()
            self.to_y(0, zq).start()
            self.pair(0, zq).start()

        def xy(self, zq):
            self.to_x(1, zq).wait_recv()
            self.part_y(1, zq).start()
            self.pair(1, zq).start()
            self.to_y(2, zq).wait_recv()
            self.part_x(2, zq).start()
            self.pair(2, zq).start()

        def diag(self, zq):
            self.part_y(3, zq).wait_recv()
            self.part_x(3, zq).wait_recv()
            self.pair(3, zq).start()

        def pairs(self, zq):
            for col in range(4):
                self.pair(col, zq).wait_recv()

        def z_sends(self, go):
            if self.chain:
                for zq in range(nz):
                    @pl.when(jnp.logical_and(z >= zq, z + 1 < nz))
                    def _():
                        go(self.along_z(zq, z + 1, 0))

                    @pl.when(jnp.logical_and(z <= zq, z > 0))
                    def _():
                        go(self.along_z(zq, z - 1, 1))
            else:
                for d in range(1, nz):
                    @pl.when(z + d < nz)
                    def _():
                        go(self.along_z(z, z + d, d - 1))

                    @pl.when(z - d >= 0)
                    def _():
                        go(self.along_z(z, z - d, nz - 2 + d))

        def begin(self):
            if self.chain:
                @pl.when(z + 1 < nz)
                def _():
                    self.along_z(z, z + 1, 0).start()

                @pl.when(z > 0)
                def _():
                    self.along_z(z, z - 1, 1).start()
            else:
                self.z_sends(lambda c: c.start())
            self.own_col(z)

        def from_z(self, d):
            @pl.when(z - d >= 0)
            def _():
                self.along_z(z - d, z, 0).wait_recv()
                if self.chain:
                    @pl.when(z + 1 < nz)
                    def _():
                        self.along_z(z - d, z + 1, 0).start()

                self.own_col(z - d)

            @pl.when(z + d < nz)
            def _():
                self.along_z(z + d, z, 1).wait_recv()
                if self.chain:
                    @pl.when(z > 0)
                    def _():
                        self.along_z(z + d, z - 1, 1).start()

                self.own_col(z + d)

        def at(self, d, f):
            if d == 0:
                f(z)
                return

            @pl.when(z - d >= 0)
            def _():
                f(z - d)

            @pl.when(z + d < nz)
            def _():
                f(z + d)

        def steps(self, ready):
            def last(zq):
                self.diag(zq)
                self.pairs(zq)
                ready(zq)

            for d in range(1, nz):
                self.from_z(d)
                self.at(d - 1, self.xy)
                yield
                if d >= 2:
                    self.at(d - 2, last)
                    yield
            self.at(nz - 1, self.xy)
            yield
            for d in range(max(nz - 2, 0), nz):
                self.at(d, last)
                yield

        def finish(self):
            self.z_sends(lambda c: c.wait_send())
            for zq in range(nz):
                for col in range(4):
                    self.pair(col, zq).wait_send()
                self.to_x(0, zq).wait_send()
                self.to_y(0, zq).wait_send()
                self.part_y(1, zq).wait_send()
                self.part_x(2, zq).wait_send()

    owner_core = lax.rem((chip + 1) // 2, 2)
    q_slot = 2 * (chip // 2) + par

    def sup_chip(s):
        return 2 * s + lax.rem(s + par, 2)

    def q_copy(i):
        head = lax.rem(chip + i, n_chip)
        return q_ref.at[head], q_recv.at[q_slot], q_ss.at[i], q_rs.at[q_slot], 2 * head + owner_core

    def do_copy(i):
        head = lax.rem(chip + i, n_chip)
        return do_ref.at[head], do_recv.at[q_slot], do_ss.at[i], do_rs.at[q_slot], 2 * head + owner_core

    def o_copy(s, i):
        return o_send.at[2 * s + i], o_out.at[chip], o_ss.at[2 * s + i], o_rs.at[chip], 2 * sup_chip(s) + i

    def dq_copy(s, i):
        return dq_send.at[2 * s + i], dq_out.at[chip], dq_ss.at[2 * s + i], dq_rs.at[chip], 2 * sup_chip(s) + i

    def dv_copy(ch):
        return dv_msg.at[par, ch], dv_recv.at[chip], dv_ss.at[ch], dv_rs.at[chip], 2 * ch + par

    def dk_copy(ch):
        return dk_msg.at[par, ch], dk_recv.at[chip], dk_ss.at[ch], dk_rs.at[chip], 2 * ch + par

    gc = Gather(c_all, 144, 80, False, cg_rz, cg_rp, cg_sz, cg_sx, cg_sp)
    with scope("send_c"):
        c_all[par, chip, pl.ds(0, BLK), :] = c_ref[...]
        for i in range(4):
            c_all[par, chip, pl.ds(BLK, 16), pl.ds(128 * i, 128)] = rt_ref[pl.ds(16 * i, 16), :]
        gc.begin()
    with scope("send_q"):
        def send_q(i):
            start(*q_copy(i))
            start(*do_copy(i))

        loop(0, n_chip, send_q)
    with scope("init"):
        dkr[...] = jnp.zeros_like(dkr)
        dv[...] = jnp.zeros_like(dv)
        w_cat[...] = jnp.concatenate([wk_ref[...], wv_ref[...]], axis=1)
        for i, w in enumerate((wk_ref, wv_ref)):
            wt_cat[pl.ds(i * 128, 128), :] = jnp.transpose(w[...].astype(F32)).astype(BF)
        qt[pl.ds(192, 64), :] = jnp.zeros((64, SUP), BF)

    def latent_of(ch):
        return jnp.concatenate([c_all[0, ch, pl.ds(0, BLK), :], c_all[1, ch, pl.ds(0, BLK), :]], axis=0)

    def up_project(ch):
        base = pl.multiple_of(ch * SUP, SUP)
        lat = latent_of(ch)
        kv = mm(lat, w_cat[...]).astype(BF)
        kvt = mm(wt_cat[...], lat, NT).astype(BF)
        kr[pl.ds(base, SUP), pl.ds(0, 128)] = kv[:, :128]
        v[pl.ds(base, SUP), :] = kv[:, 128:]
        kt[pl.ds(0, 128), pl.ds(base, SUP)] = kvt[:128]
        vt[:, pl.ds(base, SUP)] = kvt[128:]
        for q in range(2):
            rt = jnp.concatenate([c_all[q, ch, pl.ds(BLK, 16), pl.ds(128 * i, 128)] for i in range(4)], axis=0)
            kt[pl.ds(128, 64), pl.ds(base + q * BLK, BLK)] = rt
            r = jnp.transpose(rt.astype(F32))
            kr[pl.ds(base + q * BLK, BLK), pl.ds(128, 128)] = jnp.concatenate(
                [r, jnp.zeros_like(r)], axis=1).astype(BF)

    diff = lax.broadcasted_iota(jnp.int32, (SUP, SUP), 0) - lax.broadcasted_iota(jnp.int32, (SUP, SUP), 1)

    def load_q(s):
        for i in range(2):
            qt[pl.ds(0, 192), pl.ds(i * BLK, BLK)] = q_recv[2 * s + i]
            dof[pl.ds(i * BLK, BLK), :] = do_recv[2 * s + i]

    def store_row(s):
        a = s // 2
        return (a + 1) * (a + s % 2) * CH

    def forward(s):
        ch = sup_chip(s)
        for i in range(2):
            arrived(q_recv.at[2 * s + i], q_rs.at[2 * s + i])
            arrived(do_recv.at[2 * s + i], do_rs.at[2 * s + i])
        load_q(s)
        dot_[...] = jnp.transpose(dof[...].astype(F32))
        n_ch = s // 2 + 1

        def score(j, m8):
            for t in range(CH // SUP):
                r0 = pl.multiple_of(j * CH + t * SUP, SUP)
                st = mm(kr[pl.ds(r0, SUP), :], qt[...])
                st = jnp.where(diff <= ch * SUP - r0, st, NEG)
                s_buf[pl.ds(r0, SUP), :] = st
                m8 = jnp.maximum(m8, jnp.max(st.reshape(SUP // 8, 8, SUP), axis=0))
            return m8

        m8 = lax.fori_loop(0, n_ch, score, jnp.full((8, SUP), NEG, F32))
        m2 = jnp.max(m8, axis=0, keepdims=True) * c1
        ot[...] = jnp.zeros_like(ot)

        def values(j, l8):
            base = pl.multiple_of(j * CH, CH)
            for t in range(CH // SUP):
                p = jnp.exp2(s_buf[pl.ds(base + t * SUP, SUP), :] * c1 - m2)
                l8 = l8 + jnp.sum(p.reshape(SUP // 8, 8, SUP), axis=0)
                p_buf[pl.ds(t * SUP, SUP), :] = p.astype(BF)
            ot[...] += mm(vt[:, pl.ds(base, CH)], p_buf[...])
            return l8

        l8 = lax.fori_loop(0, n_ch, values, jnp.zeros((8, SUP), F32))
        l = jnp.sum(l8, axis=0, keepdims=True)
        o = ot[...] / l
        lse2 = m2 + jnp.log2(l)
        delta_s[s] = jnp.sum(o * dot_[...], axis=0, keepdims=True)
        o_rows = jnp.transpose(o)
        for i in range(2):
            o_send[2 * s + i] = o_rows[i * BLK:(i + 1) * BLK].astype(BF)
        for i in range(2):
            start(*o_copy(s, i))
        row0 = store_row(s)

        def values_grad(j):
            base = pl.multiple_of(j * CH, CH)
            for t in range(CH // SUP):
                rows = pl.ds(base + t * SUP, SUP)
                p = jnp.exp2(s_buf[rows, :] * c1 - lse2).astype(BF)
                p_store[pl.ds(pl.multiple_of(row0 + base + t * SUP, SUP), SUP), :] = p
                dv[rows, :] += mm(p, dof[...])

        loop(0, n_ch, values_grad)

    def backward(s):
        load_q(s)
        dqt[...] = jnp.zeros_like(dqt)
        row0 = store_row(s)
        delta = delta_s[s]

        def keys_grad(j):
            base = pl.multiple_of(j * CH, CH)
            for t in range(CH // SUP):
                rows = pl.ds(base + t * SUP, SUP)
                dp = mm(v[rows, :], dof[...], NT)
                p = p_store[pl.ds(pl.multiple_of(row0 + base + t * SUP, SUP), SUP), :].astype(F32)
                ds_buf[pl.ds(t * SUP, SUP), :] = (p * (dp - delta) * scale).astype(BF)
            for t in range(CH // SUP):
                rows = pl.ds(base + t * SUP, SUP)
                dkr[rows, :] += mm(ds_buf[pl.ds(t * SUP, SUP), :], qt[...], NT)
            dqt[...] += mm(kt[:, pl.ds(base, CH)], ds_buf[...])

        loop(0, s // 2 + 1, keys_grad)
        for i in range(2):
            dq_send[2 * s + i] = dqt[:, pl.ds(i * BLK, BLK)].astype(BF)
        for i in range(2):
            start(*dq_copy(s, i))

    def ready_c(zq):
        gc.pairs(zq)
        loop(zq * PLANE, (zq + 1) * PLANE, up_project)

    def col_ready(zq):
        @pl.when(z != zq)
        def _():
            gc.along_z(zq, z, 0).wait_recv()
            gc.own_col(zq)

    def step_c(k):
        if k < nz:
            col_ready(k)
        if 0 <= k - 1 < nz:
            gc.xy(k - 1)
        if 0 <= k - 2 < nz:
            gc.diag(k - 2)
            ready_c(k - 2)

    for k in range(nz + 2):
        with scope(f"c{k}"):
            step_c(k)
        if k >= 3:
            with scope(f"fwd{k - 3}"):
                loop(2 * (k - 3), 2 * (k - 3) + 2, forward)
    with scope(f"fwd{nz - 1}"):
        loop(2 * (nz - 1), 2 * nz, forward)

    def head_dw(k, lo, hi, grads):
        def add(ch):
            base = pl.multiple_of(ch * SUP, SUP)
            g = jnp.transpose(grads(pl.ds(base, SUP))).astype(BF)
            dwt[k] += mm(g, latent_of(ch))

        loop(lo, hi, add)

    def dw_exchange(k):
        dw_msg[k] = jnp.transpose(dwt[k]).reshape(2, SUP, 128)
        c = remote(dw_msg.at[k, 1 - par], dw_part.at[k], pair_s.at[k], pair_r.at[k], partner)
        c.start()
        return c

    def dw_begin(k, c):
        c.wait_recv()
        dw_all[k, par, chip] = dw_msg[k, par] + dw_part[k]

    def dw_out_copy(k, q, h):
        dst = dwk_out if k == 0 else dwv_out
        return pltpu.make_async_copy(dw_all.at[k, q, h], dst.at[pl.ds(q * SUP, SUP), h, 0], dw_sem.at[k, q, h])

    def put_dw(k):
        def put(zq):
            for q in range(2):
                loop(zq * PLANE, (zq + 1) * PLANE, lambda h: dw_out_copy(k, q, h).start())

        return put

    dwt[...] = jnp.zeros_like(dwt)
    gv = Gather(dw_all.at[1], SUP, 128, True, v_rz, v_rp, v_sz, v_sx, v_sp)
    gk = Gather(dw_all.at[0], SUP, 128, True, k_rz, k_rp, k_sz, k_sx, k_sp)
    with scope("dv"):
        def dv_out(ch):
            for q in range(2):
                dv_msg[q, ch] = dv[pl.ds(pl.multiple_of(ch * SUP, SUP) + q * BLK, BLK), :].astype(BF)

        loop(0, n_chip, dv_out)
        pair_dv = remote(dv_msg.at[1 - par], dv_part, pair_s.at[2], pair_r.at[2], partner)
        pair_dv.start()
        head_dw(1, 0, n_chip, lambda rows: dv[rows, :])
        pair_dwv = dw_exchange(1)
        pair_dv.wait_recv()

        def dv_add(ch):
            dv_msg[par, ch] = (dv_msg[par, ch].astype(F32) + dv_part[ch].astype(F32)).astype(BF)

        loop(0, n_chip, dv_add)
        dw_begin(1, pair_dwv)
        gv.begin()

        def dv_send(i):
            start(*dv_copy(lax.rem(chip + i, n_chip)))

        loop(0, n_chip, dv_send)

    pair_dk = [remote(dk_msg.at[1 - par, pl.ds(PLANE * g, PLANE)], dk_part.at[pl.ds(PLANE * g, PLANE)],
                      pair_s.at[3 + g], pair_r.at[3 + g], partner) for g in range(nz)]

    def dk_out(g):
        def put(ch):
            for q in range(2):
                rows = pl.ds(pl.multiple_of(ch * SUP, SUP) + q * BLK, BLK)
                dk_msg[q, ch, pl.ds(0, BLK), :] = dkr[rows, pl.ds(0, 128)].astype(BF)
                dk_msg[q, ch, pl.ds(BLK, 64), :] = pack_rope(dkr[rows, pl.ds(128, 128)][:, :64]).astype(BF)

        loop(PLANE * g, PLANE * (g + 1), put)
        pair_dk[g].start()
        head_dw(0, PLANE * g, PLANE * (g + 1), lambda rows: dkr[rows, pl.ds(0, 128)])

    def dk_send(g):
        pair_dk[g].wait_recv()

        def put(i):
            ch = PLANE * g + lax.rem(chip + i, PLANE)
            dk_msg[par, ch] = (dk_msg[par, ch].astype(F32) + dk_part[ch].astype(F32)).astype(BF)
            start(*dk_copy(ch))

        loop(0, PLANE, put)

    v_steps = gv.steps(put_dw(1))
    for g in reversed(range(nz)):
        for s in (2 * g + 1, 2 * g):
            with scope(f"bwd{s}"):
                backward(s)
            with scope(f"gv{s}"):
                next(v_steps, None)
        if g + 1 < nz:
            with scope(f"dks{g + 1}"):
                dk_send(g + 1)
        with scope(f"dko{g}"):
            dk_out(g)

    with scope("dwk"):
        pair_dwk = dw_exchange(0)
        dw_begin(0, pair_dwk)
        gk.begin()
    with scope("dks0"):
        dk_send(0)
    with scope("gv"):
        for _ in v_steps:
            pass
    with scope("gk"):
        for _ in gk.steps(put_dw(0)):
            pass

    with scope("drain"):
        for g in (gc, gv, gk):
            g.finish()
        for c in [pair_dv, pair_dwv, pair_dwk] + pair_dk:
            c.wait_send()

        def drain(i):
            sent(*q_copy(i))
            sent(*do_copy(i))
            sent(*o_copy(i // 2, i % 2))
            sent(*dq_copy(i // 2, i % 2))
            sent(*dv_copy(i))
            sent(*dk_copy(i))
            arrived(o_out.at[i], o_rs.at[i])
            arrived(dq_out.at[i], dq_rs.at[i])
            arrived(dv_recv.at[i], dv_rs.at[i])
            arrived(dk_recv.at[i], dk_rs.at[i])
            for k in range(2):
                for q in range(2):
                    dw_out_copy(k, q, i).wait()

        loop(0, n_chip, drain)


def solution(mesh):
    n_dev = mesh.shape["cp"]
    n_chip = n_dev // 2
    nz = n_chip // PLANE
    seq = n_dev * BLK
    seq_spec = P("cp")

    def local_step(queries, latent, key_rope, w_uk, w_uv, d_out):
        head = lax.axis_index("cp") // 2
        wk = lax.dynamic_index_in_dim(w_uk, head, 1, keepdims=False)
        wv = lax.dynamic_index_in_dim(w_uv, head, 1, keepdims=False)
        vm = pl.BlockSpec(memory_space=pltpu.VMEM)
        hbm = pl.BlockSpec(memory_space=pl.ANY)
        dma = pltpu.SemaphoreType.DMA
        gather_sems = [dma((4, nz, 2)), dma((4, nz)), dma((max(2 * nz - 2, 2), nz)), dma((4, nz)), dma((4, nz))]
        o, dq, dv, dk, dwk, dwv = pl.pallas_call(
            functools.partial(kernel, nz, queries.shape[-1]),
            out_shape=(jax.ShapeDtypeStruct((n_chip, BLK, 128), BF),
                       jax.ShapeDtypeStruct((n_chip, 192, BLK), BF),
                       jax.ShapeDtypeStruct((n_chip, BLK, 128), BF),
                       jax.ShapeDtypeStruct((n_chip, 192, 128), BF),
                       jax.ShapeDtypeStruct((512, n_chip, 1, 128), F32),
                       jax.ShapeDtypeStruct((512, n_chip, 1, 128), F32)),
            in_specs=[vm] * 6,
            out_specs=(vm, vm, vm, vm, hbm, hbm),
            scratch_shapes=[
                pltpu.VMEM((512, 256), BF),
                pltpu.VMEM((256, 512), BF),
                pltpu.VMEM((n_chip, 192, BLK), BF),
                pltpu.VMEM((n_chip, BLK, 128), BF),
                pltpu.VMEM((2, n_chip, 144, 512), BF),
                pltpu.VMEM((seq, 256), BF),
                pltpu.VMEM((seq, 128), BF),
                pltpu.VMEM((192, seq), BF),
                pltpu.VMEM((128, seq), BF),
                pltpu.VMEM((seq, SUP), F32),
                pltpu.VMEM((CH, SUP), BF),
                pltpu.VMEM((nz * (nz + 1) * CH, SUP), BF),
                pltpu.VMEM((CH, SUP), BF),
                pltpu.VMEM((seq, 256), F32),
                pltpu.VMEM((seq, 128), F32),
                pltpu.VMEM((256, SUP), BF),
                pltpu.VMEM((SUP, 128), BF),
                pltpu.VMEM((128, SUP), F32),
                pltpu.VMEM((128, SUP), F32),
                pltpu.VMEM((192, SUP), F32),
                pltpu.VMEM((8, SUP), F32),
                pltpu.VMEM((n_chip // 2, 1, SUP), F32),
                pltpu.VMEM((n_chip, BLK, 128), BF),
                pltpu.VMEM((n_chip, 192, BLK), BF),
                pltpu.VMEM((2, n_chip, BLK, 128), BF),
                pltpu.VMEM((n_chip, BLK, 128), BF),
                pltpu.VMEM((2, n_chip, 192, 128), BF),
                pltpu.VMEM((n_chip, 192, 128), BF),
                pltpu.VMEM((2, 128, 512), F32),
                pltpu.VMEM((2, 2, SUP, 128), F32),
                pltpu.VMEM((2, SUP, 128), F32),
                pltpu.VMEM((2, 2, n_chip, SUP, 128), F32),
            ] + [dma((n_chip,))] * 12 + [dma((3 + nz,)), dma((3 + nz,)), dma((2, 2, n_chip))] + gather_sems * 3,
            compiler_params=pltpu.CompilerParams(
                collective_id=0, has_side_effects=True, vmem_limit_bytes=62 * 1024 * 1024),
        )(queries.transpose(1, 2, 0), d_out.transpose(1, 0, 2), latent, key_rope.T, wk, wv)
        d_latent = (jnp.einsum("htd,lhd->tl", dk[:, :BLK], w_uk, preferred_element_type=F32)
                    + jnp.einsum("htd,lhd->tl", dv, w_uv, preferred_element_type=F32)).astype(BF)
        dr = jnp.sum(dk[:, BLK:].astype(F32), axis=0)
        d_key_rope = jnp.concatenate([dr[:, :64], dr[:, 64:]], axis=0).astype(BF)
        return (o.transpose(1, 0, 2), dq.transpose(2, 0, 1), d_latent, d_key_rope,
                dwk.reshape(512, n_chip, 128), dwv.reshape(512, n_chip, 128))

    return jax.shard_map(local_step, mesh=mesh,
                         in_specs=(seq_spec, seq_spec, seq_spec, P(), P(), seq_spec),
                         out_specs=(seq_spec, seq_spec, seq_spec, seq_spec, P(), P()),
                         check_vma=False)
```

```python
import functools
import math

import jax
import jax.numpy as jnp
from jax import lax
from jax.experimental import pallas as pl
from jax.experimental.pallas import tpu as pltpu
from jax.sharding import PartitionSpec as P

MESH = pl.DeviceIdType.MESH
NX, NY = 2, 2
PLANE = NX * NY
BLK = 128
SUP = 256
CH = SUP * PLANE
NEG = -1e30
NT = (((1,), (1,)), ((), ()))
NN = (((1,), (0,)), ((), ()))
BF, F32 = jnp.bfloat16, jnp.float32


def mm(a, b, dims=NN):
    return lax.dot_general(a, b, dims, preferred_element_type=F32)


def pack_rope(x):
    return jnp.concatenate([x[:64], x[64:]], axis=1)


def kernel(nz, qk_dim, q_ref, do_ref, c_ref, rt_ref, wk_ref, wv_ref,
           o_out, dq_out, dv_recv, dk_recv, dwk_out, dwv_out,
           w_cat, wt_cat, q_recv, do_recv, c_all, kr, v, kt, vt, s_buf, p_buf, p_store, ds_buf, dkr, dv,
           qt, dof, dot_, ot, dqt, lse, delta_s, o_send, dq_send, dv_msg, dv_part, dk_msg, dk_part,
           dwt, dw_msg, dw_part, dw_all,
           q_ss, q_rs, do_ss, do_rs, o_ss, o_rs, dq_ss, dq_rs, dv_ss, dv_rs, dk_ss, dk_rs, pair_s, pair_r, dw_sem,
           cg_rz, cg_rp, cg_sz, cg_sx, cg_sp, w_rz, w_rp, w_sz, w_sx, w_sp):
    n_chip = PLANE * nz
    n_dev = 2 * n_chip
    n_sup = n_chip // 2
    me = lax.axis_index("cp")
    chip, par = me // 2, me % 2
    partner = 2 * chip + (1 - par)
    x, y, z = chip % NX, (chip // NX) % NY, chip // PLANE
    scale = 1.0 / math.sqrt(qk_dim)
    c1 = scale * math.log2(math.e)
    scope = jax.named_scope

    def chip_at(zq, yq, xq):
        return (zq * NY + yq) * NX + xq

    def col_chip(col, zq):
        return chip_at(zq, 1 - y if col >= 2 else y, 1 - x if col % 2 else x)

    def remote(src, dst, ssem, rsem, dev):
        return pltpu.make_async_remote_copy(src_ref=src, dst_ref=dst, send_sem=ssem, recv_sem=rsem,
                                            device_id=(dev,), device_id_type=MESH)

    def start(src, dst, ssem, rsem, dev):
        @pl.when(dev == me)
        def _():
            pltpu.make_async_copy(src, dst, rsem).start()

        @pl.when(dev != me)
        def _():
            remote(src, dst, ssem, rsem, dev).start()

    def sent(src, dst, ssem, rsem, dev):
        @pl.when(dev != me)
        def _():
            remote(src, dst, ssem, rsem, dev).wait_send()

    def arrived(dst, rsem):
        pltpu.make_async_copy(dst, dst, rsem).wait()

    def loop(lo, hi, f):
        def body(i, carry):
            f(i)
            return carry

        lax.fori_loop(lo, hi, body, 0)

    with scope("barrier"):
        barrier = pltpu.get_barrier_semaphore()
        loop(1, n_dev, lambda i: pl.semaphore_signal(
            barrier, inc=1, device_id=(lax.rem(me + i, n_dev),), device_id_type=MESH))
        pl.semaphore_wait(barrier, n_dev - 1)

    class Gather:
        def __init__(self, buf, rows, split, chain, rz, rp, sz, sx, sp):
            self.buf, self.rows, self.split, self.chain = buf, rows, split, chain
            self.rz, self.rp, self.sz, self.sx, self.sp = rz, rp, sz, sx, sp
            self.dev_x = 2 * chip_at(z, y, 1 - x) + par
            self.dev_y = 2 * chip_at(z, 1 - y, x) + par

        def blk(self, col, zq):
            return self.buf.at[par, col_chip(col, zq)]

        def along_z(self, zq, to, k):
            b = self.blk(0, zq)
            return remote(b, b, self.sz.at[k, zq], self.rz.at[0, zq, 0], 2 * chip_at(to, y, x) + par)

        def to_x(self, col, zq):
            b = self.blk(col, zq)
            return remote(b, b, self.sx.at[0, zq], self.rz.at[1, zq, 0], self.dev_x)

        def to_y(self, col, zq):
            b = self.blk(col, zq)
            return remote(b, b, self.sx.at[1, zq], self.rz.at[2, zq, 0], self.dev_y)

        def part_y(self, col, zq):
            b = self.blk(col, zq).at[pl.ds(0, self.split)]
            return remote(b, b, self.sx.at[2, zq], self.rz.at[3, zq, 0], self.dev_y)

        def part_x(self, col, zq):
            b = self.blk(col, zq).at[pl.ds(self.split, self.rows - self.split)]
            return remote(b, b, self.sx.at[3, zq], self.rz.at[3, zq, 1], self.dev_x)

        def pair(self, col, zq):
            b = self.blk(col, zq)
            return remote(b, b, self.sp.at[col, zq], self.rp.at[col, zq], partner)

        def own_col(self, zq):
            self.to_x(0, zq).start()
            self.to_y(0, zq).start()
            self.pair(0, zq).start()

        def xy(self, zq):
            self.to_x(1, zq).wait_recv()
            self.part_y(1, zq).start()
            self.pair(1, zq).start()
            self.to_y(2, zq).wait_recv()
            self.part_x(2, zq).start()
            self.pair(2, zq).start()

        def diag(self, zq):
            self.part_y(3, zq).wait_recv()
            self.part_x(3, zq).wait_recv()
            self.pair(3, zq).start()

        def pairs(self, zq):
            for col in range(4):
                self.pair(col, zq).wait_recv()

        def z_sends(self, go):
            if self.chain:
                for zq in range(nz):
                    @pl.when(jnp.logical_and(z >= zq, z + 1 < nz))
                    def _():
                        go(self.along_z(zq, z + 1, 0))

                    @pl.when(jnp.logical_and(z <= zq, z > 0))
                    def _():
                        go(self.along_z(zq, z - 1, 1))
            else:
                for d in range(1, nz):
                    @pl.when(z + d < nz)
                    def _():
                        go(self.along_z(z, z + d, d - 1))

                    @pl.when(z - d >= 0)
                    def _():
                        go(self.along_z(z, z - d, nz - 2 + d))

        def begin(self):
            if self.chain:
                @pl.when(z + 1 < nz)
                def _():
                    self.along_z(z, z + 1, 0).start()

                @pl.when(z > 0)
                def _():
                    self.along_z(z, z - 1, 1).start()
            else:
                self.z_sends(lambda c: c.start())
            self.own_col(z)

        def from_z(self, d):
            @pl.when(z - d >= 0)
            def _():
                self.along_z(z - d, z, 0).wait_recv()
                if self.chain:
                    @pl.when(z + 1 < nz)
                    def _():
                        self.along_z(z - d, z + 1, 0).start()

                self.own_col(z - d)

            @pl.when(z + d < nz)
            def _():
                self.along_z(z + d, z, 1).wait_recv()
                if self.chain:
                    @pl.when(z > 0)
                    def _():
                        self.along_z(z + d, z - 1, 1).start()

                self.own_col(z + d)

        def at(self, d, f):
            if d == 0:
                f(z)
                return

            @pl.when(z - d >= 0)
            def _():
                f(z - d)

            @pl.when(z + d < nz)
            def _():
                f(z + d)

        def steps(self, ready):
            def last(zq):
                self.diag(zq)
                self.pairs(zq)
                ready(zq)

            for d in range(1, nz):
                with scope(f"wz{d}"):
                    self.from_z(d)
                with scope(f"wxy{d - 1}"):
                    self.at(d - 1, self.xy)
                yield
                if d >= 2:
                    with scope(f"wd{d - 2}"):
                        self.at(d - 2, last)
                    yield
            with scope(f"wxy{nz - 1}"):
                self.at(nz - 1, self.xy)
            yield
            for d in range(max(nz - 2, 0), nz):
                with scope(f"wd{d}"):
                    self.at(d, last)
                yield

        def finish(self):
            self.z_sends(lambda c: c.wait_send())
            for zq in range(nz):
                for col in range(4):
                    self.pair(col, zq).wait_send()
                self.to_x(0, zq).wait_send()
                self.to_y(0, zq).wait_send()
                self.part_y(1, zq).wait_send()
                self.part_x(2, zq).wait_send()

    owner_core = lax.rem((chip + 1) // 2, 2)
    q_slot = 2 * (chip // 2) + par

    def sup_chip(s):
        return 2 * s + lax.rem(s + par, 2)

    def q_copy(i):
        head = lax.rem(chip + i, n_chip)
        return q_ref.at[head], q_recv.at[q_slot], q_ss.at[i], q_rs.at[q_slot], 2 * head + owner_core

    def do_copy(i):
        head = lax.rem(chip + i, n_chip)
        return do_ref.at[head], do_recv.at[q_slot], do_ss.at[i], do_rs.at[q_slot], 2 * head + owner_core

    def o_copy(s, i):
        return o_send.at[2 * s + i], o_out.at[chip], o_ss.at[2 * s + i], o_rs.at[chip], 2 * sup_chip(s) + i

    def dq_copy(s, i):
        return dq_send.at[2 * s + i], dq_out.at[chip], dq_ss.at[2 * s + i], dq_rs.at[chip], 2 * sup_chip(s) + i

    def dv_copy(ch):
        return dv_msg.at[par, ch], dv_recv.at[chip], dv_ss.at[ch], dv_rs.at[chip], 2 * ch + par

    def dk_copy(ch):
        return dk_msg.at[par, ch], dk_recv.at[chip], dk_ss.at[ch], dk_rs.at[chip], 2 * ch + par

    gc = Gather(c_all, 144, 80, False, cg_rz, cg_rp, cg_sz, cg_sx, cg_sp)
    with scope("send_c"):
        c_all[par, chip, pl.ds(0, BLK), :] = c_ref[...]
        for i in range(4):
            c_all[par, chip, pl.ds(BLK, 16), pl.ds(128 * i, 128)] = rt_ref[pl.ds(16 * i, 16), :]
        gc.begin()
    with scope("send_q"):
        def send_q(i):
            start(*q_copy(i))
            start(*do_copy(i))

        @pl.when(z < nz // 2)
        def _():
            loop(0, n_chip, send_q)

    with scope("init"):
        dkr[...] = jnp.zeros_like(dkr)
        dv[...] = jnp.zeros_like(dv)
        w_cat[...] = jnp.concatenate([wk_ref[...], wv_ref[...]], axis=1)
        for i, w in enumerate((wk_ref, wv_ref)):
            wt_cat[pl.ds(i * 128, 128), :] = jnp.transpose(w[...].astype(F32)).astype(BF)
        qt[pl.ds(192, 64), :] = jnp.zeros((64, SUP), BF)

    def latent_of(ch):
        return jnp.concatenate([c_all[0, ch, pl.ds(0, BLK), :], c_all[1, ch, pl.ds(0, BLK), :]], axis=0)

    def up_project(ch):
        base = pl.multiple_of(ch * SUP, SUP)
        lat = latent_of(ch)
        kv = mm(lat, w_cat[...]).astype(BF)
        kvt = mm(wt_cat[...], lat, NT).astype(BF)
        kr[pl.ds(base, SUP), pl.ds(0, 128)] = kv[:, :128]
        v[pl.ds(base, SUP), :] = kv[:, 128:]
        kt[pl.ds(0, 128), pl.ds(base, SUP)] = kvt[:128]
        vt[:, pl.ds(base, SUP)] = kvt[128:]
        for q in range(2):
            rt = jnp.concatenate([c_all[q, ch, pl.ds(BLK, 16), pl.ds(128 * i, 128)] for i in range(4)], axis=0)
            kt[pl.ds(128, 64), pl.ds(base + q * BLK, BLK)] = rt
            r = jnp.transpose(rt.astype(F32))
            kr[pl.ds(base + q * BLK, BLK), pl.ds(128, 128)] = jnp.concatenate(
                [r, jnp.zeros_like(r)], axis=1).astype(BF)

    diff = lax.broadcasted_iota(jnp.int32, (SUP, SUP), 0) - lax.broadcasted_iota(jnp.int32, (SUP, SUP), 1)

    def load_q(s):
        for i in range(2):
            qt[pl.ds(0, 192), pl.ds(i * BLK, BLK)] = q_recv[2 * s + i]
            dof[pl.ds(i * BLK, BLK), :] = do_recv[2 * s + i]

    def store_row(s):
        a = s // 2
        return (a + 1) * (a + s % 2) * CH

    def forward(s):
        ch = sup_chip(s)
        for i in range(2):
            arrived(q_recv.at[2 * s + i], q_rs.at[2 * s + i])
            arrived(do_recv.at[2 * s + i], do_rs.at[2 * s + i])
        load_q(s)
        dot_[...] = jnp.transpose(dof[...].astype(F32))
        n_ch = s // 2 + 1

        def score(j, m8):
            for t in range(CH // SUP):
                r0 = pl.multiple_of(j * CH + t * SUP, SUP)
                st = mm(kr[pl.ds(r0, SUP), :], qt[...])
                st = jnp.where(diff <= ch * SUP - r0, st, NEG)
                s_buf[pl.ds(r0, SUP), :] = st
                m8 = jnp.maximum(m8, jnp.max(st.reshape(SUP // 8, 8, SUP), axis=0))
            return m8

        m8 = lax.fori_loop(0, n_ch, score, jnp.full((8, SUP), NEG, F32))
        m2 = jnp.max(m8, axis=0, keepdims=True) * c1
        ot[...] = jnp.zeros_like(ot)

        def values(j, l8):
            base = pl.multiple_of(j * CH, CH)
            for t in range(CH // SUP):
                p = jnp.exp2(s_buf[pl.ds(base + t * SUP, SUP), :] * c1 - m2)
                l8 = l8 + jnp.sum(p.reshape(SUP // 8, 8, SUP), axis=0)
                p_buf[pl.ds(t * SUP, SUP), :] = p.astype(BF)
            ot[...] += mm(vt[:, pl.ds(base, CH)], p_buf[...])
            return l8

        l8 = lax.fori_loop(0, n_ch, values, jnp.zeros((8, SUP), F32))
        l = jnp.sum(l8, axis=0, keepdims=True)
        o = ot[...] / l
        lse2 = m2 + jnp.log2(l)
        delta_s[s] = jnp.sum(o * dot_[...], axis=0, keepdims=True)
        o_rows = jnp.transpose(o)
        for i in range(2):
            o_send[2 * s + i] = o_rows[i * BLK:(i + 1) * BLK].astype(BF)
        for i in range(2):
            start(*o_copy(s, i))
        row0 = store_row(s)

        def values_grad(j):
            base = pl.multiple_of(j * CH, CH)
            for t in range(CH // SUP):
                rows = pl.ds(base + t * SUP, SUP)
                p = jnp.exp2(s_buf[rows, :] * c1 - lse2).astype(BF)
                p_store[pl.ds(pl.multiple_of(row0 + base + t * SUP, SUP), SUP), :] = p
                dv[rows, :] += mm(p, dof[...])

        loop(0, n_ch, values_grad)

    def backward(s):
        load_q(s)
        dqt[...] = jnp.zeros_like(dqt)
        row0 = store_row(s)
        delta = delta_s[s]

        def keys_grad(j):
            base = pl.multiple_of(j * CH, CH)
            for t in range(CH // SUP):
                rows = pl.ds(base + t * SUP, SUP)
                dp = mm(v[rows, :], dof[...], NT)
                p = p_store[pl.ds(pl.multiple_of(row0 + base + t * SUP, SUP), SUP), :].astype(F32)
                ds_buf[pl.ds(t * SUP, SUP), :] = (p * (dp - delta) * scale).astype(BF)
            for t in range(CH // SUP):
                rows = pl.ds(base + t * SUP, SUP)
                dkr[rows, :] += mm(ds_buf[pl.ds(t * SUP, SUP), :], qt[...], NT)
            dqt[...] += mm(kt[:, pl.ds(base, CH)], ds_buf[...])

        loop(0, s // 2 + 1, keys_grad)
        for i in range(2):
            dq_send[2 * s + i] = dqt[:, pl.ds(i * BLK, BLK)].astype(BF)
        for i in range(2):
            start(*dq_copy(s, i))

    def ready_c(zq):
        gc.pairs(zq)
        loop(zq * PLANE, (zq + 1) * PLANE, up_project)

    def col_ready(zq):
        @pl.when(z != zq)
        def _():
            gc.along_z(zq, z, 0).wait_recv()
            gc.own_col(zq)

    def step_c(k):
        if k < nz:
            col_ready(k)
        if 0 <= k - 1 < nz:
            gc.xy(k - 1)
        if 0 <= k - 2 < nz:
            gc.diag(k - 2)
            ready_c(k - 2)

    for k in range(nz + 2):
        with scope(f"c{k}"):
            step_c(k)
            if k == nz - 1:
                @pl.when(z >= nz // 2)
                def _():
                    loop(0, n_chip, send_q)

        if k >= 3:
            with scope(f"fwd{k - 3}"):
                loop(2 * (k - 3), 2 * (k - 3) + 2, forward)
    with scope(f"fwd{nz - 1}"):
        loop(2 * (nz - 1), 2 * nz, forward)

    def head_dw(k, lo, hi, grads):
        def add(ch):
            base = pl.multiple_of(ch * SUP, SUP)
            g = jnp.transpose(grads(pl.ds(base, SUP))).astype(BF)
            dwt[k] += mm(g, latent_of(ch))

        loop(lo, hi, add)

    def dw_exchange(k):
        dw_msg[k] = jnp.transpose(dwt[k]).reshape(2, SUP, 128)
        c = remote(dw_msg.at[k, 1 - par], dw_part.at[k], pair_s.at[k], pair_r.at[k], partner)
        c.start()
        return c

    def dw_begin(k, c):
        c.wait_recv()
        dw_all[par, chip, pl.ds(k * SUP, SUP), :] = dw_msg[k, par] + dw_part[k]

    def dw_out_copy(k, q, h):
        dst = dwk_out if k == 0 else dwv_out
        return pltpu.make_async_copy(dw_all.at[q, h, pl.ds(k * SUP, SUP)], dst.at[pl.ds(q * SUP, SUP), h, 0], dw_sem.at[k, q, h])

    def put_dw(zq):
        for k in range(2):
            for q in range(2):
                loop(zq * PLANE, (zq + 1) * PLANE, lambda h: dw_out_copy(k, q, h).start())

    dwt[...] = jnp.zeros_like(dwt)
    gw = Gather(dw_all, 2 * SUP, SUP, True, w_rz, w_rp, w_sz, w_sx, w_sp)
    with scope("dv"):
        def dv_out(ch):
            for q in range(2):
                dv_msg[q, ch] = dv[pl.ds(pl.multiple_of(ch * SUP, SUP) + q * BLK, BLK), :].astype(BF)

        loop(0, n_chip, dv_out)
        pair_dv = remote(dv_msg.at[1 - par], dv_part, pair_s.at[2], pair_r.at[2], partner)
        pair_dv.start()
        head_dw(1, 0, n_chip, lambda rows: dv[rows, :])
        pair_dwv = dw_exchange(1)
        pair_dv.wait_recv()

        def dv_add(ch):
            dv_msg[par, ch] = (dv_msg[par, ch].astype(F32) + dv_part[ch].astype(F32)).astype(BF)

        loop(0, n_chip, dv_add)
        dw_begin(1, pair_dwv)

        def dv_send(i):
            start(*dv_copy(lax.rem(chip + i, n_chip)))

        loop(0, n_chip, dv_send)

    pair_dk = [remote(dk_msg.at[1 - par, pl.ds(PLANE * g, PLANE)], dk_part.at[pl.ds(PLANE * g, PLANE)],
                      pair_s.at[3 + g], pair_r.at[3 + g], partner) for g in range(nz)]

    def dk_out(g):
        def put(ch):
            for q in range(2):
                rows = pl.ds(pl.multiple_of(ch * SUP, SUP) + q * BLK, BLK)
                dk_msg[q, ch, pl.ds(0, BLK), :] = dkr[rows, pl.ds(0, 128)].astype(BF)
                dk_msg[q, ch, pl.ds(BLK, 64), :] = pack_rope(dkr[rows, pl.ds(128, 128)][:, :64]).astype(BF)

        loop(PLANE * g, PLANE * (g + 1), put)
        pair_dk[g].start()
        head_dw(0, PLANE * g, PLANE * (g + 1), lambda rows: dkr[rows, pl.ds(0, 128)])

    def dk_send(g):
        pair_dk[g].wait_recv()

        def put(i):
            ch = PLANE * g + lax.rem(chip + i, PLANE)
            dk_msg[par, ch] = (dk_msg[par, ch].astype(F32) + dk_part[ch].astype(F32)).astype(BF)
            start(*dk_copy(ch))

        loop(0, PLANE, put)

    for g in reversed(range(nz)):
        for s in (2 * g + 1, 2 * g):
            with scope(f"bwd{s}"):
                backward(s)
        if g + 1 < nz:
            with scope(f"dks{g + 1}"):
                dk_send(g + 1)
        with scope(f"dko{g}"):
            dk_out(g)

    with scope("dwk"):
        pair_dwk = dw_exchange(0)
        dw_begin(0, pair_dwk)
        gw.begin()
    with scope("dks0"):
        dk_send(0)
    for i, _ in enumerate(gw.steps(put_dw)):
        pass

    with scope("drain"):
        for g in (gc, gw):
            g.finish()
        for c in [pair_dv, pair_dwv, pair_dwk] + pair_dk:
            c.wait_send()

        def drain(i):
            sent(*q_copy(i))
            sent(*do_copy(i))
            sent(*o_copy(i // 2, i % 2))
            sent(*dq_copy(i // 2, i % 2))
            sent(*dv_copy(i))
            sent(*dk_copy(i))
            arrived(o_out.at[i], o_rs.at[i])
            arrived(dq_out.at[i], dq_rs.at[i])
            arrived(dv_recv.at[i], dv_rs.at[i])
            arrived(dk_recv.at[i], dk_rs.at[i])
            for k in range(2):
                for q in range(2):
                    dw_out_copy(k, q, i).wait()

        loop(0, n_chip, drain)


def solution(mesh):
    n_dev = mesh.shape["cp"]
    n_chip = n_dev // 2
    nz = n_chip // PLANE
    seq = n_dev * BLK
    seq_spec = P("cp")

    def local_step(queries, latent, key_rope, w_uk, w_uv, d_out):
        head = lax.axis_index("cp") // 2
        wk = lax.dynamic_index_in_dim(w_uk, head, 1, keepdims=False)
        wv = lax.dynamic_index_in_dim(w_uv, head, 1, keepdims=False)
        vm = pl.BlockSpec(memory_space=pltpu.VMEM)
        hbm = pl.BlockSpec(memory_space=pl.ANY)
        dma = pltpu.SemaphoreType.DMA
        gather_sems = [dma((4, nz, 2)), dma((4, nz)), dma((max(2 * nz - 2, 2), nz)), dma((4, nz)), dma((4, nz))]
        o, dq, dv, dk, dwk, dwv = pl.pallas_call(
            functools.partial(kernel, nz, queries.shape[-1]),
            out_shape=(jax.ShapeDtypeStruct((n_chip, BLK, 128), BF),
                       jax.ShapeDtypeStruct((n_chip, 192, BLK), BF),
                       jax.ShapeDtypeStruct((n_chip, BLK, 128), BF),
                       jax.ShapeDtypeStruct((n_chip, 192, 128), BF),
                       jax.ShapeDtypeStruct((512, n_chip, 1, 128), F32),
                       jax.ShapeDtypeStruct((512, n_chip, 1, 128), F32)),
            in_specs=[vm] * 6,
            out_specs=(vm, vm, vm, vm, hbm, hbm),
            scratch_shapes=[
                pltpu.VMEM((512, 256), BF),
                pltpu.VMEM((256, 512), BF),
                pltpu.VMEM((n_chip, 192, BLK), BF),
                pltpu.VMEM((n_chip, BLK, 128), BF),
                pltpu.VMEM((2, n_chip, 144, 512), BF),
                pltpu.VMEM((seq, 256), BF),
                pltpu.VMEM((seq, 128), BF),
                pltpu.VMEM((192, seq), BF),
                pltpu.VMEM((128, seq), BF),
                pltpu.VMEM((seq, SUP), F32),
                pltpu.VMEM((CH, SUP), BF),
                pltpu.VMEM((nz * (nz + 1) * CH, SUP), BF),
                pltpu.VMEM((CH, SUP), BF),
                pltpu.VMEM((seq, 256), F32),
                pltpu.VMEM((seq, 128), F32),
                pltpu.VMEM((256, SUP), BF),
                pltpu.VMEM((SUP, 128), BF),
                pltpu.VMEM((128, SUP), F32),
                pltpu.VMEM((128, SUP), F32),
                pltpu.VMEM((192, SUP), F32),
                pltpu.VMEM((8, SUP), F32),
                pltpu.VMEM((n_chip // 2, 1, SUP), F32),
                pltpu.VMEM((n_chip, BLK, 128), BF),
                pltpu.VMEM((n_chip, 192, BLK), BF),
                pltpu.VMEM((2, n_chip, BLK, 128), BF),
                pltpu.VMEM((n_chip, BLK, 128), BF),
                pltpu.VMEM((2, n_chip, 192, 128), BF),
                pltpu.VMEM((n_chip, 192, 128), BF),
                pltpu.VMEM((2, 128, 512), F32),
                pltpu.VMEM((2, 2, SUP, 128), F32),
                pltpu.VMEM((2, SUP, 128), F32),
                pltpu.VMEM((2, n_chip, 2 * SUP, 128), F32),
            ] + [dma((n_chip,))] * 12 + [dma((3 + nz,)), dma((3 + nz,)), dma((2, 2, n_chip))] + gather_sems * 2,
            compiler_params=pltpu.CompilerParams(
                collective_id=0, has_side_effects=True, vmem_limit_bytes=62 * 1024 * 1024),
        )(queries.transpose(1, 2, 0), d_out.transpose(1, 0, 2), latent, key_rope.T, wk, wv)
        d_latent = (jnp.einsum("htd,lhd->tl", dk[:, :BLK], w_uk, preferred_element_type=F32)
                    + jnp.einsum("htd,lhd->tl", dv, w_uv, preferred_element_type=F32)).astype(BF)
        dr = jnp.sum(dk[:, BLK:].astype(F32), axis=0)
        d_key_rope = jnp.concatenate([dr[:, :64], dr[:, 64:]], axis=0).astype(BF)
        return (o.transpose(1, 0, 2), dq.transpose(2, 0, 1), d_latent, d_key_rope,
                dwk.reshape(512, n_chip, 128), dwv.reshape(512, n_chip, 128))

    return jax.shard_map(local_step, mesh=mesh,
                         in_specs=(seq_spec, seq_spec, seq_spec, P(), P(), seq_spec),
                         out_specs=(seq_spec, seq_spec, seq_spec, seq_spec, P(), P()),
                         check_vma=False)
```

```python
import functools
import math

import jax
import jax.numpy as jnp
from jax import lax
from jax.experimental import pallas as pl
from jax.experimental.pallas import tpu as pltpu
from jax.sharding import PartitionSpec as P

MESH = pl.DeviceIdType.MESH
NX, NY = 2, 2
PLANE = NX * NY
BLK = 128
SUP = 256
CH = SUP * PLANE
NEG = -1e30
NT = (((1,), (1,)), ((), ()))
NN = (((1,), (0,)), ((), ()))
BF, F32 = jnp.bfloat16, jnp.float32


def mm(a, b, dims=NN):
    return lax.dot_general(a, b, dims, preferred_element_type=F32)


def pack_rope(x):
    return jnp.concatenate([x[:64], x[64:]], axis=1)


def kernel(nz, qk_dim, q_ref, do_ref, c_ref, rt_ref, wk_ref, wv_ref,
           o_hbm, dq_hbm, dv_hbm, dk_hbm, dwk_out, dwv_out,
           o_out, dq_out, dv_recv, dk_recv,
           w_cat, wt_cat, q_recv, do_recv, c_all, kr, v, kt, vt, s_buf, p_buf, p_store, ds_buf, dkr, dv,
           qt, dof, dot_, ot, dqt, lse, delta_s, o_send, dq_send, dv_msg, dv_part, dk_msg, dk_part,
           dwt, dw_msg, dw_part, dw_all,
           q_ss, q_rs, do_ss, do_rs, o_ss, o_rs, dq_ss, dq_rs, dv_ss, dv_rs, dk_ss, dk_rs, pair_s, pair_r, dw_sem, out_sem,
           cg_rz, cg_rp, cg_sz, cg_sx, cg_sp, v_rz, v_rp, v_sz, v_sx, v_sp, k_rz, k_rp, k_sz, k_sx, k_sp):
    n_chip = PLANE * nz
    n_dev = 2 * n_chip
    n_sup = n_chip // 2
    me = lax.axis_index("cp")
    chip, par = me // 2, me % 2
    partner = 2 * chip + (1 - par)
    x, y, z = chip % NX, (chip // NX) % NY, chip // PLANE
    scale = 1.0 / math.sqrt(qk_dim)
    c1 = scale * math.log2(math.e)
    scope = jax.named_scope

    def chip_at(zq, yq, xq):
        return (zq * NY + yq) * NX + xq

    def col_chip(col, zq):
        return chip_at(zq, 1 - y if col >= 2 else y, 1 - x if col % 2 else x)

    def remote(src, dst, ssem, rsem, dev):
        return pltpu.make_async_remote_copy(src_ref=src, dst_ref=dst, send_sem=ssem, recv_sem=rsem,
                                            device_id=(dev,), device_id_type=MESH)

    def start(src, dst, ssem, rsem, dev):
        @pl.when(dev == me)
        def _():
            pltpu.make_async_copy(src, dst, rsem).start()

        @pl.when(dev != me)
        def _():
            remote(src, dst, ssem, rsem, dev).start()

    def sent(src, dst, ssem, rsem, dev):
        @pl.when(dev != me)
        def _():
            remote(src, dst, ssem, rsem, dev).wait_send()

    def arrived(dst, rsem):
        pltpu.make_async_copy(dst, dst, rsem).wait()

    def loop(lo, hi, f):
        def body(i, carry):
            f(i)
            return carry

        lax.fori_loop(lo, hi, body, 0)

    with scope("barrier"):
        barrier = pltpu.get_barrier_semaphore()
        loop(1, n_dev, lambda i: pl.semaphore_signal(
            barrier, inc=1, device_id=(lax.rem(me + i, n_dev),), device_id_type=MESH))
        pl.semaphore_wait(barrier, n_dev - 1)

    class Gather:
        def __init__(self, buf, rows, split, chain, rz, rp, sz, sx, sp):
            self.buf, self.rows, self.split, self.chain = buf, rows, split, chain
            self.rz, self.rp, self.sz, self.sx, self.sp = rz, rp, sz, sx, sp
            self.dev_x = 2 * chip_at(z, y, 1 - x) + par
            self.dev_y = 2 * chip_at(z, 1 - y, x) + par

        def blk(self, col, zq):
            return self.buf.at[par, col_chip(col, zq)]

        def along_z(self, zq, to, k):
            b = self.blk(0, zq)
            return remote(b, b, self.sz.at[k, zq], self.rz.at[0, zq, 0], 2 * chip_at(to, y, x) + par)

        def to_x(self, col, zq):
            b = self.blk(col, zq)
            return remote(b, b, self.sx.at[0, zq], self.rz.at[1, zq, 0], self.dev_x)

        def to_y(self, col, zq):
            b = self.blk(col, zq)
            return remote(b, b, self.sx.at[1, zq], self.rz.at[2, zq, 0], self.dev_y)

        def part_y(self, col, zq):
            b = self.blk(col, zq).at[pl.ds(0, self.split)]
            return remote(b, b, self.sx.at[2, zq], self.rz.at[3, zq, 0], self.dev_y)

        def part_x(self, col, zq):
            b = self.blk(col, zq).at[pl.ds(self.split, self.rows - self.split)]
            return remote(b, b, self.sx.at[3, zq], self.rz.at[3, zq, 1], self.dev_x)

        def pair(self, col, zq):
            b = self.blk(col, zq)
            return remote(b, b, self.sp.at[col, zq], self.rp.at[col, zq], partner)

        def own_col(self, zq):
            self.to_x(0, zq).start()
            self.to_y(0, zq).start()
            self.pair(0, zq).start()

        def xy(self, zq):
            self.to_x(1, zq).wait_recv()
            self.part_y(1, zq).start()
            self.pair(1, zq).start()
            self.to_y(2, zq).wait_recv()
            self.part_x(2, zq).start()
            self.pair(2, zq).start()

        def diag(self, zq):
            self.part_y(3, zq).wait_recv()
            self.part_x(3, zq).wait_recv()
            self.pair(3, zq).start()

        def pairs(self, zq):
            for col in range(4):
                self.pair(col, zq).wait_recv()

        def z_sends(self, go):
            if self.chain:
                for zq in range(nz):
                    @pl.when(jnp.logical_and(z >= zq, z + 1 < nz))
                    def _():
                        go(self.along_z(zq, z + 1, 0))

                    @pl.when(jnp.logical_and(z <= zq, z > 0))
                    def _():
                        go(self.along_z(zq, z - 1, 1))
            else:
                for d in range(1, nz):
                    @pl.when(z + d < nz)
                    def _():
                        go(self.along_z(z, z + d, d - 1))

                    @pl.when(z - d >= 0)
                    def _():
                        go(self.along_z(z, z - d, nz - 2 + d))

        def begin(self):
            if self.chain:
                @pl.when(z + 1 < nz)
                def _():
                    self.along_z(z, z + 1, 0).start()

                @pl.when(z > 0)
                def _():
                    self.along_z(z, z - 1, 1).start()
            else:
                self.z_sends(lambda c: c.start())
            self.own_col(z)

        def from_z(self, d):
            @pl.when(z - d >= 0)
            def _():
                self.along_z(z - d, z, 0).wait_recv()
                if self.chain:
                    @pl.when(z + 1 < nz)
                    def _():
                        self.along_z(z - d, z + 1, 0).start()

                self.own_col(z - d)

            @pl.when(z + d < nz)
            def _():
                self.along_z(z + d, z, 1).wait_recv()
                if self.chain:
                    @pl.when(z > 0)
                    def _():
                        self.along_z(z + d, z - 1, 1).start()

                self.own_col(z + d)

        def at(self, d, f):
            if d == 0:
                f(z)
                return

            @pl.when(z - d >= 0)
            def _():
                f(z - d)

            @pl.when(z + d < nz)
            def _():
                f(z + d)

        def steps(self, tag, ready):
            def last(zq):
                self.diag(zq)
                self.pairs(zq)
                ready(zq)

            for d in range(1, nz):
                with scope(f"{tag}z{d}"):
                    self.from_z(d)
                with scope(f"{tag}xy{d - 1}"):
                    self.at(d - 1, self.xy)
                yield
                if d >= 2:
                    with scope(f"{tag}d{d - 2}"):
                        self.at(d - 2, last)
                    yield
            with scope(f"{tag}xy{nz - 1}"):
                self.at(nz - 1, self.xy)
            yield
            for d in range(max(nz - 2, 0), nz):
                with scope(f"{tag}d{d}"):
                    self.at(d, last)
                yield

        def finish(self):
            self.z_sends(lambda c: c.wait_send())
            for zq in range(nz):
                for col in range(4):
                    self.pair(col, zq).wait_send()
                self.to_x(0, zq).wait_send()
                self.to_y(0, zq).wait_send()
                self.part_y(1, zq).wait_send()
                self.part_x(2, zq).wait_send()

    owner_core = lax.rem((chip + 1) // 2, 2)
    q_slot = 2 * (chip // 2) + par

    def sup_chip(s):
        return 2 * s + lax.rem(s + par, 2)

    def q_copy(i):
        head = lax.rem(chip + i, n_chip)
        return q_ref.at[head], q_recv.at[q_slot], q_ss.at[i], q_rs.at[q_slot], 2 * head + owner_core

    def do_copy(i):
        head = lax.rem(chip + i, n_chip)
        return do_ref.at[head], do_recv.at[q_slot], do_ss.at[i], do_rs.at[q_slot], 2 * head + owner_core

    def o_copy(s, i):
        return o_send.at[2 * s + i], o_out.at[chip], o_ss.at[2 * s + i], o_rs.at[chip], 2 * sup_chip(s) + i

    def dq_copy(s, i):
        return dq_send.at[2 * s + i], dq_out.at[chip], dq_ss.at[2 * s + i], dq_rs.at[chip], 2 * sup_chip(s) + i

    def dv_copy(ch):
        return dv_msg.at[par, ch], dv_recv.at[chip], dv_ss.at[ch], dv_rs.at[chip], 2 * ch + par

    def dk_copy(ch):
        return dk_msg.at[par, ch], dk_recv.at[chip], dk_ss.at[ch], dk_rs.at[chip], 2 * ch + par

    gc = Gather(c_all, 144, 80, False, cg_rz, cg_rp, cg_sz, cg_sx, cg_sp)
    with scope("send_c"):
        c_all[par, chip, pl.ds(0, BLK), :] = c_ref[...]
        for i in range(4):
            c_all[par, chip, pl.ds(BLK, 16), pl.ds(128 * i, 128)] = rt_ref[pl.ds(16 * i, 16), :]
        gc.begin()
    with scope("send_q"):
        def send_q(i):
            start(*q_copy(i))
            start(*do_copy(i))

        late = z >= nz // 2

        @pl.when(jnp.logical_not(late))
        def _():
            loop(0, n_chip, send_q)

    with scope("init"):
        dkr[...] = jnp.zeros_like(dkr)
        dv[...] = jnp.zeros_like(dv)
        w_cat[...] = jnp.concatenate([wk_ref[...], wv_ref[...]], axis=1)
        for i, w in enumerate((wk_ref, wv_ref)):
            wt_cat[pl.ds(i * 128, 128), :] = jnp.transpose(w[...].astype(F32)).astype(BF)
        qt[pl.ds(192, 64), :] = jnp.zeros((64, SUP), BF)

    def latent_of(ch):
        return jnp.concatenate([c_all[0, ch, pl.ds(0, BLK), :], c_all[1, ch, pl.ds(0, BLK), :]], axis=0)

    def up_project(ch):
        base = pl.multiple_of(ch * SUP, SUP)
        lat = latent_of(ch)
        kv = mm(lat, w_cat[...]).astype(BF)
        kvt = mm(wt_cat[...], lat, NT).astype(BF)
        kr[pl.ds(base, SUP), pl.ds(0, 128)] = kv[:, :128]
        v[pl.ds(base, SUP), :] = kv[:, 128:]
        kt[pl.ds(0, 128), pl.ds(base, SUP)] = kvt[:128]
        vt[:, pl.ds(base, SUP)] = kvt[128:]
        for q in range(2):
            rt = jnp.concatenate([c_all[q, ch, pl.ds(BLK, 16), pl.ds(128 * i, 128)] for i in range(4)], axis=0)
            kt[pl.ds(128, 64), pl.ds(base + q * BLK, BLK)] = rt
            r = jnp.transpose(rt.astype(F32))
            kr[pl.ds(base + q * BLK, BLK), pl.ds(128, 128)] = jnp.concatenate(
                [r, jnp.zeros_like(r)], axis=1).astype(BF)

    diff = lax.broadcasted_iota(jnp.int32, (SUP, SUP), 0) - lax.broadcasted_iota(jnp.int32, (SUP, SUP), 1)

    def load_q(s):
        for i in range(2):
            qt[pl.ds(0, 192), pl.ds(i * BLK, BLK)] = q_recv[2 * s + i]
            dof[pl.ds(i * BLK, BLK), :] = do_recv[2 * s + i]

    def store_row(s):
        a = s // 2
        return (a + 1) * (a + s % 2) * CH

    def forward(s):
        ch = sup_chip(s)
        for i in range(2):
            arrived(q_recv.at[2 * s + i], q_rs.at[2 * s + i])
            arrived(do_recv.at[2 * s + i], do_rs.at[2 * s + i])
        load_q(s)
        dot_[...] = jnp.transpose(dof[...].astype(F32))
        n_ch = s // 2 + 1

        def score(j, m8):
            for t in range(CH // SUP):
                r0 = pl.multiple_of(j * CH + t * SUP, SUP)
                st = mm(kr[pl.ds(r0, SUP), :], qt[...])
                st = jnp.where(diff <= ch * SUP - r0, st, NEG)
                s_buf[pl.ds(r0, SUP), :] = st
                m8 = jnp.maximum(m8, jnp.max(st.reshape(SUP // 8, 8, SUP), axis=0))
            return m8

        m8 = lax.fori_loop(0, n_ch, score, jnp.full((8, SUP), NEG, F32))
        m2 = jnp.max(m8, axis=0, keepdims=True) * c1
        ot[...] = jnp.zeros_like(ot)

        def values(j, l8):
            base = pl.multiple_of(j * CH, CH)
            for t in range(CH // SUP):
                p = jnp.exp2(s_buf[pl.ds(base + t * SUP, SUP), :] * c1 - m2)
                l8 = l8 + jnp.sum(p.reshape(SUP // 8, 8, SUP), axis=0)
                p_buf[pl.ds(t * SUP, SUP), :] = p.astype(BF)
            ot[...] += mm(vt[:, pl.ds(base, CH)], p_buf[...])
            return l8

        l8 = lax.fori_loop(0, n_ch, values, jnp.zeros((8, SUP), F32))
        l = jnp.sum(l8, axis=0, keepdims=True)
        o = ot[...] / l
        lse2 = m2 + jnp.log2(l)
        delta_s[s] = jnp.sum(o * dot_[...], axis=0, keepdims=True)
        o_rows = jnp.transpose(o)
        for i in range(2):
            o_send[2 * s + i] = o_rows[i * BLK:(i + 1) * BLK].astype(BF)
        for i in range(2):
            start(*o_copy(s, i))
        row0 = store_row(s)

        def values_grad(j):
            base = pl.multiple_of(j * CH, CH)
            for t in range(CH // SUP):
                rows = pl.ds(base + t * SUP, SUP)
                p = jnp.exp2(s_buf[rows, :] * c1 - lse2).astype(BF)
                p_store[pl.ds(pl.multiple_of(row0 + base + t * SUP, SUP), SUP), :] = p
                dv[rows, :] += mm(p, dof[...])

        loop(0, n_ch, values_grad)

    def backward(s):
        load_q(s)
        dqt[...] = jnp.zeros_like(dqt)
        row0 = store_row(s)
        delta = delta_s[s]

        def keys_grad(j):
            base = pl.multiple_of(j * CH, CH)
            for t in range(CH // SUP):
                rows = pl.ds(base + t * SUP, SUP)
                dp = mm(v[rows, :], dof[...], NT)
                p = p_store[pl.ds(pl.multiple_of(row0 + base + t * SUP, SUP), SUP), :].astype(F32)
                ds_buf[pl.ds(t * SUP, SUP), :] = (p * (dp - delta) * scale).astype(BF)
            for t in range(CH // SUP):
                rows = pl.ds(base + t * SUP, SUP)
                dkr[rows, :] += mm(ds_buf[pl.ds(t * SUP, SUP), :], qt[...], NT)
            dqt[...] += mm(kt[:, pl.ds(base, CH)], ds_buf[...])

        loop(0, s // 2 + 1, keys_grad)
        for i in range(2):
            dq_send[2 * s + i] = dqt[:, pl.ds(i * BLK, BLK)].astype(BF)
        for i in range(2):
            start(*dq_copy(s, i))

    def ready_c(zq):
        gc.pairs(zq)
        loop(zq * PLANE, (zq + 1) * PLANE, up_project)

    def col_ready(zq):
        @pl.when(z != zq)
        def _():
            gc.along_z(zq, z, 0).wait_recv()
            gc.own_col(zq)

    def step_c(k):
        if k < nz:
            col_ready(k)
        if 0 <= k - 1 < nz:
            gc.xy(k - 1)
        if 0 <= k - 2 < nz:
            gc.diag(k - 2)
            ready_c(k - 2)

    for k in range(nz + 2):
        with scope(f"c{k}"):
            step_c(k)
            if k < 2:
                @pl.when(late)
                def _():
                    loop(k * n_chip // 2, (k + 1) * n_chip // 2, send_q)

        if k >= 3:
            with scope(f"fwd{k - 3}"):
                loop(2 * (k - 3), 2 * (k - 3) + 2, forward)
    with scope(f"fwd{nz - 1}"):
        loop(2 * (nz - 1), 2 * nz, forward)

    def head_dw(k, lo, hi, grads):
        def add(ch):
            base = pl.multiple_of(ch * SUP, SUP)
            g = jnp.transpose(grads(pl.ds(base, SUP))).astype(BF)
            dwt[k] += mm(g, latent_of(ch))

        loop(lo, hi, add)

    def dw_exchange(k):
        dw_msg[k] = jnp.transpose(dwt[k]).reshape(2, SUP, 128)
        c = remote(dw_msg.at[k, 1 - par], dw_part.at[k], pair_s.at[k], pair_r.at[k], partner)
        c.start()
        return c

    def dw_begin(k, c):
        c.wait_recv()
        dw_all[k, par, chip] = dw_msg[k, par] + dw_part[k]

    def dw_out_copy(k, q, h):
        dst = dwk_out if k == 0 else dwv_out
        return pltpu.make_async_copy(dw_all.at[k, q, h], dst.at[pl.ds(q * SUP, SUP), h, 0], dw_sem.at[k, q, h])

    def put_dw(k):
        def put(zq):
            for q in range(2):
                loop(zq * PLANE, (zq + 1) * PLANE, lambda h: dw_out_copy(k, q, h).start())

        return put

    dwt[...] = jnp.zeros_like(dwt)
    gv = Gather(dw_all.at[1], SUP, 128, False, v_rz, v_rp, v_sz, v_sx, v_sp)
    gk = Gather(dw_all.at[0], SUP, 128, False, k_rz, k_rp, k_sz, k_sx, k_sp)
    with scope("dv"):
        def dv_out(ch):
            for q in range(2):
                dv_msg[q, ch] = dv[pl.ds(pl.multiple_of(ch * SUP, SUP) + q * BLK, BLK), :].astype(BF)

        loop(0, n_chip, dv_out)
        pair_dv = remote(dv_msg.at[1 - par], dv_part, pair_s.at[2], pair_r.at[2], partner)
        pair_dv.start()
        head_dw(1, 0, n_chip, lambda rows: dv[rows, :])
        pair_dwv = dw_exchange(1)
        pair_dv.wait_recv()

        def dv_add(ch):
            dv_msg[par, ch] = (dv_msg[par, ch].astype(F32) + dv_part[ch].astype(F32)).astype(BF)

        loop(0, n_chip, dv_add)
        dw_begin(1, pair_dwv)
        gv.begin()

        def dv_send(i):
            start(*dv_copy(lax.rem(chip + i, n_chip)))

        loop(0, n_chip, dv_send)

    pair_dk = [remote(dk_msg.at[1 - par, pl.ds(PLANE * g, PLANE)], dk_part.at[pl.ds(PLANE * g, PLANE)],
                      pair_s.at[3 + g], pair_r.at[3 + g], partner) for g in range(nz)]

    def dk_out(g):
        def put(ch):
            for q in range(2):
                rows = pl.ds(pl.multiple_of(ch * SUP, SUP) + q * BLK, BLK)
                dk_msg[q, ch, pl.ds(0, BLK), :] = dkr[rows, pl.ds(0, 128)].astype(BF)
                dk_msg[q, ch, pl.ds(BLK, 64), :] = pack_rope(dkr[rows, pl.ds(128, 128)][:, :64]).astype(BF)

        loop(PLANE * g, PLANE * (g + 1), put)
        pair_dk[g].start()
        head_dw(0, PLANE * g, PLANE * (g + 1), lambda rows: dkr[rows, pl.ds(0, 128)])

    def dk_add(g):
        pair_dk[g].wait_recv()

        def put(ch):
            dk_msg[par, ch] = (dk_msg[par, ch].astype(F32) + dk_part[ch].astype(F32)).astype(BF)

        loop(PLANE * g, PLANE * (g + 1), put)

    for g in reversed(range(nz)):
        for s in (2 * g + 1, 2 * g):
            with scope(f"bwd{s}"):
                backward(s)
        if g + 1 < nz:
            with scope(f"dks{g + 1}"):
                dk_add(g + 1)
        with scope(f"dko{g}"):
            dk_out(g)

    with scope("dwk"):
        pair_dwk = dw_exchange(0)
        dw_begin(0, pair_dwk)
        gk.begin()
    with scope("dks0"):
        dk_add(0)
        loop(0, n_chip, lambda i: start(*dk_copy(lax.rem(chip + i, n_chip))))
    dv_steps, dk_steps = gv.steps("v", put_dw(1)), gk.steps("k", put_dw(0))
    next(dv_steps)
    for _ in dv_steps:
        next(dk_steps)
    for _ in dk_steps:
        pass

    with scope("drain"):
        outs = []
        for buf, rs, dst in ((o_out, o_rs, o_hbm), (dq_out, dq_rs, dq_hbm), (dv_recv, dv_rs, dv_hbm),
                             (dk_recv, dk_rs, dk_hbm)):
            loop(0, n_chip, lambda i: arrived(buf.at[i], rs.at[i]))
            outs.append(pltpu.make_async_copy(buf, dst, out_sem.at[len(outs)]))
            outs[-1].start()
        for g in (gc, gv, gk):
            g.finish()
        for c in [pair_dv, pair_dwv, pair_dwk] + pair_dk:
            c.wait_send()

        def drain(i):
            sent(*q_copy(i))
            sent(*do_copy(i))
            sent(*o_copy(i // 2, i % 2))
            sent(*dq_copy(i // 2, i % 2))
            sent(*dv_copy(i))
            sent(*dk_copy(i))
            for k in range(2):
                for q in range(2):
                    dw_out_copy(k, q, i).wait()

        loop(0, n_chip, drain)
        for c in outs:
            c.wait()


def solution(mesh):
    n_dev = mesh.shape["cp"]
    n_chip = n_dev // 2
    nz = n_chip // PLANE
    seq = n_dev * BLK
    seq_spec = P("cp")

    def local_step(queries, latent, key_rope, w_uk, w_uv, d_out):
        head = lax.axis_index("cp") // 2
        wk = lax.dynamic_index_in_dim(w_uk, head, 1, keepdims=False)
        wv = lax.dynamic_index_in_dim(w_uv, head, 1, keepdims=False)
        vm = pl.BlockSpec(memory_space=pltpu.VMEM)
        hbm = pl.BlockSpec(memory_space=pl.ANY)
        dma = pltpu.SemaphoreType.DMA
        gather_sems = [dma((4, nz, 2)), dma((4, nz)), dma((max(2 * nz - 2, 2), nz)), dma((4, nz)), dma((4, nz))]
        o, dq, dv, dk, dwk, dwv = pl.pallas_call(
            functools.partial(kernel, nz, queries.shape[-1]),
            out_shape=(jax.ShapeDtypeStruct((n_chip, BLK, 128), BF),
                       jax.ShapeDtypeStruct((n_chip, 192, BLK), BF),
                       jax.ShapeDtypeStruct((n_chip, BLK, 128), BF),
                       jax.ShapeDtypeStruct((n_chip, 192, 128), BF),
                       jax.ShapeDtypeStruct((512, n_chip, 1, 128), F32),
                       jax.ShapeDtypeStruct((512, n_chip, 1, 128), F32)),
            in_specs=[vm] * 6,
            out_specs=(hbm,) * 6,
            scratch_shapes=[
                pltpu.VMEM((n_chip, BLK, 128), BF),
                pltpu.VMEM((n_chip, 192, BLK), BF),
                pltpu.VMEM((n_chip, BLK, 128), BF),
                pltpu.VMEM((n_chip, 192, 128), BF),
                pltpu.VMEM((512, 256), BF),
                pltpu.VMEM((256, 512), BF),
                pltpu.VMEM((n_chip, 192, BLK), BF),
                pltpu.VMEM((n_chip, BLK, 128), BF),
                pltpu.VMEM((2, n_chip, 144, 512), BF),
                pltpu.VMEM((seq, 256), BF),
                pltpu.VMEM((seq, 128), BF),
                pltpu.VMEM((192, seq), BF),
                pltpu.VMEM((128, seq), BF),
                pltpu.VMEM((seq, SUP), F32),
                pltpu.VMEM((CH, SUP), BF),
                pltpu.VMEM((nz * (nz + 1) * CH, SUP), BF),
                pltpu.VMEM((CH, SUP), BF),
                pltpu.VMEM((seq, 256), F32),
                pltpu.VMEM((seq, 128), F32),
                pltpu.VMEM((256, SUP), BF),
                pltpu.VMEM((SUP, 128), BF),
                pltpu.VMEM((128, SUP), F32),
                pltpu.VMEM((128, SUP), F32),
                pltpu.VMEM((192, SUP), F32),
                pltpu.VMEM((8, SUP), F32),
                pltpu.VMEM((n_chip // 2, 1, SUP), F32),
                pltpu.VMEM((n_chip, BLK, 128), BF),
                pltpu.VMEM((n_chip, 192, BLK), BF),
                pltpu.VMEM((2, n_chip, BLK, 128), BF),
                pltpu.VMEM((n_chip, BLK, 128), BF),
                pltpu.VMEM((2, n_chip, 192, 128), BF),
                pltpu.VMEM((n_chip, 192, 128), BF),
                pltpu.VMEM((2, 128, 512), F32),
                pltpu.VMEM((2, 2, SUP, 128), F32),
                pltpu.VMEM((2, SUP, 128), F32),
                pltpu.VMEM((2, 2, n_chip, SUP, 128), F32),
            ] + [dma((n_chip,))] * 12 + [dma((3 + nz,)), dma((3 + nz,)), dma((2, 2, n_chip)), dma((4,))] + gather_sems * 3,
            compiler_params=pltpu.CompilerParams(
                collective_id=0, has_side_effects=True, vmem_limit_bytes=62 * 1024 * 1024),
        )(queries.transpose(1, 2, 0), d_out.transpose(1, 0, 2), latent, key_rope.T, wk, wv)
        d_latent = (jnp.einsum("htd,lhd->tl", dk[:, :BLK], w_uk, preferred_element_type=F32)
                    + jnp.einsum("htd,lhd->tl", dv, w_uv, preferred_element_type=F32)).astype(BF)
        dr = jnp.sum(dk[:, BLK:].astype(F32), axis=0)
        d_key_rope = jnp.concatenate([dr[:, :64], dr[:, 64:]], axis=0).astype(BF)
        return (o.transpose(1, 0, 2), dq.transpose(2, 0, 1), d_latent, d_key_rope,
                dwk.reshape(512, n_chip, 128), dwv.reshape(512, n_chip, 128))

    return jax.shard_map(local_step, mesh=mesh,
                         in_specs=(seq_spec, seq_spec, seq_spec, P(), P(), seq_spec),
                         out_specs=(seq_spec, seq_spec, seq_spec, seq_spec, P(), P()),
                         check_vma=False)
```

```python
import functools
import math

import jax
import jax.numpy as jnp
from jax import lax
from jax.experimental import pallas as pl
from jax.experimental.pallas import tpu as pltpu
from jax.sharding import PartitionSpec as P

MESH = pl.DeviceIdType.MESH
NX, NY = 2, 2
PLANE = NX * NY
BLK = 128
SUP = 256
CH = SUP * PLANE
NEG = -1e30
NT = (((1,), (1,)), ((), ()))
NN = (((1,), (0,)), ((), ()))
BF, F32 = jnp.bfloat16, jnp.float32


def mm(a, b, dims=NN):
    return lax.dot_general(a, b, dims, preferred_element_type=F32)


def pack_rope(x):
    return jnp.concatenate([x[:64], x[64:]], axis=1)


def kernel(nz, qk_dim, q_ref, do_ref, c_ref, rt_ref, wk_ref, wv_ref,
           o_hbm, dq_hbm, dv_hbm, dk_hbm, dwk_out, dwv_out,
           o_out, dq_out, dv_recv, dk_recv,
           w_cat, wt_cat, q_recv, do_recv, c_all, kr, v, kt, vt, s_buf, p_buf, p_store, ds_buf, dkr, dv,
           qt, dof, dot_, ot, dqt, lse, delta_s, o_send, dq_send, dv_msg, dv_part, dk_msg, dk_part,
           dwt, dw_msg, dw_part, dw_all,
           msg_ss, msg_rs, q_rs, do_rs, pair_s, pair_r, dw_sem, out_sem,
           cg_rz, cg_rp, cg_ss, v_rz, v_rp, v_ss, k_rz, k_rp, k_ss):
    n_chip = PLANE * nz
    n_dev = 2 * n_chip
    n_sup = n_chip // 2
    me = lax.axis_index("cp")
    chip, par = me // 2, me % 2
    partner = 2 * chip + (1 - par)
    x, y, z = chip % NX, (chip // NX) % NY, chip // PLANE
    scale = 1.0 / math.sqrt(qk_dim)
    c1 = scale * math.log2(math.e)
    scope = jax.named_scope

    def chip_at(zq, yq, xq):
        return (zq * NY + yq) * NX + xq

    def col_chip(col, zq):
        return chip_at(zq, 1 - y if col >= 2 else y, 1 - x if col % 2 else x)

    def remote(src, dst, ssem, rsem, dev):
        return pltpu.make_async_remote_copy(src_ref=src, dst_ref=dst, send_sem=ssem, recv_sem=rsem,
                                            device_id=(dev,), device_id_type=MESH)

    def start(src, dst, ssem, rsem, dev):
        @pl.when(dev == me)
        def _():
            pltpu.make_async_copy(src, dst, rsem).start()

        @pl.when(dev != me)
        def _():
            remote(src, dst, ssem, rsem, dev).start()

    def arrived(dst, rsem):
        pltpu.make_async_copy(dst, dst, rsem).wait()

    def loop(lo, hi, f):
        def body(i, carry):
            f(i)
            return carry

        lax.fori_loop(lo, hi, body, 0)

    with scope("barrier"):
        barrier = pltpu.get_barrier_semaphore()
        loop(1, n_dev, lambda i: pl.semaphore_signal(
            barrier, inc=1, device_id=(lax.rem(me + i, n_dev),), device_id_type=MESH))
        pl.semaphore_wait(barrier, n_dev - 1)

    class Gather:
        def __init__(self, buf, rows, split, rz, rp, ss):
            self.buf, self.rows, self.split = buf, rows, split
            self.rz, self.rp, self.ss = rz, rp, ss
            self.dev_x = 2 * chip_at(z, y, 1 - x) + par
            self.dev_y = 2 * chip_at(z, 1 - y, x) + par

        def blk(self, col, zq):
            return self.buf.at[par, col_chip(col, zq)]

        def along_z(self, zq, to):
            b = self.blk(0, zq)
            return remote(b, b, self.ss.at[0], self.rz.at[0, zq], 2 * chip_at(to, y, x) + par)

        def to_x(self, col, zq):
            b = self.blk(col, zq)
            return remote(b, b, self.ss.at[0], self.rz.at[1, zq], self.dev_x)

        def to_y(self, col, zq):
            b = self.blk(col, zq)
            return remote(b, b, self.ss.at[0], self.rz.at[2, zq], self.dev_y)

        def part_y(self, col, zq):
            b = self.blk(col, zq).at[pl.ds(0, self.split)]
            return remote(b, b, self.ss.at[0], self.rz.at[3, zq], self.dev_y)

        def part_x(self, col, zq):
            b = self.blk(col, zq).at[pl.ds(self.split, self.rows - self.split)]
            return remote(b, b, self.ss.at[0], self.rz.at[3, zq], self.dev_x)

        def pair(self, col, zq):
            b = self.blk(col, zq)
            return remote(b, b, self.ss.at[1], self.rp.at[zq], partner)

        def own_col(self, zq):
            self.to_x(0, zq).start()
            self.to_y(0, zq).start()
            self.pair(0, zq).start()

        def xy(self, zq):
            self.to_x(1, zq).wait_recv()
            self.part_y(1, zq).start()
            self.pair(1, zq).start()
            self.to_y(2, zq).wait_recv()
            self.part_x(2, zq).start()
            self.pair(2, zq).start()

        def diag(self, zq):
            arrived(self.blk(3, zq), self.rz.at[3, zq])
            self.pair(3, zq).start()

        def pairs(self, zq):
            arrived(self.buf.at[1 - par, pl.ds(zq * PLANE, PLANE)], self.rp.at[zq])

        def begin(self):
            for d in range(1, nz):
                @pl.when(z + d < nz)
                def _():
                    self.along_z(z, z + d).start()

                @pl.when(z - d >= 0)
                def _():
                    self.along_z(z, z - d).start()

            self.own_col(z)

        def from_z(self, zq):
            self.along_z(zq, z).wait_recv()
            self.own_col(zq)

        def at(self, d, f):
            if d == 0:
                f(z)
                return

            @pl.when(z - d >= 0)
            def _():
                f(z - d)

            @pl.when(z + d < nz)
            def _():
                f(z + d)

        def steps(self, tag, ready):
            def last(zq):
                self.diag(zq)
                self.pairs(zq)
                ready(zq)

            for d in range(1, nz):
                with scope(f"{tag}z{d}"):
                    self.at(d, self.from_z)
                with scope(f"{tag}xy{d - 1}"):
                    self.at(d - 1, self.xy)
                if d >= 2:
                    with scope(f"{tag}d{d - 2}"):
                        self.at(d - 2, last)
            with scope(f"{tag}xy{nz - 1}"):
                self.at(nz - 1, self.xy)
            for d in range(max(nz - 2, 0), nz):
                with scope(f"{tag}d{d}"):
                    self.at(d, last)

        def finish(self):
            arrived(self.buf.at[0, pl.ds(0, n_chip - 1)], self.ss.at[0])
            arrived(self.buf.at[0], self.ss.at[1])

    owner_core = lax.rem((chip + 1) // 2, 2)
    q_slot = 2 * (chip // 2) + par

    def sup_chip(s):
        return 2 * s + lax.rem(s + par, 2)

    def q_copy(i):
        head = lax.rem(chip + i, n_chip)
        return q_ref.at[head], q_recv.at[q_slot], msg_ss.at[0], q_rs.at[q_slot // 2], 2 * head + owner_core

    def do_copy(i):
        head = lax.rem(chip + i, n_chip)
        return do_ref.at[head], do_recv.at[q_slot], msg_ss.at[1], do_rs.at[q_slot // 2], 2 * head + owner_core

    def o_copy(s, i):
        return o_send.at[2 * s + i], o_out.at[chip], msg_ss.at[2], msg_rs.at[0], 2 * sup_chip(s) + i

    def dq_copy(s, i):
        return dq_send.at[2 * s + i], dq_out.at[chip], msg_ss.at[3], msg_rs.at[1], 2 * sup_chip(s) + i

    def dv_copy(ch):
        return dv_msg.at[par, ch], dv_recv.at[chip], msg_ss.at[4], msg_rs.at[2], 2 * ch + par

    def dk_copy(ch):
        return dk_msg.at[par, ch], dk_recv.at[chip], msg_ss.at[5], msg_rs.at[3], 2 * ch + par

    gc = Gather(c_all, 144, 80, cg_rz, cg_rp, cg_ss)
    with scope("send_c"):
        c_all[par, chip, pl.ds(0, BLK), :] = c_ref[...]
        for i in range(4):
            c_all[par, chip, pl.ds(BLK, 16), pl.ds(128 * i, 128)] = rt_ref[pl.ds(16 * i, 16), :]
        gc.begin()
    with scope("send_q"):
        def send_q(i):
            start(*q_copy(i))
            start(*do_copy(i))

        late = z >= nz // 2

        @pl.when(jnp.logical_not(late))
        def _():
            loop(0, n_chip, send_q)

    with scope("init"):
        dkr[...] = jnp.zeros_like(dkr)
        dv[...] = jnp.zeros_like(dv)
        w_cat[...] = jnp.concatenate([wk_ref[...], wv_ref[...]], axis=1)
        for i, w in enumerate((wk_ref, wv_ref)):
            wt_cat[pl.ds(i * 128, 128), :] = jnp.transpose(w[...].astype(F32)).astype(BF)
        qt[pl.ds(192, 64), :] = jnp.zeros((64, SUP), BF)

    def latent_of(ch):
        return jnp.concatenate([c_all[0, ch, pl.ds(0, BLK), :], c_all[1, ch, pl.ds(0, BLK), :]], axis=0)

    def up_project(ch):
        base = pl.multiple_of(ch * SUP, SUP)
        lat = latent_of(ch)
        kv = mm(lat, w_cat[...]).astype(BF)
        kvt = mm(wt_cat[...], lat, NT).astype(BF)
        kr[pl.ds(base, SUP), pl.ds(0, 128)] = kv[:, :128]
        v[pl.ds(base, SUP), :] = kv[:, 128:]
        kt[pl.ds(0, 128), pl.ds(base, SUP)] = kvt[:128]
        vt[:, pl.ds(base, SUP)] = kvt[128:]
        for q in range(2):
            rt = jnp.concatenate([c_all[q, ch, pl.ds(BLK, 16), pl.ds(128 * i, 128)] for i in range(4)], axis=0)
            kt[pl.ds(128, 64), pl.ds(base + q * BLK, BLK)] = rt
            r = jnp.transpose(rt.astype(F32))
            kr[pl.ds(base + q * BLK, BLK), pl.ds(128, 128)] = jnp.concatenate(
                [r, jnp.zeros_like(r)], axis=1).astype(BF)

    diff = lax.broadcasted_iota(jnp.int32, (SUP, SUP), 0) - lax.broadcasted_iota(jnp.int32, (SUP, SUP), 1)

    def load_q(s):
        for i in range(2):
            qt[pl.ds(0, 192), pl.ds(i * BLK, BLK)] = q_recv[2 * s + i]
            dof[pl.ds(i * BLK, BLK), :] = do_recv[2 * s + i]

    def store_row(s):
        a = s // 2
        return (a + 1) * (a + s % 2) * CH

    def forward(s):
        ch = sup_chip(s)
        arrived(q_recv.at[pl.ds(2 * s, 2)], q_rs.at[s])
        arrived(do_recv.at[pl.ds(2 * s, 2)], do_rs.at[s])
        load_q(s)
        dot_[...] = jnp.transpose(dof[...].astype(F32))
        n_ch = s // 2 + 1

        def score(j, m8):
            for t in range(CH // SUP):
                r0 = pl.multiple_of(j * CH + t * SUP, SUP)
                st = mm(kr[pl.ds(r0, SUP), :], qt[...])
                st = jnp.where(diff <= ch * SUP - r0, st, NEG)
                s_buf[pl.ds(r0, SUP), :] = st
                m8 = jnp.maximum(m8, jnp.max(st.reshape(SUP // 8, 8, SUP), axis=0))
            return m8

        m8 = lax.fori_loop(0, n_ch, score, jnp.full((8, SUP), NEG, F32))
        m2 = jnp.max(m8, axis=0, keepdims=True) * c1
        ot[...] = jnp.zeros_like(ot)

        def values(j, l8):
            base = pl.multiple_of(j * CH, CH)
            for t in range(CH // SUP):
                p = jnp.exp2(s_buf[pl.ds(base + t * SUP, SUP), :] * c1 - m2)
                l8 = l8 + jnp.sum(p.reshape(SUP // 8, 8, SUP), axis=0)
                p_buf[pl.ds(t * SUP, SUP), :] = p.astype(BF)
            ot[...] += mm(vt[:, pl.ds(base, CH)], p_buf[...])
            return l8

        l8 = lax.fori_loop(0, n_ch, values, jnp.zeros((8, SUP), F32))
        l = jnp.sum(l8, axis=0, keepdims=True)
        o = ot[...] / l
        lse2 = m2 + jnp.log2(l)
        delta_s[s] = jnp.sum(o * dot_[...], axis=0, keepdims=True)
        o_rows = jnp.transpose(o)
        for i in range(2):
            o_send[2 * s + i] = o_rows[i * BLK:(i + 1) * BLK].astype(BF)
        for i in range(2):
            start(*o_copy(s, i))
        row0 = store_row(s)

        def values_grad(j):
            base = pl.multiple_of(j * CH, CH)
            for t in range(CH // SUP):
                rows = pl.ds(base + t * SUP, SUP)
                p = jnp.exp2(s_buf[rows, :] * c1 - lse2).astype(BF)
                p_store[pl.ds(pl.multiple_of(row0 + base + t * SUP, SUP), SUP), :] = p
                dv[rows, :] += mm(p, dof[...])

        loop(0, n_ch, values_grad)

    def backward(s):
        load_q(s)
        dqt[...] = jnp.zeros_like(dqt)
        row0 = store_row(s)
        delta = delta_s[s]

        def keys_grad(j):
            base = pl.multiple_of(j * CH, CH)
            for t in range(CH // SUP):
                rows = pl.ds(base + t * SUP, SUP)
                dp = mm(v[rows, :], dof[...], NT)
                p = p_store[pl.ds(pl.multiple_of(row0 + base + t * SUP, SUP), SUP), :].astype(F32)
                ds_buf[pl.ds(t * SUP, SUP), :] = (p * (dp - delta) * scale).astype(BF)
            for t in range(CH // SUP):
                rows = pl.ds(base + t * SUP, SUP)
                dkr[rows, :] += mm(ds_buf[pl.ds(t * SUP, SUP), :], qt[...], NT)
            dqt[...] += mm(kt[:, pl.ds(base, CH)], ds_buf[...])

        loop(0, s // 2 + 1, keys_grad)
        for i in range(2):
            dq_send[2 * s + i] = dqt[:, pl.ds(i * BLK, BLK)].astype(BF)
        for i in range(2):
            start(*dq_copy(s, i))

    def ready_c(zq):
        gc.pairs(zq)
        loop(zq * PLANE, (zq + 1) * PLANE, up_project)

    def col_ready(zq):
        @pl.when(z != zq)
        def _():
            gc.from_z(zq)

    def step_c(k):
        if k < nz:
            col_ready(k)
        if 0 <= k - 1 < nz:
            gc.xy(k - 1)
        if 0 <= k - 2 < nz:
            gc.diag(k - 2)
            ready_c(k - 2)

    for k in range(nz + 2):
        with scope(f"c{k}"):
            step_c(k)
            if k < 2:
                @pl.when(late)
                def _():
                    loop(k * n_chip // 2, (k + 1) * n_chip // 2, send_q)

        if k >= 2:
            with scope(f"fwd{k - 2}"):
                loop(2 * (k - 2), 2 * (k - 2) + 2, forward)

    def head_dw(k, lo, hi, grads):
        def add(ch):
            base = pl.multiple_of(ch * SUP, SUP)
            g = jnp.transpose(grads(pl.ds(base, SUP))).astype(BF)
            dwt[k] += mm(g, latent_of(ch))

        loop(lo, hi, add)

    def dw_exchange(k):
        dw_msg[k] = jnp.transpose(dwt[k]).reshape(2, SUP, 128)
        c = remote(dw_msg.at[k, 1 - par], dw_part.at[k], pair_s.at[k], pair_r.at[k], partner)
        c.start()
        return c

    def dw_begin(k, c):
        c.wait_recv()
        dw_all[k, par, chip] = dw_msg[k, par] + dw_part[k]

    def dw_out_copy(k, q, h):
        dst = dwk_out if k == 0 else dwv_out
        return pltpu.make_async_copy(dw_all.at[k, q, h], dst.at[pl.ds(q * SUP, SUP), h, 0], dw_sem.at[k])

    def put_dw(k):
        def put(zq):
            for q in range(2):
                loop(zq * PLANE, (zq + 1) * PLANE, lambda h: dw_out_copy(k, q, h).start())

        return put

    dwt[...] = jnp.zeros_like(dwt)
    gv = Gather(dw_all.at[1], SUP, 128, v_rz, v_rp, v_ss)
    gk = Gather(dw_all.at[0], SUP, 128, k_rz, k_rp, k_ss)
    with scope("dv"):
        def dv_out(ch):
            for q in range(2):
                dv_msg[q, ch] = dv[pl.ds(pl.multiple_of(ch * SUP, SUP) + q * BLK, BLK), :].astype(BF)

        loop(0, n_chip, dv_out)
        pair_dv = remote(dv_msg.at[1 - par], dv_part, pair_s.at[2], pair_r.at[2], partner)
        pair_dv.start()
        head_dw(1, 0, n_chip, lambda rows: dv[rows, :])
        pair_dwv = dw_exchange(1)
        pair_dv.wait_recv()

        def dv_add(ch):
            dv_msg[par, ch] = (dv_msg[par, ch].astype(F32) + dv_part[ch].astype(F32)).astype(BF)

        loop(0, n_chip, dv_add)
        dw_begin(1, pair_dwv)
        gv.begin()

        def dv_send(i):
            start(*dv_copy(lax.rem(chip + i, n_chip)))

        loop(0, n_chip, dv_send)

    pair_dk = [remote(dk_msg.at[1 - par, pl.ds(PLANE * g, PLANE)], dk_part.at[pl.ds(PLANE * g, PLANE)],
                      pair_s.at[3 + g], pair_r.at[3 + g], partner) for g in range(nz)]

    def dk_out(g):
        def put(ch):
            for q in range(2):
                rows = pl.ds(pl.multiple_of(ch * SUP, SUP) + q * BLK, BLK)
                dk_msg[q, ch, pl.ds(0, BLK), :] = dkr[rows, pl.ds(0, 128)].astype(BF)
                dk_msg[q, ch, pl.ds(BLK, 64), :] = pack_rope(dkr[rows, pl.ds(128, 128)][:, :64]).astype(BF)

        loop(PLANE * g, PLANE * (g + 1), put)
        pair_dk[g].start()
        head_dw(0, PLANE * g, PLANE * (g + 1), lambda rows: dkr[rows, pl.ds(0, 128)])

    def dk_add(g):
        pair_dk[g].wait_recv()

        def put(ch):
            dk_msg[par, ch] = (dk_msg[par, ch].astype(F32) + dk_part[ch].astype(F32)).astype(BF)

        loop(PLANE * g, PLANE * (g + 1), put)

    for g in reversed(range(nz)):
        for s in (2 * g + 1, 2 * g):
            with scope(f"bwd{s}"):
                backward(s)
        if g + 1 < nz:
            with scope(f"dks{g + 1}"):
                dk_add(g + 1)
        with scope(f"dko{g}"):
            dk_out(g)

    with scope("dwk"):
        pair_dwk = dw_exchange(0)
        dw_begin(0, pair_dwk)
        gk.begin()
    with scope("dks0"):
        dk_add(0)
        loop(0, n_chip, lambda i: start(*dk_copy(lax.rem(chip + i, n_chip))))
    gv.steps("v", put_dw(1))
    gk.steps("k", put_dw(0))

    with scope("drain"):
        outs = []
        for buf, dst in ((o_out, o_hbm), (dq_out, dq_hbm), (dv_recv, dv_hbm), (dk_recv, dk_hbm)):
            arrived(buf, msg_rs.at[len(outs)])
            outs.append(pltpu.make_async_copy(buf, dst, out_sem.at[len(outs)]))
            outs[-1].start()
        for g in (gc, gv, gk):
            g.finish()
        for c in [pair_dv, pair_dwv, pair_dwk] + pair_dk:
            c.wait_send()
        for k, buf in enumerate((q_recv, do_recv, o_out, dq_out)):
            @pl.when(owner_core == par)
            def _():
                arrived(buf.at[pl.ds(0, n_chip - 1)], msg_ss.at[k])

            @pl.when(owner_core != par)
            def _():
                arrived(buf, msg_ss.at[k])
        for k, buf in enumerate((dv_recv, dk_recv)):
            arrived(buf.at[pl.ds(0, n_chip - 1)], msg_ss.at[4 + k])
        for k in range(2):
            arrived(dw_all.at[k], dw_sem.at[k])
        for c in outs:
            c.wait()


def solution(mesh):
    n_dev = mesh.shape["cp"]
    n_chip = n_dev // 2
    nz = n_chip // PLANE
    seq = n_dev * BLK
    seq_spec = P("cp")

    def local_step(queries, latent, key_rope, w_uk, w_uv, d_out):
        head = lax.axis_index("cp") // 2
        wk = lax.dynamic_index_in_dim(w_uk, head, 1, keepdims=False)
        wv = lax.dynamic_index_in_dim(w_uv, head, 1, keepdims=False)
        vm = pl.BlockSpec(memory_space=pltpu.VMEM)
        hbm = pl.BlockSpec(memory_space=pl.ANY)
        dma = pltpu.SemaphoreType.DMA
        gather_sems = [dma((4, nz)), dma((nz,)), dma((2,))]
        o, dq, dv, dk, dwk, dwv = pl.pallas_call(
            functools.partial(kernel, nz, queries.shape[-1]),
            out_shape=(jax.ShapeDtypeStruct((n_chip, BLK, 128), BF),
                       jax.ShapeDtypeStruct((n_chip, 192, BLK), BF),
                       jax.ShapeDtypeStruct((n_chip, BLK, 128), BF),
                       jax.ShapeDtypeStruct((n_chip, 192, 128), BF),
                       jax.ShapeDtypeStruct((512, n_chip, 1, 128), F32),
                       jax.ShapeDtypeStruct((512, n_chip, 1, 128), F32)),
            in_specs=[vm] * 6,
            out_specs=(hbm,) * 6,
            scratch_shapes=[
                pltpu.VMEM((n_chip, BLK, 128), BF),
                pltpu.VMEM((n_chip, 192, BLK), BF),
                pltpu.VMEM((n_chip, BLK, 128), BF),
                pltpu.VMEM((n_chip, 192, 128), BF),
                pltpu.VMEM((512, 256), BF),
                pltpu.VMEM((256, 512), BF),
                pltpu.VMEM((n_chip, 192, BLK), BF),
                pltpu.VMEM((n_chip, BLK, 128), BF),
                pltpu.VMEM((2, n_chip, 144, 512), BF),
                pltpu.VMEM((seq, 256), BF),
                pltpu.VMEM((seq, 128), BF),
                pltpu.VMEM((192, seq), BF),
                pltpu.VMEM((128, seq), BF),
                pltpu.VMEM((seq, SUP), F32),
                pltpu.VMEM((CH, SUP), BF),
                pltpu.VMEM((nz * (nz + 1) * CH, SUP), BF),
                pltpu.VMEM((CH, SUP), BF),
                pltpu.VMEM((seq, 256), F32),
                pltpu.VMEM((seq, 128), F32),
                pltpu.VMEM((256, SUP), BF),
                pltpu.VMEM((SUP, 128), BF),
                pltpu.VMEM((128, SUP), F32),
                pltpu.VMEM((128, SUP), F32),
                pltpu.VMEM((192, SUP), F32),
                pltpu.VMEM((8, SUP), F32),
                pltpu.VMEM((n_chip // 2, 1, SUP), F32),
                pltpu.VMEM((n_chip, BLK, 128), BF),
                pltpu.VMEM((n_chip, 192, BLK), BF),
                pltpu.VMEM((2, n_chip, BLK, 128), BF),
                pltpu.VMEM((n_chip, BLK, 128), BF),
                pltpu.VMEM((2, n_chip, 192, 128), BF),
                pltpu.VMEM((n_chip, 192, 128), BF),
                pltpu.VMEM((2, 128, 512), F32),
                pltpu.VMEM((2, 2, SUP, 128), F32),
                pltpu.VMEM((2, SUP, 128), F32),
                pltpu.VMEM((2, 2, n_chip, SUP, 128), F32),
            ] + [dma((6,)), dma((4,)), dma((n_chip // 2,)), dma((n_chip // 2,))] + [dma((3 + nz,)), dma((3 + nz,)), dma((2,)), dma((4,))] + gather_sems * 3,
            compiler_params=pltpu.CompilerParams(
                collective_id=0, has_side_effects=True, vmem_limit_bytes=62 * 1024 * 1024),
        )(queries.transpose(1, 2, 0), d_out.transpose(1, 0, 2), latent, key_rope.T, wk, wv)
        d_latent = (jnp.einsum("htd,lhd->tl", dk[:, :BLK], w_uk, preferred_element_type=F32)
                    + jnp.einsum("htd,lhd->tl", dv, w_uv, preferred_element_type=F32)).astype(BF)
        dr = jnp.sum(dk[:, BLK:].astype(F32), axis=0)
        d_key_rope = jnp.concatenate([dr[:, :64], dr[:, 64:]], axis=0).astype(BF)
        return (o.transpose(1, 0, 2), dq.transpose(2, 0, 1), d_latent, d_key_rope,
                dwk.reshape(512, n_chip, 128), dwv.reshape(512, n_chip, 128))

    return jax.shard_map(local_step, mesh=mesh,
                         in_specs=(seq_spec, seq_spec, seq_spec, P(), P(), seq_spec),
                         out_specs=(seq_spec, seq_spec, seq_spec, seq_spec, P(), P()),
                         check_vma=False)
```

```python
import functools
import math

import jax
import jax.numpy as jnp
from jax import lax
from jax.experimental import pallas as pl
from jax.experimental.pallas import tpu as pltpu
from jax.sharding import PartitionSpec as P

MESH = pl.DeviceIdType.MESH
NX, NY = 2, 2
PLANE = NX * NY
BLK = 128
SUP = 256
CH = SUP * PLANE
NEG = -1e30
NT = (((1,), (1,)), ((), ()))
NN = (((1,), (0,)), ((), ()))
BF, F32 = jnp.bfloat16, jnp.float32


def mm(a, b, dims=NN):
    return lax.dot_general(a, b, dims, preferred_element_type=F32)


def pack_rope(x):
    return jnp.concatenate([x[:64], x[64:]], axis=1)


def kernel(nz, qk_dim, q_ref, do_raw, c_ref, rt_ref, wk_hbm, wv_hbm,
           o_hbm, dq_hbm, dc_hbm, dr_hbm, dwk_out, dwv_out,
           o_out, dq_out, dv_recv, dk_recv, o_fin, dc_fin, dr_fin, do_ref,
           w_big, w_stage, wt_cat, q_recv, do_recv, c_all, kr, v, kt, vt, s_buf, p_buf, p_store, ds_buf, dkr, dv,
           qt, dof, dot_, ot, dqt, lse, delta_s, o_send, dq_send, dv_msg, dv_part, dk_msg, dk_part,
           dwt, dw_msg, dw_part, dw_all,
           msg_ss, msg_rs, q_rs, do_rs, pair_s, pair_r, dw_sem, out_sem, w_sem,
           cg_rz, cg_rp, cg_ss, v_rz, v_rp, v_ss, k_rz, k_rp, k_ss):
    n_chip = PLANE * nz
    n_dev = 2 * n_chip
    n_sup = n_chip // 2
    me = lax.axis_index("cp")
    chip, par = me // 2, me % 2
    partner = 2 * chip + (1 - par)
    x, y, z = chip % NX, (chip // NX) % NY, chip // PLANE
    scale = 1.0 / math.sqrt(qk_dim)
    c1 = scale * math.log2(math.e)
    scope = jax.named_scope

    def chip_at(zq, yq, xq):
        return (zq * NY + yq) * NX + xq

    def col_chip(col, zq):
        return chip_at(zq, 1 - y if col >= 2 else y, 1 - x if col % 2 else x)

    def remote(src, dst, ssem, rsem, dev):
        return pltpu.make_async_remote_copy(src_ref=src, dst_ref=dst, send_sem=ssem, recv_sem=rsem,
                                            device_id=(dev,), device_id_type=MESH)

    def start(src, dst, ssem, rsem, dev):
        @pl.when(dev == me)
        def _():
            pltpu.make_async_copy(src, dst, rsem).start()

        @pl.when(dev != me)
        def _():
            remote(src, dst, ssem, rsem, dev).start()

    def arrived(dst, rsem):
        pltpu.make_async_copy(dst, dst, rsem).wait()

    def loop(lo, hi, f):
        def body(i, carry):
            f(i)
            return carry

        lax.fori_loop(lo, hi, body, 0)

    n_piece = 8

    def w_copy(i):
        src = wk_hbm if i < n_piece // 2 else wv_hbm
        return pltpu.make_async_copy(src.at[pl.ds(i % (n_piece // 2) * BLK, BLK)], w_stage.at[i % 2], w_sem.at[i % 2])

    for i in range(2):
        w_copy(i).start()

    def heads_first(x):
        return jnp.transpose(x, (1, 0, 2))

    with scope("barrier"):
        barrier = pltpu.get_barrier_semaphore()
        loop(1, n_dev, lambda i: pl.semaphore_signal(
            barrier, inc=1, device_id=(lax.rem(me + i, n_dev),), device_id_type=MESH))
        pl.semaphore_wait(barrier, n_dev - 1)

    class Gather:
        def __init__(self, buf, rows, split, rz, rp, ss, ready):
            self.buf, self.rows, self.split = buf, rows, split
            self.rz, self.rp, self.ss, self.ready = rz, rp, ss, ready
            self.dev_x = 2 * chip_at(z, y, 1 - x) + par
            self.dev_y = 2 * chip_at(z, 1 - y, x) + par

        def blk(self, col, zq):
            return self.buf.at[par, col_chip(col, zq)]

        def along_z(self, zq, to):
            b = self.blk(0, zq)
            return remote(b, b, self.ss.at[0], self.rz.at[0, zq], 2 * chip_at(to, y, x) + par)

        def to_x(self, col, zq):
            b = self.blk(col, zq)
            return remote(b, b, self.ss.at[0], self.rz.at[1, zq], self.dev_x)

        def to_y(self, col, zq):
            b = self.blk(col, zq)
            return remote(b, b, self.ss.at[0], self.rz.at[2, zq], self.dev_y)

        def part_y(self, col, zq):
            b = self.blk(col, zq).at[pl.ds(0, self.split)]
            return remote(b, b, self.ss.at[0], self.rz.at[3, zq], self.dev_y)

        def part_x(self, col, zq):
            b = self.blk(col, zq).at[pl.ds(self.split, self.rows - self.split)]
            return remote(b, b, self.ss.at[0], self.rz.at[3, zq], self.dev_x)

        def pair(self, col, zq):
            b = self.blk(col, zq)
            return remote(b, b, self.ss.at[1], self.rp.at[zq], partner)

        def own_col(self, zq):
            self.to_x(0, zq).start()
            self.to_y(0, zq).start()
            self.pair(0, zq).start()

        def xy(self, zq):
            self.to_x(1, zq).wait_recv()
            self.part_y(1, zq).start()
            self.pair(1, zq).start()
            self.to_y(2, zq).wait_recv()
            self.part_x(2, zq).start()
            self.pair(2, zq).start()

        def diag(self, zq):
            arrived(self.blk(3, zq), self.rz.at[3, zq])
            self.pair(3, zq).start()

        def pairs(self, zq):
            arrived(self.buf.at[1 - par, pl.ds(zq * PLANE, PLANE)], self.rp.at[zq])

        def begin(self):
            for d in range(1, nz):
                @pl.when(z + d < nz)
                def _():
                    self.along_z(z, z + d).start()

                @pl.when(z - d >= 0)
                def _():
                    self.along_z(z, z - d).start()

            self.own_col(z)

        def from_z(self, zq):
            self.along_z(zq, z).wait_recv()
            self.own_col(zq)

        def at(self, d, f):
            if d == 0:
                f(z)
                return

            @pl.when(z - d >= 0)
            def _():
                f(z - d)

            @pl.when(z + d < nz)
            def _():
                f(z + d)

        def last(self, zq):
            self.diag(zq)
            self.pairs(zq)
            self.ready(zq)

        def steps(self, tag, before_last):
            for d in range(1, nz):
                with scope(f"{tag}z{d}"):
                    self.at(d, self.from_z)
                with scope(f"{tag}xy{d - 1}"):
                    self.at(d - 1, self.xy)
                if d >= 2:
                    with scope(f"{tag}d{d - 2}"):
                        self.at(d - 2, self.last)
            with scope(f"{tag}xy{nz - 1}"):
                self.at(nz - 1, self.xy)
            for d in range(max(nz - 2, 0), nz):
                if d == nz - 1:
                    before_last()
                with scope(f"{tag}d{d}"):
                    self.at(d, self.last)

        def finish(self):
            arrived(self.buf.at[0, pl.ds(0, n_chip - 1)], self.ss.at[0])
            arrived(self.buf.at[0], self.ss.at[1])

    owner_core = lax.rem((chip + 1) // 2, 2)
    q_slot = 2 * (chip // 2) + par

    def sup_chip(s):
        return 2 * s + lax.rem(s + par, 2)

    def q_copy(i):
        head = lax.rem(chip + i, n_chip)
        return q_ref.at[head], q_recv.at[q_slot], msg_ss.at[0], q_rs.at[q_slot // 2], 2 * head + owner_core

    def do_copy(i):
        head = lax.rem(chip + i, n_chip)
        return do_ref.at[head], do_recv.at[q_slot], msg_ss.at[1], do_rs.at[q_slot // 2], 2 * head + owner_core

    def o_copy(s, i):
        return o_send.at[2 * s + i], o_out.at[chip], msg_ss.at[2], msg_rs.at[0], 2 * sup_chip(s) + i

    def dq_copy(s, i):
        return dq_send.at[2 * s + i], dq_out.at[chip], msg_ss.at[3], msg_rs.at[1], 2 * sup_chip(s) + i

    def dv_copy(ch):
        return dv_msg.at[par, ch], dv_recv.at[chip], msg_ss.at[4], msg_rs.at[2], 2 * ch + par

    def dk_copy(ch):
        return dk_msg.at[par, ch], dk_recv.at[chip], msg_ss.at[5], msg_rs.at[3], 2 * ch + par

    gc = Gather(c_all, 144, 80, cg_rz, cg_rp, cg_ss, None)
    with scope("send_c"):
        c_all[par, chip, pl.ds(0, BLK), :] = c_ref[...]
        for i in range(4):
            c_all[par, chip, pl.ds(BLK, 16), pl.ds(128 * i, 128)] = rt_ref[pl.ds(16 * i, 16), :]
        gc.begin()
    with scope("send_q"):
        def send_q(i):
            start(*q_copy(i))
            start(*do_copy(i))

        late = z >= nz // 2

        def lay_do(i):
            rows = pl.ds(pl.multiple_of(i * 32, 32), 32)
            do_ref[:, rows, :] = heads_first(do_raw[rows])

        loop(0, BLK // 32, lay_do)

        @pl.when(jnp.logical_not(late))
        def _():
            loop(0, n_chip, send_q)

    with scope("init"):
        dkr[...] = jnp.zeros_like(dkr)
        dv[...] = jnp.zeros_like(dv)
        for i in range(n_piece):
            w_copy(i).wait()

            def lay_w(r):
                w = heads_first(w_stage[i % 2, pl.ds(pl.multiple_of(r * 32, 32), 32)])
                rows = pl.ds(pl.multiple_of(i % (n_piece // 2) * BLK + r * 32, 32), 32)
                for h in range(n_chip):
                    w_big[rows, pl.ds(h * 256 + 128 * (i // (n_piece // 2)), 128)] = w[h]

            loop(0, BLK // 32, lay_w)
            if i + 2 < n_piece:
                w_copy(i + 2).start()
        wt_cat[...] = jnp.transpose(w_big[:, pl.ds(pl.multiple_of(chip * 256, 256), 256)].astype(F32)).astype(BF)
        qt[pl.ds(192, 64), :] = jnp.zeros((64, SUP), BF)

    def latent_of(ch):
        return jnp.concatenate([c_all[0, ch, pl.ds(0, BLK), :], c_all[1, ch, pl.ds(0, BLK), :]], axis=0)

    def up_project(ch):
        base = pl.multiple_of(ch * SUP, SUP)
        lat = latent_of(ch)
        kv = mm(lat, w_big[:, pl.ds(pl.multiple_of(chip * 256, 256), 256)]).astype(BF)
        kvt = mm(wt_cat[...], lat, NT).astype(BF)
        kr[pl.ds(base, SUP), pl.ds(0, 128)] = kv[:, :128]
        v[pl.ds(base, SUP), :] = kv[:, 128:]
        kt[pl.ds(0, 128), pl.ds(base, SUP)] = kvt[:128]
        vt[:, pl.ds(base, SUP)] = kvt[128:]
        for q in range(2):
            rt = jnp.concatenate([c_all[q, ch, pl.ds(BLK, 16), pl.ds(128 * i, 128)] for i in range(4)], axis=0)
            kt[pl.ds(128, 64), pl.ds(base + q * BLK, BLK)] = rt
            r = jnp.transpose(rt.astype(F32))
            kr[pl.ds(base + q * BLK, BLK), pl.ds(128, 128)] = jnp.concatenate(
                [r, jnp.zeros_like(r)], axis=1).astype(BF)

    diff = lax.broadcasted_iota(jnp.int32, (SUP, SUP), 0) - lax.broadcasted_iota(jnp.int32, (SUP, SUP), 1)

    def load_q(s):
        for i in range(2):
            qt[pl.ds(0, 192), pl.ds(i * BLK, BLK)] = q_recv[2 * s + i]
            dof[pl.ds(i * BLK, BLK), :] = do_recv[2 * s + i]

    def store_row(s):
        a = s // 2
        return (a + 1) * (a + s % 2) * CH

    def forward(s):
        ch = sup_chip(s)
        arrived(q_recv.at[pl.ds(2 * s, 2)], q_rs.at[s])
        arrived(do_recv.at[pl.ds(2 * s, 2)], do_rs.at[s])
        load_q(s)
        dot_[...] = jnp.transpose(dof[...].astype(F32))
        n_ch = s // 2 + 1

        def score(j, m8):
            for t in range(CH // SUP):
                r0 = pl.multiple_of(j * CH + t * SUP, SUP)
                st = mm(kr[pl.ds(r0, SUP), :], qt[...])
                st = jnp.where(diff <= ch * SUP - r0, st, NEG)
                s_buf[pl.ds(r0, SUP), :] = st
                m8 = jnp.maximum(m8, jnp.max(st.reshape(SUP // 8, 8, SUP), axis=0))
            return m8

        m8 = lax.fori_loop(0, n_ch, score, jnp.full((8, SUP), NEG, F32))
        m2 = jnp.max(m8, axis=0, keepdims=True) * c1
        ot[...] = jnp.zeros_like(ot)

        def values(j, l8):
            base = pl.multiple_of(j * CH, CH)
            for t in range(CH // SUP):
                p = jnp.exp2(s_buf[pl.ds(base + t * SUP, SUP), :] * c1 - m2)
                l8 = l8 + jnp.sum(p.reshape(SUP // 8, 8, SUP), axis=0)
                p_buf[pl.ds(t * SUP, SUP), :] = p.astype(BF)
            ot[...] += mm(vt[:, pl.ds(base, CH)], p_buf[...])
            return l8

        l8 = lax.fori_loop(0, n_ch, values, jnp.zeros((8, SUP), F32))
        l = jnp.sum(l8, axis=0, keepdims=True)
        o = ot[...] / l
        lse2 = m2 + jnp.log2(l)
        delta_s[s] = jnp.sum(o * dot_[...], axis=0, keepdims=True)
        o_rows = jnp.transpose(o)
        for i in range(2):
            o_send[2 * s + i] = o_rows[i * BLK:(i + 1) * BLK].astype(BF)
        for i in range(2):
            start(*o_copy(s, i))
        row0 = store_row(s)

        def values_grad(j):
            base = pl.multiple_of(j * CH, CH)
            for t in range(CH // SUP):
                rows = pl.ds(base + t * SUP, SUP)
                p = jnp.exp2(s_buf[rows, :] * c1 - lse2).astype(BF)
                p_store[pl.ds(pl.multiple_of(row0 + base + t * SUP, SUP), SUP), :] = p
                dv[rows, :] += mm(p, dof[...])

        loop(0, n_ch, values_grad)

    def backward(s):
        load_q(s)
        dqt[...] = jnp.zeros_like(dqt)
        row0 = store_row(s)
        delta = delta_s[s]

        def keys_grad(j):
            base = pl.multiple_of(j * CH, CH)
            for t in range(CH // SUP):
                rows = pl.ds(base + t * SUP, SUP)
                dp = mm(v[rows, :], dof[...], NT)
                p = p_store[pl.ds(pl.multiple_of(row0 + base + t * SUP, SUP), SUP), :].astype(F32)
                ds_buf[pl.ds(t * SUP, SUP), :] = (p * (dp - delta) * scale).astype(BF)
            for t in range(CH // SUP):
                rows = pl.ds(base + t * SUP, SUP)
                dkr[rows, :] += mm(ds_buf[pl.ds(t * SUP, SUP), :], qt[...], NT)
            dqt[...] += mm(kt[:, pl.ds(base, CH)], ds_buf[...])

        loop(0, s // 2 + 1, keys_grad)
        for i in range(2):
            dq_send[2 * s + i] = dqt[:, pl.ds(i * BLK, BLK)].astype(BF)
        for i in range(2):
            start(*dq_copy(s, i))

    def ready_c(zq):
        gc.pairs(zq)
        loop(zq * PLANE, (zq + 1) * PLANE, up_project)

    def col_ready(zq):
        @pl.when(z != zq)
        def _():
            gc.from_z(zq)

    def step_c(k):
        if k < nz:
            col_ready(k)
        if 0 <= k - 1 < nz:
            gc.xy(k - 1)
        if 0 <= k - 2 < nz:
            gc.diag(k - 2)
            ready_c(k - 2)

    for k in range(nz + 2):
        with scope(f"c{k}"):
            step_c(k)
            if k < 2:
                @pl.when(late)
                def _():
                    loop(k * n_chip // 2, (k + 1) * n_chip // 2, send_q)

        if k >= 2:
            with scope(f"fwd{k - 2}"):
                loop(2 * (k - 2), 2 * (k - 2) + 2, forward)

    def head_dw(k, lo, hi, grads):
        def add(ch):
            base = pl.multiple_of(ch * SUP, SUP)
            g = jnp.transpose(grads(pl.ds(base, SUP))).astype(BF)
            dwt[k] += mm(g, latent_of(ch))

        loop(lo, hi, add)

    def dw_exchange(k):
        dw_msg[k] = jnp.transpose(dwt[k]).reshape(2, SUP, 128)
        c = remote(dw_msg.at[k, 1 - par], dw_part.at[k], pair_s.at[k], pair_r.at[k], partner)
        c.start()
        return c

    def dw_begin(k, c):
        c.wait_recv()
        dw_all[k, par, chip] = dw_msg[k, par] + dw_part[k]

    def dw_out_copy(k, q, h):
        dst = dwk_out if k == 0 else dwv_out
        return pltpu.make_async_copy(dw_all.at[k, q, h], dst.at[pl.ds(q * SUP, SUP), h, 0], dw_sem.at[k])

    def put_dw(k):
        def put(zq):
            for q in range(2):
                loop(zq * PLANE, (zq + 1) * PLANE, lambda h: dw_out_copy(k, q, h).start())

        return put

    dwt[...] = jnp.zeros_like(dwt)
    gv = Gather(dw_all.at[1], SUP, 128, v_rz, v_rp, v_ss, put_dw(1))
    gk = Gather(dw_all.at[0], SUP, 128, k_rz, k_rp, k_ss, put_dw(0))
    with scope("dv"):
        def dv_out(ch):
            for q in range(2):
                dv_msg[q, ch] = dv[pl.ds(pl.multiple_of(ch * SUP, SUP) + q * BLK, BLK), :].astype(BF)

        loop(0, n_chip, dv_out)
        pair_dv = remote(dv_msg.at[1 - par], dv_part, pair_s.at[2], pair_r.at[2], partner)
        pair_dv.start()
        head_dw(1, 0, n_chip, lambda rows: dv[rows, :])
        pair_dwv = dw_exchange(1)
        pair_dv.wait_recv()

        def dv_add(ch):
            dv_msg[par, ch] = (dv_msg[par, ch].astype(F32) + dv_part[ch].astype(F32)).astype(BF)

        loop(0, n_chip, dv_add)
        dw_begin(1, pair_dwv)
        gv.begin()

        def dv_send(i):
            start(*dv_copy(lax.rem(chip + i, n_chip)))

        loop(0, n_chip, dv_send)

    pair_dk = [remote(dk_msg.at[1 - par, pl.ds(PLANE * g, PLANE)], dk_part.at[pl.ds(PLANE * g, PLANE)],
                      pair_s.at[3 + g], pair_r.at[3 + g], partner) for g in range(nz)]

    def dk_out(g):
        def put(ch):
            for q in range(2):
                rows = pl.ds(pl.multiple_of(ch * SUP, SUP) + q * BLK, BLK)
                dk_msg[q, ch, pl.ds(0, BLK), :] = dkr[rows, pl.ds(0, 128)].astype(BF)
                dk_msg[q, ch, pl.ds(BLK, 64), :] = pack_rope(dkr[rows, pl.ds(128, 128)][:, :64]).astype(BF)

        loop(PLANE * g, PLANE * (g + 1), put)
        pair_dk[g].start()
        head_dw(0, PLANE * g, PLANE * (g + 1), lambda rows: dkr[rows, pl.ds(0, 128)])

    def dk_add(g):
        pair_dk[g].wait_recv()

        def put(ch):
            dk_msg[par, ch] = (dk_msg[par, ch].astype(F32) + dk_part[ch].astype(F32)).astype(BF)

        loop(PLANE * g, PLANE * (g + 1), put)

    for g in reversed(range(nz)):
        for s in (2 * g + 1, 2 * g):
            with scope(f"bwd{s}"):
                backward(s)
        if g + 1 < nz:
            with scope(f"dks{g + 1}"):
                dk_add(g + 1)
        with scope(f"dko{g}"):
            dk_out(g)
        if g == 1:
            with scope("vz"):
                for d in range(1, nz):
                    gv.at(d, gv.from_z)

    with scope("dwk"):
        pair_dwk = dw_exchange(0)
        dw_begin(0, pair_dwk)
        gk.begin()
    with scope("dks0"):
        dk_add(0)
    with scope("vxy0"):
        gv.at(0, gv.xy)
    for d in range(nz):
        if d + 1 < nz:
            with scope(f"vxy{d + 1}"):
                gv.at(d + 1, gv.xy)
        with scope(f"vd{d}"):
            gv.at(d, gv.last)
            loop(d * n_chip // nz, (d + 1) * n_chip // nz, lambda i: start(*dk_copy(lax.rem(chip + i, n_chip))))
        if d == 0:
            with scope("ofin"):
                arrived(o_out, msg_rs.at[0])

                def lay_o(i):
                    rows = pl.ds(pl.multiple_of(i * 32, 32), 32)
                    o_fin[rows] = heads_first(o_out[:, rows, :])

                loop(0, BLK // 32, lay_o)

    def latent_grad():
        with scope("dc"):
            arrived(dv_recv, msg_rs.at[2])
            arrived(dk_recv, msg_rs.at[3])
            dkv = jnp.concatenate([g for h in range(n_chip) for g in (dk_recv[h, pl.ds(0, BLK), :], dv_recv[h])], axis=1)
            dc_fin[...] = mm(dkv, w_big[...], NT).astype(BF)
            dr = dk_recv[0, pl.ds(BLK, 64), :].astype(F32)
            for h in range(1, n_chip):
                dr = dr + dk_recv[h, pl.ds(BLK, 64), :].astype(F32)
            dr_fin[...] = jnp.transpose(jnp.concatenate([dr[:, :64], dr[:, 64:]], axis=0)).astype(BF)

    gk.steps("k", latent_grad)

    with scope("drain"):
        arrived(dq_out, msg_rs.at[1])
        outs = [pltpu.make_async_copy(buf, dst, out_sem.at[i]) for i, (buf, dst) in enumerate(
            ((dq_out, dq_hbm), (o_fin, o_hbm), (dc_fin, dc_hbm), (dr_fin, dr_hbm)))]
        for c in outs:
            c.start()
        for g in (gc, gv, gk):
            g.finish()
        for c in [pair_dv, pair_dwv, pair_dwk] + pair_dk:
            c.wait_send()
        for k, buf in enumerate((q_recv, do_recv, o_out, dq_out)):
            @pl.when(owner_core == par)
            def _():
                arrived(buf.at[pl.ds(0, n_chip - 1)], msg_ss.at[k])

            @pl.when(owner_core != par)
            def _():
                arrived(buf, msg_ss.at[k])
        for k, buf in enumerate((dv_recv, dk_recv)):
            arrived(buf.at[pl.ds(0, n_chip - 1)], msg_ss.at[4 + k])
        for k in range(2):
            arrived(dw_all.at[k], dw_sem.at[k])
        for c in outs:
            c.wait()


def solution(mesh):
    n_dev = mesh.shape["cp"]
    n_chip = n_dev // 2
    nz = n_chip // PLANE
    seq = n_dev * BLK
    seq_spec = P("cp")

    def local_step(queries, latent, key_rope, w_uk, w_uv, d_out):
        vm = pl.BlockSpec(memory_space=pltpu.VMEM)
        hbm = pl.BlockSpec(memory_space=pl.ANY)
        dma = pltpu.SemaphoreType.DMA
        gather_sems = [dma((4, nz)), dma((nz,)), dma((2,))]
        o, dq, dc, dr, dwk, dwv = pl.pallas_call(
            functools.partial(kernel, nz, queries.shape[-1]),
            out_shape=(jax.ShapeDtypeStruct((BLK, n_chip, 128), BF),
                       jax.ShapeDtypeStruct((n_chip, 192, BLK), BF),
                       jax.ShapeDtypeStruct((BLK, 512), BF),
                       jax.ShapeDtypeStruct((64, BLK), BF),
                       jax.ShapeDtypeStruct((512, n_chip, 1, 128), F32),
                       jax.ShapeDtypeStruct((512, n_chip, 1, 128), F32)),
            in_specs=[vm] * 4 + [hbm] * 2,
            out_specs=(hbm,) * 6,
            scratch_shapes=[
                pltpu.VMEM((n_chip, BLK, 128), BF),
                pltpu.VMEM((n_chip, 192, BLK), BF),
                pltpu.VMEM((n_chip, BLK, 128), BF),
                pltpu.VMEM((n_chip, 192, 128), BF),
                pltpu.VMEM((BLK, n_chip, 128), BF),
                pltpu.VMEM((BLK, 512), BF),
                pltpu.VMEM((64, BLK), BF),
                pltpu.VMEM((n_chip, BLK, 128), BF),
                pltpu.VMEM((512, n_chip * 256), BF),
                pltpu.VMEM((2, BLK, n_chip, 128), BF),
                pltpu.VMEM((256, 512), BF),
                pltpu.VMEM((n_chip, 192, BLK), BF),
                pltpu.VMEM((n_chip, BLK, 128), BF),
                pltpu.VMEM((2, n_chip, 144, 512), BF),
                pltpu.VMEM((seq, 256), BF),
                pltpu.VMEM((seq, 128), BF),
                pltpu.VMEM((192, seq), BF),
                pltpu.VMEM((128, seq), BF),
                pltpu.VMEM((seq, SUP), F32),
                pltpu.VMEM((CH, SUP), BF),
                pltpu.VMEM((nz * (nz + 1) * CH, SUP), BF),
                pltpu.VMEM((CH, SUP), BF),
                pltpu.VMEM((seq, 256), F32),
                pltpu.VMEM((seq, 128), F32),
                pltpu.VMEM((256, SUP), BF),
                pltpu.VMEM((SUP, 128), BF),
                pltpu.VMEM((128, SUP), F32),
                pltpu.VMEM((128, SUP), F32),
                pltpu.VMEM((192, SUP), F32),
                pltpu.VMEM((8, SUP), F32),
                pltpu.VMEM((n_chip // 2, 1, SUP), F32),
                pltpu.VMEM((n_chip, BLK, 128), BF),
                pltpu.VMEM((n_chip, 192, BLK), BF),
                pltpu.VMEM((2, n_chip, BLK, 128), BF),
                pltpu.VMEM((n_chip, BLK, 128), BF),
                pltpu.VMEM((2, n_chip, 192, 128), BF),
                pltpu.VMEM((n_chip, 192, 128), BF),
                pltpu.VMEM((2, 128, 512), F32),
                pltpu.VMEM((2, 2, SUP, 128), F32),
                pltpu.VMEM((2, SUP, 128), F32),
                pltpu.VMEM((2, 2, n_chip, SUP, 128), F32),
            ] + [dma((6,)), dma((4,)), dma((n_chip // 2,)), dma((n_chip // 2,))] + [dma((3 + nz,)), dma((3 + nz,)), dma((2,)), dma((4,)), dma((2,))] + gather_sems * 3,
            compiler_params=pltpu.CompilerParams(
                collective_id=0, has_side_effects=True, vmem_limit_bytes=62 * 1024 * 1024),
        )(queries.transpose(1, 2, 0), d_out, latent, key_rope.T, w_uk, w_uv)
        return (o, dq.transpose(2, 0, 1), dc, dr.T,
                dwk.reshape(512, n_chip, 128), dwv.reshape(512, n_chip, 128))

    return jax.shard_map(local_step, mesh=mesh,
                         in_specs=(seq_spec, seq_spec, seq_spec, P(), P(), seq_spec),
                         out_specs=(seq_spec, seq_spec, seq_spec, seq_spec, P(), P()),
                         check_vma=False)
```

```python
import functools
import math

import jax
import jax.numpy as jnp
from jax import lax
from jax.experimental import pallas as pl
from jax.experimental.pallas import tpu as pltpu
from jax.sharding import PartitionSpec as P

MESH = pl.DeviceIdType.MESH
NX, NY = 2, 2
PLANE = NX * NY
BLK = 128
SUP = 256
CH = SUP * PLANE
NEG = -1e30
NT = (((1,), (1,)), ((), ()))
NN = (((1,), (0,)), ((), ()))
BF, F32 = jnp.bfloat16, jnp.float32


def mm(a, b, dims=NN):
    return lax.dot_general(a, b, dims, preferred_element_type=F32)


def pack_rope(x):
    return jnp.concatenate([x[:64], x[64:]], axis=1)


def kernel(nz, qk_dim, q_ref, do_raw, c_ref, rt_ref, wk_hbm, wv_hbm,
           o_hbm, dq_hbm, dc_hbm, dr_hbm, dwk_out, dwv_out,
           o_out, dq_out, dv_recv, dk_recv, o_fin, dc_fin, dr_fin, do_ref,
           w_big, w_stage, wt_cat, q_recv, do_recv, c_all, kr, v, kt, vt, s_buf, p_buf, p_store, ds_buf, dkr, dv,
           qt, dof, dot_, ot, dqt, lse, delta_s, o_send, dq_send, dv_msg, dv_part, dk_msg, dk_part,
           dwt, dw_msg, dw_part, dw_all,
           msg_ss, msg_rs, q_rs, do_rs, pair_s, pair_r, dw_sem, out_sem, w_sem,
           cg_rz, cg_rp, cg_ss, v_rz, v_rp, v_ss, k_rz, k_rp, k_ss):
    n_chip = PLANE * nz
    n_dev = 2 * n_chip
    n_sup = n_chip // 2
    me = lax.axis_index("cp")
    chip, par = me // 2, me % 2
    partner = 2 * chip + (1 - par)
    x, y, z = chip % NX, (chip // NX) % NY, chip // PLANE
    scale = 1.0 / math.sqrt(qk_dim)
    c1 = scale * math.log2(math.e)
    scope = jax.named_scope

    def chip_at(zq, yq, xq):
        return (zq * NY + yq) * NX + xq

    def col_chip(col, zq):
        return chip_at(zq, 1 - y if col >= 2 else y, 1 - x if col % 2 else x)

    def remote(src, dst, ssem, rsem, dev):
        return pltpu.make_async_remote_copy(src_ref=src, dst_ref=dst, send_sem=ssem, recv_sem=rsem,
                                            device_id=(dev,), device_id_type=MESH)

    def start(src, dst, ssem, rsem, dev):
        @pl.when(dev == me)
        def _():
            pltpu.make_async_copy(src, dst, rsem).start()

        @pl.when(dev != me)
        def _():
            remote(src, dst, ssem, rsem, dev).start()

    def arrived(dst, rsem):
        pltpu.make_async_copy(dst, dst, rsem).wait()

    def loop(lo, hi, f):
        def body(i, carry):
            f(i)
            return carry

        lax.fori_loop(lo, hi, body, 0)

    n_piece = 8

    def w_copy(i):
        src = wk_hbm if i < n_piece // 2 else wv_hbm
        return pltpu.make_async_copy(src.at[pl.ds(i % (n_piece // 2) * BLK, BLK)], w_stage.at[i % 2], w_sem.at[i % 2])

    for i in range(2):
        w_copy(i).start()

    def heads_first(x):
        return jnp.transpose(x, (1, 0, 2))

    with scope("barrier"):
        barrier = pltpu.get_barrier_semaphore()
        loop(1, n_dev, lambda i: pl.semaphore_signal(
            barrier, inc=1, device_id=(lax.rem(me + i, n_dev),), device_id_type=MESH))
        pl.semaphore_wait(barrier, n_dev - 1)

    class Gather:
        def __init__(self, buf, rows, split, rz, rp, ss, ready):
            self.buf, self.rows, self.split = buf, rows, split
            self.rz, self.rp, self.ss, self.ready = rz, rp, ss, ready
            self.dev_x = 2 * chip_at(z, y, 1 - x) + par
            self.middle = ((1, 0, 2), (2, 3, 1)) if nz == 4 else ()
            self.dev_y = 2 * chip_at(z, 1 - y, x) + par

        def blk(self, col, zq):
            return self.buf.at[par, col_chip(col, zq)]

        def along_z(self, zq, to):
            b = self.blk(0, zq)
            return remote(b, b, self.ss.at[2], self.rz.at[0, zq], 2 * chip_at(to, y, x) + par)

        def to_x(self, col, zq):
            b = self.blk(col, zq)
            return remote(b, b, self.ss.at[0], self.rz.at[1, zq], self.dev_x)

        def to_y(self, col, zq):
            b = self.blk(col, zq)
            return remote(b, b, self.ss.at[0], self.rz.at[2, zq], self.dev_y)

        def part_y(self, col, zq):
            b = self.blk(col, zq).at[pl.ds(0, self.split)]
            return remote(b, b, self.ss.at[0], self.rz.at[3, zq], self.dev_y)

        def part_x(self, col, zq):
            b = self.blk(col, zq).at[pl.ds(self.split, self.rows - self.split)]
            return remote(b, b, self.ss.at[0], self.rz.at[3, zq], self.dev_x)

        def pair(self, col, zq):
            b = self.blk(col, zq)
            return remote(b, b, self.ss.at[1], self.rp.at[zq], partner)

        def own_col(self, zq):
            self.to_x(0, zq).start()
            self.to_y(0, zq).start()
            self.pair(0, zq).start()

        def xy(self, zq):
            self.to_x(1, zq).wait_recv()
            self.part_y(1, zq).start()
            self.pair(1, zq).start()
            self.to_y(2, zq).wait_recv()
            self.part_x(2, zq).start()
            self.pair(2, zq).start()

        def diag(self, zq):
            arrived(self.blk(3, zq), self.rz.at[3, zq])
            self.pair(3, zq).start()

        def pairs(self, zq):
            arrived(self.buf.at[1 - par, pl.ds(zq * PLANE, PLANE)], self.rp.at[zq])

        def begin(self):
            for d in range(1, nz):
                @pl.when(z + d < nz)
                def _():
                    self.along_z(z, z + d).start()

                @pl.when(z - d >= 0)
                def _():
                    self.along_z(z, z - d).start()

            self.own_col(z)

        def from_z(self, zq):
            self.along_z(zq, z).wait_recv()
            self.own_col(zq)

        def begin_chain(self):
            @pl.when(z + 1 < nz)
            def _():
                self.along_z(z, z + 1).start()

            @pl.when(z > 0)
            def _():
                self.along_z(z, z - 1).start()

            self.own_col(z)
            for mid, outer, inner in self.middle:
                @pl.when(z == mid)
                def _():
                    self.along_z(outer, z).wait_recv()
                    self.along_z(outer, inner).start()
                    self.own_col(outer)

        def from_z_chain(self, zq):
            done = z == zq
            for mid, outer, inner in self.middle:
                done = jnp.logical_or(done, jnp.logical_and(z == mid, zq == outer))

            @pl.when(jnp.logical_not(done))
            def _():
                self.along_z(zq, z).wait_recv()
                for mid, outer, inner in self.middle:
                    @pl.when(z == mid)
                    def _():
                        self.along_z(zq, outer).start()

                self.own_col(zq)

        def at(self, d, f):
            if d == 0:
                f(z)
                return

            @pl.when(z - d >= 0)
            def _():
                f(z - d)

            @pl.when(z + d < nz)
            def _():
                f(z + d)

        def last(self, zq):
            self.diag(zq)
            self.pairs(zq)
            self.ready(zq)

        def steps(self, tag, after_z, before_last):
            for d in range(1, nz):
                with scope(f"{tag}z{d}"):
                    self.at(d, self.from_z)
                    after_z(d)
                with scope(f"{tag}xy{d - 1}"):
                    self.at(d - 1, self.xy)
                if d >= 2:
                    with scope(f"{tag}d{d - 2}"):
                        self.at(d - 2, self.last)
            with scope(f"{tag}xy{nz - 1}"):
                self.at(nz - 1, self.xy)
            for d in range(max(nz - 2, 0), nz):
                if d == nz - 1:
                    before_last()
                with scope(f"{tag}d{d}"):
                    self.at(d, self.last)

        def finish(self, chain):
            arrived(self.buf.at[0, pl.ds(0, 3 * nz)], self.ss.at[0])
            arrived(self.buf.at[0], self.ss.at[1])
            if not chain:
                arrived(self.buf.at[0, pl.ds(0, nz - 1)], self.ss.at[2])
            else:
                outer = jnp.logical_or(z == 0, z == nz - 1)

                @pl.when(outer)
                def _():
                    arrived(self.buf.at[0, pl.ds(0, 1)], self.ss.at[2])

                @pl.when(jnp.logical_not(outer))
                def _():
                    arrived(self.buf.at[0, pl.ds(0, 5)], self.ss.at[2])

    owner_core = lax.rem((chip + 1) // 2, 2)
    q_slot = 2 * (chip // 2) + par

    def sup_chip(s):
        return 2 * s + lax.rem(s + par, 2)

    def q_copy(i):
        head = lax.rem(chip + i, n_chip)
        return q_ref.at[head], q_recv.at[q_slot], msg_ss.at[0], q_rs.at[q_slot // 2], 2 * head + owner_core

    def do_copy(i):
        head = lax.rem(chip + i, n_chip)
        return do_ref.at[head], do_recv.at[q_slot], msg_ss.at[1], do_rs.at[q_slot // 2], 2 * head + owner_core

    def o_copy(s, i):
        return o_send.at[2 * s + i], o_out.at[chip], msg_ss.at[2], msg_rs.at[0], 2 * sup_chip(s) + i

    def dq_copy(s, i):
        return dq_send.at[2 * s + i], dq_out.at[chip], msg_ss.at[3], msg_rs.at[1], 2 * sup_chip(s) + i

    def dv_copy(ch):
        return dv_msg.at[par, ch], dv_recv.at[chip], msg_ss.at[4], msg_rs.at[2], 2 * ch + par

    def dk_copy(ch):
        return dk_msg.at[par, ch], dk_recv.at[chip], msg_ss.at[5], msg_rs.at[3], 2 * ch + par

    gc = Gather(c_all, 144, 80, cg_rz, cg_rp, cg_ss, None)
    with scope("send_c"):
        c_all[par, chip, pl.ds(0, BLK), :] = c_ref[...]
        for i in range(4):
            c_all[par, chip, pl.ds(BLK, 16), pl.ds(128 * i, 128)] = rt_ref[pl.ds(16 * i, 16), :]
        gc.begin_chain()
    with scope("send_q"):
        def send_q(i):
            start(*q_copy(i))
            start(*do_copy(i))

        late = z >= nz // 2

        def lay_do(i):
            rows = pl.ds(pl.multiple_of(i * 32, 32), 32)
            do_ref[:, rows, :] = heads_first(do_raw[rows])

        loop(0, BLK // 32, lay_do)

        @pl.when(jnp.logical_not(late))
        def _():
            loop(0, n_chip, send_q)

    with scope("init"):
        dkr[...] = jnp.zeros_like(dkr)
        dv[...] = jnp.zeros_like(dv)
        for i in range(n_piece):
            w_copy(i).wait()

            def lay_w(r):
                w = heads_first(w_stage[i % 2, pl.ds(pl.multiple_of(r * 32, 32), 32)])
                rows = pl.ds(pl.multiple_of(i % (n_piece // 2) * BLK + r * 32, 32), 32)
                for h in range(n_chip):
                    w_big[rows, pl.ds(h * 256 + 128 * (i // (n_piece // 2)), 128)] = w[h]

            loop(0, BLK // 32, lay_w)
            if i + 2 < n_piece:
                w_copy(i + 2).start()
        wt_cat[...] = jnp.transpose(w_big[:, pl.ds(pl.multiple_of(chip * 256, 256), 256)].astype(F32)).astype(BF)
        qt[pl.ds(192, 64), :] = jnp.zeros((64, SUP), BF)

    def latent_of(ch):
        return jnp.concatenate([c_all[0, ch, pl.ds(0, BLK), :], c_all[1, ch, pl.ds(0, BLK), :]], axis=0)

    def up_project(ch):
        base = pl.multiple_of(ch * SUP, SUP)
        lat = latent_of(ch)
        kv = mm(lat, w_big[:, pl.ds(pl.multiple_of(chip * 256, 256), 256)]).astype(BF)
        kvt = mm(wt_cat[...], lat, NT).astype(BF)
        kr[pl.ds(base, SUP), pl.ds(0, 128)] = kv[:, :128]
        v[pl.ds(base, SUP), :] = kv[:, 128:]
        kt[pl.ds(0, 128), pl.ds(base, SUP)] = kvt[:128]
        vt[:, pl.ds(base, SUP)] = kvt[128:]
        for q in range(2):
            rt = jnp.concatenate([c_all[q, ch, pl.ds(BLK, 16), pl.ds(128 * i, 128)] for i in range(4)], axis=0)
            kt[pl.ds(128, 64), pl.ds(base + q * BLK, BLK)] = rt
            r = jnp.transpose(rt.astype(F32))
            kr[pl.ds(base + q * BLK, BLK), pl.ds(128, 128)] = jnp.concatenate(
                [r, jnp.zeros_like(r)], axis=1).astype(BF)

    diff = lax.broadcasted_iota(jnp.int32, (SUP, SUP), 0) - lax.broadcasted_iota(jnp.int32, (SUP, SUP), 1)

    def load_q(s):
        for i in range(2):
            qt[pl.ds(0, 192), pl.ds(i * BLK, BLK)] = q_recv[2 * s + i]
            dof[pl.ds(i * BLK, BLK), :] = do_recv[2 * s + i]

    def store_row(s):
        a = s // 2
        return (a + 1) * (a + s % 2) * CH

    def forward(s):
        ch = sup_chip(s)
        arrived(q_recv.at[pl.ds(2 * s, 2)], q_rs.at[s])
        arrived(do_recv.at[pl.ds(2 * s, 2)], do_rs.at[s])
        load_q(s)
        dot_[...] = jnp.transpose(dof[...].astype(F32))
        n_ch = s // 2 + 1

        def score(j, m8):
            for t in range(CH // SUP):
                r0 = pl.multiple_of(j * CH + t * SUP, SUP)
                st = mm(kr[pl.ds(r0, SUP), :], qt[...])
                st = jnp.where(diff <= ch * SUP - r0, st, NEG)
                s_buf[pl.ds(r0, SUP), :] = st
                m8 = jnp.maximum(m8, jnp.max(st.reshape(SUP // 8, 8, SUP), axis=0))
            return m8

        m8 = lax.fori_loop(0, n_ch, score, jnp.full((8, SUP), NEG, F32))
        m2 = jnp.max(m8, axis=0, keepdims=True) * c1
        ot[...] = jnp.zeros_like(ot)

        def values(j, l8):
            base = pl.multiple_of(j * CH, CH)
            for t in range(CH // SUP):
                p = jnp.exp2(s_buf[pl.ds(base + t * SUP, SUP), :] * c1 - m2)
                l8 = l8 + jnp.sum(p.reshape(SUP // 8, 8, SUP), axis=0)
                p_buf[pl.ds(t * SUP, SUP), :] = p.astype(BF)
            ot[...] += mm(vt[:, pl.ds(base, CH)], p_buf[...])
            return l8

        l8 = lax.fori_loop(0, n_ch, values, jnp.zeros((8, SUP), F32))
        l = jnp.sum(l8, axis=0, keepdims=True)
        o = ot[...] / l
        lse2 = m2 + jnp.log2(l)
        delta_s[s] = jnp.sum(o * dot_[...], axis=0, keepdims=True)
        o_rows = jnp.transpose(o)
        for i in range(2):
            o_send[2 * s + i] = o_rows[i * BLK:(i + 1) * BLK].astype(BF)
        for i in range(2):
            start(*o_copy(s, i))
        row0 = store_row(s)

        def values_grad(j):
            base = pl.multiple_of(j * CH, CH)
            for t in range(CH // SUP):
                rows = pl.ds(base + t * SUP, SUP)
                p = jnp.exp2(s_buf[rows, :] * c1 - lse2).astype(BF)
                p_store[pl.ds(pl.multiple_of(row0 + base + t * SUP, SUP), SUP), :] = p
                dv[rows, :] += mm(p, dof[...])

        loop(0, n_ch, values_grad)

    def backward(s):
        load_q(s)
        dqt[...] = jnp.zeros_like(dqt)
        row0 = store_row(s)
        delta = delta_s[s]

        def keys_grad(j):
            base = pl.multiple_of(j * CH, CH)
            for t in range(CH // SUP):
                rows = pl.ds(base + t * SUP, SUP)
                dp = mm(v[rows, :], dof[...], NT)
                p = p_store[pl.ds(pl.multiple_of(row0 + base + t * SUP, SUP), SUP), :].astype(F32)
                ds_buf[pl.ds(t * SUP, SUP), :] = (p * (dp - delta) * scale).astype(BF)
            for t in range(CH // SUP):
                rows = pl.ds(base + t * SUP, SUP)
                dkr[rows, :] += mm(ds_buf[pl.ds(t * SUP, SUP), :], qt[...], NT)
            dqt[...] += mm(kt[:, pl.ds(base, CH)], ds_buf[...])

        loop(0, s // 2 + 1, keys_grad)
        for i in range(2):
            dq_send[2 * s + i] = dqt[:, pl.ds(i * BLK, BLK)].astype(BF)
        for i in range(2):
            start(*dq_copy(s, i))

    def ready_c(zq):
        gc.pairs(zq)
        loop(zq * PLANE, (zq + 1) * PLANE, up_project)

    def col_ready(zq):
        gc.from_z_chain(zq)

    def step_c(k):
        if k < nz:
            col_ready(k)
        if 0 <= k - 1 < nz:
            gc.xy(k - 1)
        if 0 <= k - 2 < nz:
            gc.diag(k - 2)
            ready_c(k - 2)

    for k in range(nz + 2):
        with scope(f"c{k}"):
            step_c(k)
            if k < 2:
                @pl.when(late)
                def _():
                    loop(k * n_chip // 2, (k + 1) * n_chip // 2, send_q)

        if k >= 2:
            with scope(f"fwd{k - 2}"):
                loop(2 * (k - 2), 2 * (k - 2) + 2, forward)

    def head_dw(k, lo, hi, grads):
        def add(ch):
            base = pl.multiple_of(ch * SUP, SUP)
            g = jnp.transpose(grads(pl.ds(base, SUP))).astype(BF)
            dwt[k] += mm(g, latent_of(ch))

        loop(lo, hi, add)

    def dw_exchange(k):
        dw_msg[k] = jnp.transpose(dwt[k]).reshape(2, SUP, 128)
        c = remote(dw_msg.at[k, 1 - par], dw_part.at[k], pair_s.at[k], pair_r.at[k], partner)
        c.start()
        return c

    def dw_begin(k, c):
        c.wait_recv()
        dw_all[k, par, chip] = dw_msg[k, par] + dw_part[k]

    def dw_out_copy(k, q, h):
        dst = dwk_out if k == 0 else dwv_out
        return pltpu.make_async_copy(dw_all.at[k, q, h], dst.at[pl.ds(q * SUP, SUP), h, 0], dw_sem.at[k])

    def put_dw(k):
        def put(zq):
            for q in range(2):
                loop(zq * PLANE, (zq + 1) * PLANE, lambda h: dw_out_copy(k, q, h).start())

        return put

    dwt[...] = jnp.zeros_like(dwt)
    gv = Gather(dw_all.at[1], SUP, 128, v_rz, v_rp, v_ss, put_dw(1))
    gk = Gather(dw_all.at[0], SUP, 128, k_rz, k_rp, k_ss, put_dw(0))
    with scope("dv"):
        def dv_out(ch):
            for q in range(2):
                dv_msg[q, ch] = dv[pl.ds(pl.multiple_of(ch * SUP, SUP) + q * BLK, BLK), :].astype(BF)

        loop(0, n_chip, dv_out)
        pair_dv = remote(dv_msg.at[1 - par], dv_part, pair_s.at[2], pair_r.at[2], partner)
        pair_dv.start()
        head_dw(1, 0, n_chip, lambda rows: dv[rows, :])
        pair_dwv = dw_exchange(1)
        pair_dv.wait_recv()

        def dv_add(ch):
            dv_msg[par, ch] = (dv_msg[par, ch].astype(F32) + dv_part[ch].astype(F32)).astype(BF)

        loop(0, n_chip, dv_add)
        dw_begin(1, pair_dwv)
        gv.begin()

        def dv_send(i):
            start(*dv_copy(lax.rem(chip + i, n_chip)))

        loop(0, n_chip, dv_send)

    pair_dk = [remote(dk_msg.at[1 - par, pl.ds(PLANE * g, PLANE)], dk_part.at[pl.ds(PLANE * g, PLANE)],
                      pair_s.at[3 + g], pair_r.at[3 + g], partner) for g in range(nz)]

    def dk_out(g):
        def put(ch):
            for q in range(2):
                rows = pl.ds(pl.multiple_of(ch * SUP, SUP) + q * BLK, BLK)
                dk_msg[q, ch, pl.ds(0, BLK), :] = dkr[rows, pl.ds(0, 128)].astype(BF)
                dk_msg[q, ch, pl.ds(BLK, 64), :] = pack_rope(dkr[rows, pl.ds(128, 128)][:, :64]).astype(BF)

        loop(PLANE * g, PLANE * (g + 1), put)
        pair_dk[g].start()
        head_dw(0, PLANE * g, PLANE * (g + 1), lambda rows: dkr[rows, pl.ds(0, 128)])

    def dk_add(g):
        pair_dk[g].wait_recv()

        def put(ch):
            dk_msg[par, ch] = (dk_msg[par, ch].astype(F32) + dk_part[ch].astype(F32)).astype(BF)

        loop(PLANE * g, PLANE * (g + 1), put)

    for g in reversed(range(nz)):
        for s in (2 * g + 1, 2 * g):
            with scope(f"bwd{s}"):
                backward(s)
        if g + 1 < nz:
            with scope(f"dks{g + 1}"):
                dk_add(g + 1)
        with scope(f"dko{g}"):
            dk_out(g)
        if g == 1:
            with scope("vz"):
                for d in range(1, nz):
                    gv.at(d, gv.from_z)

    with scope("dwk"):
        pair_dwk = dw_exchange(0)
        dw_begin(0, pair_dwk)
        gk.begin()
    with scope("dks0"):
        dk_add(0)

    def dk_quarter(k):
        loop(k * n_chip // nz, (k + 1) * n_chip // nz, lambda i: start(*dk_copy(lax.rem(chip + i, n_chip))))

    def dk_after(d):
        for k in range(nz // 2 + d - 1, nz // 2 + d if d < nz - 1 else nz):
            if k < nz:
                dk_quarter(k)

    with scope("vxy0"):
        gv.at(0, gv.xy)
    for d in range(nz):
        if d + 1 < nz:
            with scope(f"vxy{d + 1}"):
                gv.at(d + 1, gv.xy)
        with scope(f"vd{d}"):
            gv.at(d, gv.last)
            if d >= nz // 2:
                dk_quarter(d - nz // 2)
        if d == 0:
            with scope("ofin"):
                arrived(o_out, msg_rs.at[0])

                def lay_o(i):
                    rows = pl.ds(pl.multiple_of(i * 32, 32), 32)
                    o_fin[rows] = heads_first(o_out[:, rows, :])

                loop(0, BLK // 32, lay_o)

    def latent_grad():
        with scope("dc"):
            arrived(dv_recv, msg_rs.at[2])
            arrived(dk_recv, msg_rs.at[3])
            dkv = jnp.concatenate([g for h in range(n_chip) for g in (dk_recv[h, pl.ds(0, BLK), :], dv_recv[h])], axis=1)
            dc_fin[...] = mm(dkv, w_big[...], NT).astype(BF)
            dr = dk_recv[0, pl.ds(BLK, 64), :].astype(F32)
            for h in range(1, n_chip):
                dr = dr + dk_recv[h, pl.ds(BLK, 64), :].astype(F32)
            dr_fin[...] = jnp.transpose(jnp.concatenate([dr[:, :64], dr[:, 64:]], axis=0)).astype(BF)

    gk.steps("k", dk_after, latent_grad)

    with scope("drain"):
        arrived(dq_out, msg_rs.at[1])
        outs = [pltpu.make_async_copy(buf, dst, out_sem.at[i]) for i, (buf, dst) in enumerate(
            ((dq_out, dq_hbm), (o_fin, o_hbm), (dc_fin, dc_hbm), (dr_fin, dr_hbm)))]
        for c in outs:
            c.start()
        gc.finish(True)
        gv.finish(False)
        gk.finish(False)
        for c in [pair_dv, pair_dwv, pair_dwk] + pair_dk:
            c.wait_send()
        for k, buf in enumerate((q_recv, do_recv, o_out, dq_out)):
            @pl.when(owner_core == par)
            def _():
                arrived(buf.at[pl.ds(0, n_chip - 1)], msg_ss.at[k])

            @pl.when(owner_core != par)
            def _():
                arrived(buf, msg_ss.at[k])
        for k, buf in enumerate((dv_recv, dk_recv)):
            arrived(buf.at[pl.ds(0, n_chip - 1)], msg_ss.at[4 + k])
        for k in range(2):
            arrived(dw_all.at[k], dw_sem.at[k])
        for c in outs:
            c.wait()


def copy_kernel(*refs):
    n = len(RESULT_PIECES)
    src, dst, buf, (sem_in, sem_out) = refs[:n], refs[n:2 * n], refs[2 * n:3 * n], refs[3 * n:]
    ins, outs = [], []
    for a, b, c, pieces in zip(src, dst, buf, RESULT_PIECES):
        size = a.shape[0] // pieces
        for i in range(pieces):
            rows = pl.ds(i * size, size)
            ins.append(pltpu.make_async_copy(a.at[rows], c.at[rows], sem_in.at[len(ins)]))
            outs.append(pltpu.make_async_copy(c.at[rows], b.at[rows], sem_out.at[len(outs)]))
    for c in ins:
        c.start()
    for c, d in zip(ins, outs):
        c.wait()
        d.start()
    for d in outs:
        d.wait()


RESULT_PIECES = (1, 1, 1, 1, 4, 4)


def copy_results(*arrays):
    hbm = pl.BlockSpec(memory_space=pl.ANY)
    shapes = tuple(jax.ShapeDtypeStruct(a.shape, a.dtype) for a in arrays)
    dma = pltpu.SemaphoreType.DMA((sum(RESULT_PIECES),))
    return pl.pallas_call(
        copy_kernel, out_shape=shapes, in_specs=[hbm] * len(arrays), out_specs=(hbm,) * len(arrays),
        scratch_shapes=[pltpu.VMEM(a.shape, a.dtype) for a in arrays] + [dma, dma],
    )(*arrays)


def solution(mesh):
    n_dev = mesh.shape["cp"]
    n_chip = n_dev // 2
    nz = n_chip // PLANE
    seq = n_dev * BLK
    seq_spec = P("cp")

    def local_step(queries, latent, key_rope, w_uk, w_uv, d_out):
        vm = pl.BlockSpec(memory_space=pltpu.VMEM)
        hbm = pl.BlockSpec(memory_space=pl.ANY)
        dma = pltpu.SemaphoreType.DMA
        gather_sems = [dma((4, nz)), dma((nz,)), dma((3,))]
        o, dq, dc, dr, dwk, dwv = pl.pallas_call(
            functools.partial(kernel, nz, queries.shape[-1]),
            out_shape=(jax.ShapeDtypeStruct((BLK, n_chip, 128), BF),
                       jax.ShapeDtypeStruct((n_chip, 192, BLK), BF),
                       jax.ShapeDtypeStruct((BLK, 512), BF),
                       jax.ShapeDtypeStruct((64, BLK), BF),
                       jax.ShapeDtypeStruct((512, n_chip, 1, 128), F32),
                       jax.ShapeDtypeStruct((512, n_chip, 1, 128), F32)),
            in_specs=[vm] * 4 + [hbm] * 2,
            out_specs=(hbm,) * 6,
            scratch_shapes=[
                pltpu.VMEM((n_chip, BLK, 128), BF),
                pltpu.VMEM((n_chip, 192, BLK), BF),
                pltpu.VMEM((n_chip, BLK, 128), BF),
                pltpu.VMEM((n_chip, 192, 128), BF),
                pltpu.VMEM((BLK, n_chip, 128), BF),
                pltpu.VMEM((BLK, 512), BF),
                pltpu.VMEM((64, BLK), BF),
                pltpu.VMEM((n_chip, BLK, 128), BF),
                pltpu.VMEM((512, n_chip * 256), BF),
                pltpu.VMEM((2, BLK, n_chip, 128), BF),
                pltpu.VMEM((256, 512), BF),
                pltpu.VMEM((n_chip, 192, BLK), BF),
                pltpu.VMEM((n_chip, BLK, 128), BF),
                pltpu.VMEM((2, n_chip, 144, 512), BF),
                pltpu.VMEM((seq, 256), BF),
                pltpu.VMEM((seq, 128), BF),
                pltpu.VMEM((192, seq), BF),
                pltpu.VMEM((128, seq), BF),
                pltpu.VMEM((seq, SUP), F32),
                pltpu.VMEM((CH, SUP), BF),
                pltpu.VMEM((nz * (nz + 1) * CH, SUP), BF),
                pltpu.VMEM((CH, SUP), BF),
                pltpu.VMEM((seq, 256), F32),
                pltpu.VMEM((seq, 128), F32),
                pltpu.VMEM((256, SUP), BF),
                pltpu.VMEM((SUP, 128), BF),
                pltpu.VMEM((128, SUP), F32),
                pltpu.VMEM((128, SUP), F32),
                pltpu.VMEM((192, SUP), F32),
                pltpu.VMEM((8, SUP), F32),
                pltpu.VMEM((n_chip // 2, 1, SUP), F32),
                pltpu.VMEM((n_chip, BLK, 128), BF),
                pltpu.VMEM((n_chip, 192, BLK), BF),
                pltpu.VMEM((2, n_chip, BLK, 128), BF),
                pltpu.VMEM((n_chip, BLK, 128), BF),
                pltpu.VMEM((2, n_chip, 192, 128), BF),
                pltpu.VMEM((n_chip, 192, 128), BF),
                pltpu.VMEM((2, 128, 512), F32),
                pltpu.VMEM((2, 2, SUP, 128), F32),
                pltpu.VMEM((2, SUP, 128), F32),
                pltpu.VMEM((2, 2, n_chip, SUP, 128), F32),
            ] + [dma((6,)), dma((4,)), dma((n_chip // 2,)), dma((n_chip // 2,))] + [dma((3 + nz,)), dma((3 + nz,)), dma((2,)), dma((4,)), dma((2,))] + gather_sems * 3,
            compiler_params=pltpu.CompilerParams(
                collective_id=0, has_side_effects=True, vmem_limit_bytes=62 * 1024 * 1024),
        )(queries.transpose(1, 2, 0), d_out, latent, key_rope.T, w_uk, w_uv)
        o, dq, dc, dr, dwk, dwv = copy_results(
            o, dq, dc, dr, dwk.reshape(512, n_chip, 128), dwv.reshape(512, n_chip, 128))
        return o, dq.transpose(2, 0, 1), dc, dr.T, dwk, dwv

    return jax.shard_map(local_step, mesh=mesh,
                         in_specs=(seq_spec, seq_spec, seq_spec, P(), P(), seq_spec),
                         out_specs=(seq_spec, seq_spec, seq_spec, seq_spec, P(), P()),
                         check_vma=False)
```

```python
import functools
import math

import jax
import jax.numpy as jnp
from jax import lax
from jax.experimental import pallas as pl
from jax.experimental.pallas import tpu as pltpu
from jax.sharding import PartitionSpec as P

MESH = pl.DeviceIdType.MESH
NX, NY = 2, 2
PLANE = NX * NY
BLK = 128
SUP = 256
CH = SUP * PLANE
NEG = -1e30
NT = (((1,), (1,)), ((), ()))
NN = (((1,), (0,)), ((), ()))
BF, F32 = jnp.bfloat16, jnp.float32


def mm(a, b, dims=NN):
    return lax.dot_general(a, b, dims, preferred_element_type=F32)


def pack_rope(x):
    return jnp.concatenate([x[:64], x[64:]], axis=1)


def kernel(nz, qk_dim, q_ref, do_raw, c_ref, rt_ref, wk_hbm, wv_hbm,
           o_hbm, dq_hbm, dc_hbm, dr_hbm, dwk_out, dwv_out,
           o_out, dq_out, dv_recv, dk_recv, o_fin, dc_fin, dr_fin, do_ref,
           w_big, w_stage, wt_cat, q_recv, do_recv, c_all, kr, v, kt, vt, s_buf, p_buf, p_store, ds_buf, dkr, dv,
           qt, dof, dot_, ot, dqt, lse, delta_s, o_send, dq_send, dv_msg, dv_part, dk_msg, dk_part,
           dwt, dw_msg, dw_part, dw_all,
           msg_ss, msg_rs, q_rs, do_rs, pair_s, pair_r, dw_sem, out_sem, w_sem,
           cg_rz, cg_rp, cg_ss, v_rz, v_rp, v_ss, k_rz, k_rp, k_ss):
    n_chip = PLANE * nz
    n_dev = 2 * n_chip
    n_sup = n_chip // 2
    me = lax.axis_index("cp")
    chip, par = me // 2, me % 2
    partner = 2 * chip + (1 - par)
    x, y, z = chip % NX, (chip // NX) % NY, chip // PLANE
    scale = 1.0 / math.sqrt(qk_dim)
    c1 = scale * math.log2(math.e)
    scope = jax.named_scope

    def chip_at(zq, yq, xq):
        return (zq * NY + yq) * NX + xq

    def col_chip(col, zq):
        return chip_at(zq, 1 - y if col >= 2 else y, 1 - x if col % 2 else x)

    def remote(src, dst, ssem, rsem, dev):
        return pltpu.make_async_remote_copy(src_ref=src, dst_ref=dst, send_sem=ssem, recv_sem=rsem,
                                            device_id=(dev,), device_id_type=MESH)

    def start(src, dst, ssem, rsem, dev):
        @pl.when(dev == me)
        def _():
            pltpu.make_async_copy(src, dst, rsem).start()

        @pl.when(dev != me)
        def _():
            remote(src, dst, ssem, rsem, dev).start()

    def arrived(dst, rsem):
        pltpu.make_async_copy(dst, dst, rsem).wait()

    def loop(lo, hi, f):
        def body(i, carry):
            f(i)
            return carry

        lax.fori_loop(lo, hi, body, 0)

    n_piece = 8

    def w_copy(i):
        src = wk_hbm if i < n_piece // 2 else wv_hbm
        return pltpu.make_async_copy(src.at[pl.ds(i % (n_piece // 2) * BLK, BLK)], w_stage.at[i % 2], w_sem.at[i % 2])

    for i in range(2):
        w_copy(i).start()

    def heads_first(x):
        return jnp.transpose(x, (1, 0, 2))

    with scope("barrier"):
        barrier = pltpu.get_barrier_semaphore()
        loop(1, n_dev, lambda i: pl.semaphore_signal(
            barrier, inc=1, device_id=(lax.rem(me + i, n_dev),), device_id_type=MESH))
        pl.semaphore_wait(barrier, n_dev - 1)

    class Gather:
        def __init__(self, buf, rows, split, rz, rp, ss, ready):
            self.buf, self.rows, self.split = buf, rows, split
            self.rz, self.rp, self.ss, self.ready = rz, rp, ss, ready
            self.dev_x = 2 * chip_at(z, y, 1 - x) + par
            self.middle = ((1, 0, 2), (2, 3, 1)) if nz == 4 else ()
            self.dev_y = 2 * chip_at(z, 1 - y, x) + par

        def blk(self, col, zq):
            return self.buf.at[par, col_chip(col, zq)]

        def along_z(self, zq, to):
            b = self.blk(0, zq)
            return remote(b, b, self.ss.at[2], self.rz.at[0, zq], 2 * chip_at(to, y, x) + par)

        def to_x(self, col, zq):
            b = self.blk(col, zq)
            return remote(b, b, self.ss.at[0], self.rz.at[1, zq], self.dev_x)

        def to_y(self, col, zq):
            b = self.blk(col, zq)
            return remote(b, b, self.ss.at[0], self.rz.at[2, zq], self.dev_y)

        def part_y(self, col, zq):
            b = self.blk(col, zq).at[pl.ds(0, self.split)]
            return remote(b, b, self.ss.at[0], self.rz.at[3, zq], self.dev_y)

        def part_x(self, col, zq):
            b = self.blk(col, zq).at[pl.ds(self.split, self.rows - self.split)]
            return remote(b, b, self.ss.at[0], self.rz.at[3, zq], self.dev_x)

        def pair(self, col, zq):
            b = self.blk(col, zq)
            return remote(b, b, self.ss.at[1], self.rp.at[zq], partner)

        def own_col(self, zq):
            self.to_x(0, zq).start()
            self.to_y(0, zq).start()
            self.pair(0, zq).start()

        def xy(self, zq):
            self.to_x(1, zq).wait_recv()
            self.part_y(1, zq).start()
            self.pair(1, zq).start()
            self.to_y(2, zq).wait_recv()
            self.part_x(2, zq).start()
            self.pair(2, zq).start()

        def diag(self, zq):
            arrived(self.blk(3, zq), self.rz.at[3, zq])
            self.pair(3, zq).start()

        def pairs(self, zq):
            arrived(self.buf.at[1 - par, pl.ds(zq * PLANE, PLANE)], self.rp.at[zq])

        def begin(self):
            for d in range(1, nz):
                @pl.when(z + d < nz)
                def _():
                    self.along_z(z, z + d).start()

                @pl.when(z - d >= 0)
                def _():
                    self.along_z(z, z - d).start()

            self.own_col(z)

        def from_z(self, zq):
            self.along_z(zq, z).wait_recv()
            self.own_col(zq)

        def begin_chain(self):
            @pl.when(z + 1 < nz)
            def _():
                self.along_z(z, z + 1).start()

            @pl.when(z > 0)
            def _():
                self.along_z(z, z - 1).start()

            self.own_col(z)

        def pass_on(self):
            for mid, outer, inner in self.middle:
                @pl.when(z == mid)
                def _():
                    self.along_z(outer, z).wait_recv()
                    self.along_z(outer, inner).start()
                    self.own_col(outer)

        def from_z_chain(self, zq):
            done = z == zq
            for mid, outer, inner in self.middle:
                done = jnp.logical_or(done, jnp.logical_and(z == mid, zq == outer))

            @pl.when(jnp.logical_not(done))
            def _():
                self.along_z(zq, z).wait_recv()
                for mid, outer, inner in self.middle:
                    @pl.when(z == mid)
                    def _():
                        self.along_z(zq, outer).start()

                self.own_col(zq)

        def at(self, d, f):
            if d == 0:
                f(z)
                return

            @pl.when(z - d >= 0)
            def _():
                f(z - d)

            @pl.when(z + d < nz)
            def _():
                f(z + d)

        def last(self, zq):
            self.diag(zq)
            self.pairs(zq)
            self.ready(zq)

        def finish(self, chain):
            arrived(self.buf.at[0, pl.ds(0, 3 * nz)], self.ss.at[0])
            arrived(self.buf.at[0], self.ss.at[1])
            if not chain:
                arrived(self.buf.at[0, pl.ds(0, nz - 1)], self.ss.at[2])
            else:
                outer = jnp.logical_or(z == 0, z == nz - 1)

                @pl.when(outer)
                def _():
                    arrived(self.buf.at[0, pl.ds(0, 1)], self.ss.at[2])

                @pl.when(jnp.logical_not(outer))
                def _():
                    arrived(self.buf.at[0, pl.ds(0, 5)], self.ss.at[2])

    owner_core = lax.rem((chip + 1) // 2, 2)
    q_slot = 2 * (chip // 2) + par

    def sup_chip(s):
        return 2 * s + lax.rem(s + par, 2)

    def q_copy(i):
        head = lax.rem(chip + i, n_chip)
        return q_ref.at[head], q_recv.at[q_slot], msg_ss.at[0], q_rs.at[q_slot // 2], 2 * head + owner_core

    def do_copy(i):
        head = lax.rem(chip + i, n_chip)
        return do_ref.at[head], do_recv.at[q_slot], msg_ss.at[1], do_rs.at[q_slot // 2], 2 * head + owner_core

    def o_copy(s, i):
        return o_send.at[2 * s + i], o_out.at[chip], msg_ss.at[2], msg_rs.at[0], 2 * sup_chip(s) + i

    def dq_copy(s, i):
        return dq_send.at[2 * s + i], dq_out.at[chip], msg_ss.at[3], msg_rs.at[1], 2 * sup_chip(s) + i

    def dv_copy(ch):
        return dv_msg.at[par, ch], dv_recv.at[chip], msg_ss.at[4], msg_rs.at[2], 2 * ch + par

    def dk_copy(ch):
        return dk_msg.at[par, ch], dk_recv.at[chip], msg_ss.at[5], msg_rs.at[3], 2 * ch + par

    gc = Gather(c_all, 144, 80, cg_rz, cg_rp, cg_ss, None)
    with scope("send_c"):
        c_all[par, chip, pl.ds(0, BLK), :] = c_ref[...]
        for i in range(4):
            c_all[par, chip, pl.ds(BLK, 16), pl.ds(128 * i, 128)] = rt_ref[pl.ds(16 * i, 16), :]
        gc.begin_chain()
        gc.pass_on()
    with scope("send_q"):
        def send_q(i):
            start(*q_copy(i))
            start(*do_copy(i))

        late = z >= nz // 2

        def lay_do(i):
            rows = pl.ds(pl.multiple_of(i * 32, 32), 32)
            do_ref[:, rows, :] = heads_first(do_raw[rows])

        loop(0, BLK // 32, lay_do)

        @pl.when(jnp.logical_not(late))
        def _():
            loop(0, n_chip, send_q)

    with scope("init"):
        dkr[...] = jnp.zeros_like(dkr)
        dv[...] = jnp.zeros_like(dv)
        for i in range(n_piece):
            w_copy(i).wait()

            def lay_w(r):
                w = heads_first(w_stage[i % 2, pl.ds(pl.multiple_of(r * 32, 32), 32)])
                rows = pl.ds(pl.multiple_of(i % (n_piece // 2) * BLK + r * 32, 32), 32)
                for h in range(n_chip):
                    w_big[rows, pl.ds(h * 256 + 128 * (i // (n_piece // 2)), 128)] = w[h]

            loop(0, BLK // 32, lay_w)
            if i + 2 < n_piece:
                w_copy(i + 2).start()
        wt_cat[...] = jnp.transpose(w_big[:, pl.ds(pl.multiple_of(chip * 256, 256), 256)].astype(F32)).astype(BF)
        qt[pl.ds(192, 64), :] = jnp.zeros((64, SUP), BF)

    def latent_of(ch):
        return jnp.concatenate([c_all[0, ch, pl.ds(0, BLK), :], c_all[1, ch, pl.ds(0, BLK), :]], axis=0)

    def up_project(ch):
        base = pl.multiple_of(ch * SUP, SUP)
        lat = latent_of(ch)
        kv = mm(lat, w_big[:, pl.ds(pl.multiple_of(chip * 256, 256), 256)]).astype(BF)
        kvt = mm(wt_cat[...], lat, NT).astype(BF)
        kr[pl.ds(base, SUP), pl.ds(0, 128)] = kv[:, :128]
        v[pl.ds(base, SUP), :] = kv[:, 128:]
        kt[pl.ds(0, 128), pl.ds(base, SUP)] = kvt[:128]
        vt[:, pl.ds(base, SUP)] = kvt[128:]
        for q in range(2):
            rt = jnp.concatenate([c_all[q, ch, pl.ds(BLK, 16), pl.ds(128 * i, 128)] for i in range(4)], axis=0)
            kt[pl.ds(128, 64), pl.ds(base + q * BLK, BLK)] = rt
            r = jnp.transpose(rt.astype(F32))
            kr[pl.ds(base + q * BLK, BLK), pl.ds(128, 128)] = jnp.concatenate(
                [r, jnp.zeros_like(r)], axis=1).astype(BF)

    diff = lax.broadcasted_iota(jnp.int32, (SUP, SUP), 0) - lax.broadcasted_iota(jnp.int32, (SUP, SUP), 1)

    def load_q(s):
        for i in range(2):
            qt[pl.ds(0, 192), pl.ds(i * BLK, BLK)] = q_recv[2 * s + i]
            dof[pl.ds(i * BLK, BLK), :] = do_recv[2 * s + i]

    def store_row(s):
        a = s // 2
        return (a + 1) * (a + s % 2) * CH

    def forward(s):
        ch = sup_chip(s)
        arrived(q_recv.at[pl.ds(2 * s, 2)], q_rs.at[s])
        arrived(do_recv.at[pl.ds(2 * s, 2)], do_rs.at[s])
        load_q(s)
        dot_[...] = jnp.transpose(dof[...].astype(F32))
        n_ch = s // 2 + 1

        def score(j, m8):
            for t in range(CH // SUP):
                r0 = pl.multiple_of(j * CH + t * SUP, SUP)
                st = mm(kr[pl.ds(r0, SUP), :], qt[...])
                st = jnp.where(diff <= ch * SUP - r0, st, NEG)
                s_buf[pl.ds(r0, SUP), :] = st
                m8 = jnp.maximum(m8, jnp.max(st.reshape(SUP // 8, 8, SUP), axis=0))
            return m8

        m8 = lax.fori_loop(0, n_ch, score, jnp.full((8, SUP), NEG, F32))
        m2 = jnp.max(m8, axis=0, keepdims=True) * c1
        ot[...] = jnp.zeros_like(ot)

        def values(j, l8):
            base = pl.multiple_of(j * CH, CH)
            for t in range(CH // SUP):
                p = jnp.exp2(s_buf[pl.ds(base + t * SUP, SUP), :] * c1 - m2)
                l8 = l8 + jnp.sum(p.reshape(SUP // 8, 8, SUP), axis=0)
                p_buf[pl.ds(t * SUP, SUP), :] = p.astype(BF)
            ot[...] += mm(vt[:, pl.ds(base, CH)], p_buf[...])
            return l8

        l8 = lax.fori_loop(0, n_ch, values, jnp.zeros((8, SUP), F32))
        l = jnp.sum(l8, axis=0, keepdims=True)
        o = ot[...] / l
        lse2 = m2 + jnp.log2(l)
        delta_s[s] = jnp.sum(o * dot_[...], axis=0, keepdims=True)
        o_rows = jnp.transpose(o)
        for i in range(2):
            o_send[2 * s + i] = o_rows[i * BLK:(i + 1) * BLK].astype(BF)
        for i in range(2):
            start(*o_copy(s, i))
        row0 = store_row(s)

        def values_grad(j):
            base = pl.multiple_of(j * CH, CH)
            for t in range(CH // SUP):
                rows = pl.ds(base + t * SUP, SUP)
                p = jnp.exp2(s_buf[rows, :] * c1 - lse2).astype(BF)
                p_store[pl.ds(pl.multiple_of(row0 + base + t * SUP, SUP), SUP), :] = p
                dv[rows, :] += mm(p, dof[...])

        loop(0, n_ch, values_grad)

    def backward(s):
        load_q(s)
        dqt[...] = jnp.zeros_like(dqt)
        row0 = store_row(s)
        delta = delta_s[s]

        def keys_grad(j):
            base = pl.multiple_of(j * CH, CH)
            for t in range(CH // SUP):
                rows = pl.ds(base + t * SUP, SUP)
                dp = mm(v[rows, :], dof[...], NT)
                p = p_store[pl.ds(pl.multiple_of(row0 + base + t * SUP, SUP), SUP), :].astype(F32)
                ds_buf[pl.ds(t * SUP, SUP), :] = (p * (dp - delta) * scale).astype(BF)
            for t in range(CH // SUP):
                rows = pl.ds(base + t * SUP, SUP)
                dkr[rows, :] += mm(ds_buf[pl.ds(t * SUP, SUP), :], qt[...], NT)
            dqt[...] += mm(kt[:, pl.ds(base, CH)], ds_buf[...])

        loop(0, s // 2 + 1, keys_grad)
        for i in range(2):
            dq_send[2 * s + i] = dqt[:, pl.ds(i * BLK, BLK)].astype(BF)
        for i in range(2):
            start(*dq_copy(s, i))

    def ready_c(zq):
        gc.pairs(zq)
        loop(zq * PLANE, (zq + 1) * PLANE, up_project)

    def col_ready(zq):
        gc.from_z_chain(zq)

    def step_c(k):
        if k < nz:
            col_ready(k)
        if 0 <= k - 1 < nz:
            gc.xy(k - 1)
        if 0 <= k - 2 < nz:
            gc.diag(k - 2)
            ready_c(k - 2)

    for k in range(nz + 2):
        with scope(f"c{k}"):
            step_c(k)
            if k < 2:
                @pl.when(late)
                def _():
                    loop(k * n_chip // 2, (k + 1) * n_chip // 2, send_q)

        if k >= 2:
            with scope(f"fwd{k - 2}"):
                loop(2 * (k - 2), 2 * (k - 2) + 2, forward)

    def head_dw(k, lo, hi, grads):
        def add(ch):
            base = pl.multiple_of(ch * SUP, SUP)
            g = jnp.transpose(grads(pl.ds(base, SUP))).astype(BF)
            dwt[k] += mm(g, latent_of(ch))

        loop(lo, hi, add)

    def dw_exchange(k):
        dw_msg[k] = jnp.transpose(dwt[k]).reshape(2, SUP, 128)
        c = remote(dw_msg.at[k, 1 - par], dw_part.at[k], pair_s.at[k], pair_r.at[k], partner)
        c.start()
        return c

    def dw_begin(k, c):
        c.wait_recv()
        dw_all[k, par, chip] = dw_msg[k, par] + dw_part[k]

    def dw_out_copy(k, q, h):
        dst = dwk_out if k == 0 else dwv_out
        return pltpu.make_async_copy(dw_all.at[k, q, h], dst.at[pl.ds(q * SUP, SUP), h, 0], dw_sem.at[k])

    def put_dw(k):
        def put(zq):
            for q in range(2):
                loop(zq * PLANE, (zq + 1) * PLANE, lambda h: dw_out_copy(k, q, h).start())

        return put

    dwt[...] = jnp.zeros_like(dwt)
    gv = Gather(dw_all.at[1], SUP, 128, v_rz, v_rp, v_ss, put_dw(1))
    gk = Gather(dw_all.at[0], SUP, 128, k_rz, k_rp, k_ss, put_dw(0))
    with scope("dv"):
        def dv_out(ch):
            for q in range(2):
                dv_msg[q, ch] = dv[pl.ds(pl.multiple_of(ch * SUP, SUP) + q * BLK, BLK), :].astype(BF)

        loop(0, n_chip, dv_out)
        pair_dv = remote(dv_msg.at[1 - par], dv_part, pair_s.at[2], pair_r.at[2], partner)
        pair_dv.start()
        head_dw(1, 0, n_chip, lambda rows: dv[rows, :])
        pair_dwv = dw_exchange(1)
        pair_dv.wait_recv()

        def dv_add(ch):
            dv_msg[par, ch] = (dv_msg[par, ch].astype(F32) + dv_part[ch].astype(F32)).astype(BF)

        loop(0, n_chip, dv_add)
        dw_begin(1, pair_dwv)
        gv.begin()

        def dv_send(i):
            start(*dv_copy(lax.rem(chip + i, n_chip)))

        loop(0, n_chip, dv_send)

    pair_dk = [remote(dk_msg.at[1 - par, pl.ds(PLANE * g, PLANE)], dk_part.at[pl.ds(PLANE * g, PLANE)],
                      pair_s.at[3 + g], pair_r.at[3 + g], partner) for g in range(nz)]

    def dk_out(g):
        def put(ch):
            for q in range(2):
                rows = pl.ds(pl.multiple_of(ch * SUP, SUP) + q * BLK, BLK)
                dk_msg[q, ch, pl.ds(0, BLK), :] = dkr[rows, pl.ds(0, 128)].astype(BF)
                dk_msg[q, ch, pl.ds(BLK, 64), :] = pack_rope(dkr[rows, pl.ds(128, 128)][:, :64]).astype(BF)

        loop(PLANE * g, PLANE * (g + 1), put)
        pair_dk[g].start()
        head_dw(0, PLANE * g, PLANE * (g + 1), lambda rows: dkr[rows, pl.ds(0, 128)])

    def dk_add(g):
        pair_dk[g].wait_recv()

        def put(ch):
            dk_msg[par, ch] = (dk_msg[par, ch].astype(F32) + dk_part[ch].astype(F32)).astype(BF)

        loop(PLANE * g, PLANE * (g + 1), put)

    for g in reversed(range(nz)):
        for s in (2 * g + 1, 2 * g):
            with scope(f"bwd{s}"):
                backward(s)
        if g + 1 < nz:
            with scope(f"dks{g + 1}"):
                dk_add(g + 1)
        with scope(f"dko{g}"):
            dk_out(g)
        if g == 1:
            with scope("vz"):
                for d in range(1, nz):
                    gv.at(d, gv.from_z)

    with scope("dwk"):
        pair_dwk = dw_exchange(0)
        dw_begin(0, pair_dwk)
        gk.begin_chain()
    with scope("dks0"):
        dk_add(0)

    def dk_quarter(k):
        loop(k * n_chip // nz, (k + 1) * n_chip // nz, lambda i: start(*dk_copy(lax.rem(chip + i, n_chip))))

    def k_step(d):
        with scope(f"kz{d}"):
            gk.at(d, gk.from_z_chain)
            dk_quarter(d - 1)
            if d == nz - 1:
                dk_quarter(d)

    with scope("vxy0"):
        gv.at(0, gv.xy)
    for d in range(nz):
        if d + 1 < nz:
            with scope(f"vxy{d + 1}"):
                gv.at(d + 1, gv.xy)
        if d == 0:
            with scope("kp"):
                gk.pass_on()
        with scope(f"vd{d}"):
            gv.at(d, gv.last)
        if d == 0:
            with scope("ofin"):
                arrived(o_out, msg_rs.at[0])

                def lay_o(i):
                    rows = pl.ds(pl.multiple_of(i * 32, 32), 32)
                    o_fin[rows] = heads_first(o_out[:, rows, :])

                loop(0, BLK // 32, lay_o)
        else:
            k_step(d)

    def latent_grad():
        with scope("dc"):
            arrived(dv_recv, msg_rs.at[2])
            arrived(dk_recv, msg_rs.at[3])
            dkv = jnp.concatenate([g for h in range(n_chip) for g in (dk_recv[h, pl.ds(0, BLK), :], dv_recv[h])], axis=1)
            dc_fin[...] = mm(dkv, w_big[...], NT).astype(BF)
            dr = dk_recv[0, pl.ds(BLK, 64), :].astype(F32)
            for h in range(1, n_chip):
                dr = dr + dk_recv[h, pl.ds(BLK, 64), :].astype(F32)
            dr_fin[...] = jnp.transpose(jnp.concatenate([dr[:, :64], dr[:, 64:]], axis=0)).astype(BF)

    with scope("kxy0"):
        gk.at(0, gk.xy)
    for d in range(nz):
        if d + 1 < nz:
            with scope(f"kxy{d + 1}"):
                gk.at(d + 1, gk.xy)
        if d == nz - 1:
            latent_grad()
        with scope(f"kd{d}"):
            gk.at(d, gk.last)

    with scope("drain"):
        arrived(dq_out, msg_rs.at[1])
        outs = [pltpu.make_async_copy(buf, dst, out_sem.at[i]) for i, (buf, dst) in enumerate(
            ((dq_out, dq_hbm), (o_fin, o_hbm), (dc_fin, dc_hbm), (dr_fin, dr_hbm)))]
        for c in outs:
            c.start()
        gc.finish(True)
        gv.finish(False)
        gk.finish(True)
        for c in [pair_dv, pair_dwv, pair_dwk] + pair_dk:
            c.wait_send()
        for k, buf in enumerate((q_recv, do_recv, o_out, dq_out)):
            @pl.when(owner_core == par)
            def _():
                arrived(buf.at[pl.ds(0, n_chip - 1)], msg_ss.at[k])

            @pl.when(owner_core != par)
            def _():
                arrived(buf, msg_ss.at[k])
        for k, buf in enumerate((dv_recv, dk_recv)):
            arrived(buf.at[pl.ds(0, n_chip - 1)], msg_ss.at[4 + k])
        for k in range(2):
            arrived(dw_all.at[k], dw_sem.at[k])
        for c in outs:
            c.wait()


def copy_kernel(*refs):
    n = len(RESULT_PIECES)
    src, dst, buf, (sem_in, sem_out) = refs[:n], refs[n:2 * n], refs[2 * n:3 * n], refs[3 * n:]
    ins, outs = [], []
    for a, b, c, pieces in zip(src, dst, buf, RESULT_PIECES):
        size = a.shape[0] // pieces
        for i in range(pieces):
            rows = pl.ds(i * size, size)
            ins.append(pltpu.make_async_copy(a.at[rows], c.at[rows], sem_in.at[len(ins)]))
            outs.append(pltpu.make_async_copy(c.at[rows], b.at[rows], sem_out.at[len(outs)]))
    for c in ins:
        c.start()
    for c, d in zip(ins, outs):
        c.wait()
        d.start()
    for d in outs:
        d.wait()


RESULT_PIECES = (1, 1, 1, 1, 4, 4)


def copy_results(*arrays):
    hbm = pl.BlockSpec(memory_space=pl.ANY)
    shapes = tuple(jax.ShapeDtypeStruct(a.shape, a.dtype) for a in arrays)
    dma = pltpu.SemaphoreType.DMA((sum(RESULT_PIECES),))
    return pl.pallas_call(
        copy_kernel, out_shape=shapes, in_specs=[hbm] * len(arrays), out_specs=(hbm,) * len(arrays),
        scratch_shapes=[pltpu.VMEM(a.shape, a.dtype) for a in arrays] + [dma, dma],
    )(*arrays)


def solution(mesh):
    n_dev = mesh.shape["cp"]
    n_chip = n_dev // 2
    nz = n_chip // PLANE
    seq = n_dev * BLK
    seq_spec = P("cp")

    def local_step(queries, latent, key_rope, w_uk, w_uv, d_out):
        vm = pl.BlockSpec(memory_space=pltpu.VMEM)
        hbm = pl.BlockSpec(memory_space=pl.ANY)
        dma = pltpu.SemaphoreType.DMA
        gather_sems = [dma((4, nz)), dma((nz,)), dma((3,))]
        o, dq, dc, dr, dwk, dwv = pl.pallas_call(
            functools.partial(kernel, nz, queries.shape[-1]),
            out_shape=(jax.ShapeDtypeStruct((BLK, n_chip, 128), BF),
                       jax.ShapeDtypeStruct((n_chip, 192, BLK), BF),
                       jax.ShapeDtypeStruct((BLK, 512), BF),
                       jax.ShapeDtypeStruct((64, BLK), BF),
                       jax.ShapeDtypeStruct((512, n_chip, 1, 128), F32),
                       jax.ShapeDtypeStruct((512, n_chip, 1, 128), F32)),
            in_specs=[vm] * 4 + [hbm] * 2,
            out_specs=(hbm,) * 6,
            scratch_shapes=[
                pltpu.VMEM((n_chip, BLK, 128), BF),
                pltpu.VMEM((n_chip, 192, BLK), BF),
                pltpu.VMEM((n_chip, BLK, 128), BF),
                pltpu.VMEM((n_chip, 192, 128), BF),
                pltpu.VMEM((BLK, n_chip, 128), BF),
                pltpu.VMEM((BLK, 512), BF),
                pltpu.VMEM((64, BLK), BF),
                pltpu.VMEM((n_chip, BLK, 128), BF),
                pltpu.VMEM((512, n_chip * 256), BF),
                pltpu.VMEM((2, BLK, n_chip, 128), BF),
                pltpu.VMEM((256, 512), BF),
                pltpu.VMEM((n_chip, 192, BLK), BF),
                pltpu.VMEM((n_chip, BLK, 128), BF),
                pltpu.VMEM((2, n_chip, 144, 512), BF),
                pltpu.VMEM((seq, 256), BF),
                pltpu.VMEM((seq, 128), BF),
                pltpu.VMEM((192, seq), BF),
                pltpu.VMEM((128, seq), BF),
                pltpu.VMEM((seq, SUP), F32),
                pltpu.VMEM((CH, SUP), BF),
                pltpu.VMEM((nz * (nz + 1) * CH, SUP), BF),
                pltpu.VMEM((CH, SUP), BF),
                pltpu.VMEM((seq, 256), F32),
                pltpu.VMEM((seq, 128), F32),
                pltpu.VMEM((256, SUP), BF),
                pltpu.VMEM((SUP, 128), BF),
                pltpu.VMEM((128, SUP), F32),
                pltpu.VMEM((128, SUP), F32),
                pltpu.VMEM((192, SUP), F32),
                pltpu.VMEM((8, SUP), F32),
                pltpu.VMEM((n_chip // 2, 1, SUP), F32),
                pltpu.VMEM((n_chip, BLK, 128), BF),
                pltpu.VMEM((n_chip, 192, BLK), BF),
                pltpu.VMEM((2, n_chip, BLK, 128), BF),
                pltpu.VMEM((n_chip, BLK, 128), BF),
                pltpu.VMEM((2, n_chip, 192, 128), BF),
                pltpu.VMEM((n_chip, 192, 128), BF),
                pltpu.VMEM((2, 128, 512), F32),
                pltpu.VMEM((2, 2, SUP, 128), F32),
                pltpu.VMEM((2, SUP, 128), F32),
                pltpu.VMEM((2, 2, n_chip, SUP, 128), F32),
            ] + [dma((6,)), dma((4,)), dma((n_chip // 2,)), dma((n_chip // 2,))] + [dma((3 + nz,)), dma((3 + nz,)), dma((2,)), dma((4,)), dma((2,))] + gather_sems * 3,
            compiler_params=pltpu.CompilerParams(
                collective_id=0, has_side_effects=True, vmem_limit_bytes=62 * 1024 * 1024),
        )(queries.transpose(1, 2, 0), d_out, latent, key_rope.T, w_uk, w_uv)
        o, dq, dc, dr, dwk, dwv = copy_results(
            o, dq, dc, dr, dwk.reshape(512, n_chip, 128), dwv.reshape(512, n_chip, 128))
        return o, dq.transpose(2, 0, 1), dc, dr.T, dwk, dwv

    return jax.shard_map(local_step, mesh=mesh,
                         in_specs=(seq_spec, seq_spec, seq_spec, P(), P(), seq_spec),
                         out_specs=(seq_spec, seq_spec, seq_spec, seq_spec, P(), P()),
                         check_vma=False)
```

```python
import functools
import math

import jax
import jax.numpy as jnp
from jax import lax
from jax.experimental import pallas as pl
from jax.experimental.pallas import tpu as pltpu
from jax.sharding import PartitionSpec as P

MESH = pl.DeviceIdType.MESH
NX, NY = 2, 2
PLANE = NX * NY
BLK = 128
SUP = 256
CH = SUP * PLANE
NEG = -1e30
NT = (((1,), (1,)), ((), ()))
NN = (((1,), (0,)), ((), ()))
BF, F32 = jnp.bfloat16, jnp.float32


def mm(a, b, dims=NN):
    return lax.dot_general(a, b, dims, preferred_element_type=F32)


def pack_rope(x):
    return jnp.concatenate([x[:64], x[64:]], axis=1)


def kernel(nz, qk_dim, q_ref, do_raw, c_ref, rt_ref, wk_hbm, wv_hbm,
           o_hbm, dq_hbm, dc_hbm, dr_hbm, dwk_out, dwv_out,
           o_out, dq_out, dv_recv, dk_recv, o_fin, dc_fin, dr_fin, do_ref,
           w_big, w_stage, wt_cat, q_recv, do_recv, c_all, kr, v, kt, vt, s_buf, p_buf, p_store, ds_buf, dkr, dv,
           qt, dof, dot_, ot, dqt, lse, delta_s, o_send, dq_send, dv_msg, dv_part, dk_msg, dk_part,
           dwt, dw_msg, dw_part, dw_all,
           msg_ss, msg_rs, q_rs, do_rs, pair_s, pair_r, dw_sem, out_sem, w_sem,
           cg_rz, cg_rp, cg_ss, v_rz, v_rp, v_ss, k_rz, k_rp, k_ss):
    n_chip = PLANE * nz
    n_dev = 2 * n_chip
    n_sup = n_chip // 2
    me = lax.axis_index("cp")
    chip, par = me // 2, me % 2
    partner = 2 * chip + (1 - par)
    x, y, z = chip % NX, (chip // NX) % NY, chip // PLANE
    scale = 1.0 / math.sqrt(qk_dim)
    c1 = scale * math.log2(math.e)
    scope = jax.named_scope

    def chip_at(zq, yq, xq):
        return (zq * NY + yq) * NX + xq

    def col_chip(col, zq):
        return chip_at(zq, 1 - y if col >= 2 else y, 1 - x if col % 2 else x)

    def remote(src, dst, ssem, rsem, dev):
        return pltpu.make_async_remote_copy(src_ref=src, dst_ref=dst, send_sem=ssem, recv_sem=rsem,
                                            device_id=(dev,), device_id_type=MESH)

    def start(src, dst, ssem, rsem, dev):
        @pl.when(dev == me)
        def _():
            pltpu.make_async_copy(src, dst, rsem).start()

        @pl.when(dev != me)
        def _():
            remote(src, dst, ssem, rsem, dev).start()

    def arrived(dst, rsem):
        pltpu.make_async_copy(dst, dst, rsem).wait()

    def loop(lo, hi, f):
        def body(i, carry):
            f(i)
            return carry

        lax.fori_loop(lo, hi, body, 0)

    n_piece = 8

    def w_copy(i):
        src = wk_hbm if i < n_piece // 2 else wv_hbm
        return pltpu.make_async_copy(src.at[pl.ds(i % (n_piece // 2) * BLK, BLK)], w_stage.at[i % 2], w_sem.at[i % 2])

    for i in range(2):
        w_copy(i).start()

    def heads_first(x):
        return jnp.transpose(x, (1, 0, 2))

    with scope("barrier"):
        barrier = pltpu.get_barrier_semaphore()
        loop(1, n_dev, lambda i: pl.semaphore_signal(
            barrier, inc=1, device_id=(lax.rem(me + i, n_dev),), device_id_type=MESH))
        pl.semaphore_wait(barrier, n_dev - 1)

    class Gather:
        def __init__(self, buf, rows, split, rz, rp, ss, ready):
            self.buf, self.rows, self.split = buf, rows, split
            self.rz, self.rp, self.ss, self.ready = rz, rp, ss, ready
            self.dev_x = 2 * chip_at(z, y, 1 - x) + par
            self.dev_y = 2 * chip_at(z, 1 - y, x) + par

        def blk(self, col, zq):
            return self.buf.at[par, col_chip(col, zq)]

        def along_z(self, zq, to):
            b = self.blk(0, zq)
            return remote(b, b, self.ss.at[0], self.rz.at[0, zq], 2 * chip_at(to, y, x) + par)

        def to_x(self, col, zq):
            b = self.blk(col, zq)
            return remote(b, b, self.ss.at[0], self.rz.at[1, zq], self.dev_x)

        def to_y(self, col, zq):
            b = self.blk(col, zq)
            return remote(b, b, self.ss.at[0], self.rz.at[2, zq], self.dev_y)

        def part_y(self, col, zq):
            b = self.blk(col, zq).at[pl.ds(0, self.split)]
            return remote(b, b, self.ss.at[0], self.rz.at[3, zq], self.dev_y)

        def part_x(self, col, zq):
            b = self.blk(col, zq).at[pl.ds(self.split, self.rows - self.split)]
            return remote(b, b, self.ss.at[0], self.rz.at[3, zq], self.dev_x)

        def pair(self, col, zq):
            b = self.blk(col, zq)
            return remote(b, b, self.ss.at[1], self.rp.at[zq], partner)

        def own_col(self, zq):
            self.to_x(0, zq).start()
            self.to_y(0, zq).start()
            self.pair(0, zq).start()

        def xy(self, zq):
            self.to_x(1, zq).wait_recv()
            self.part_y(1, zq).start()
            self.pair(1, zq).start()
            self.to_y(2, zq).wait_recv()
            self.part_x(2, zq).start()
            self.pair(2, zq).start()

        def diag(self, zq):
            arrived(self.blk(3, zq), self.rz.at[3, zq])
            self.pair(3, zq).start()

        def pairs(self, zq):
            arrived(self.buf.at[1 - par, pl.ds(zq * PLANE, PLANE)], self.rp.at[zq])

        def begin(self):
            for d in range(1, nz):
                @pl.when(z + d < nz)
                def _():
                    self.along_z(z, z + d).start()

                @pl.when(z - d >= 0)
                def _():
                    self.along_z(z, z - d).start()

            self.own_col(z)

        def from_z(self, zq):
            self.along_z(zq, z).wait_recv()
            self.own_col(zq)

        def at(self, d, f):
            if d == 0:
                f(z)
                return

            @pl.when(z - d >= 0)
            def _():
                f(z - d)

            @pl.when(z + d < nz)
            def _():
                f(z + d)

        def last(self, zq):
            self.diag(zq)
            self.pairs(zq)
            self.ready(zq)

        def steps(self, tag, before_last):
            for d in range(1, nz):
                with scope(f"{tag}z{d}"):
                    self.at(d, self.from_z)
                with scope(f"{tag}xy{d - 1}"):
                    self.at(d - 1, self.xy)
                if d >= 2:
                    with scope(f"{tag}d{d - 2}"):
                        self.at(d - 2, self.last)
            with scope(f"{tag}xy{nz - 1}"):
                self.at(nz - 1, self.xy)
            for d in range(max(nz - 2, 0), nz):
                if d == nz - 1:
                    before_last()
                with scope(f"{tag}d{d}"):
                    self.at(d, self.last)

        def finish(self):
            arrived(self.buf.at[0, pl.ds(0, n_chip - 1)], self.ss.at[0])
            arrived(self.buf.at[0], self.ss.at[1])

    owner_core = lax.rem((chip + 1) // 2, 2)
    q_slot = 2 * (chip // 2) + par

    def sup_chip(s):
        return 2 * s + lax.rem(s + par, 2)

    def q_copy(i):
        head = lax.rem(chip + i, n_chip)
        return q_ref.at[head], q_recv.at[q_slot], msg_ss.at[0], q_rs.at[q_slot // 2], 2 * head + owner_core

    def do_copy(i):
        head = lax.rem(chip + i, n_chip)
        return do_ref.at[head], do_recv.at[q_slot], msg_ss.at[1], do_rs.at[q_slot // 2], 2 * head + owner_core

    def o_copy(s, i):
        return o_send.at[2 * s + i], o_out.at[chip], msg_ss.at[2], msg_rs.at[0], 2 * sup_chip(s) + i

    def dq_copy(s, i):
        return dq_send.at[2 * s + i], dq_out.at[chip], msg_ss.at[3], msg_rs.at[1], 2 * sup_chip(s) + i

    def dv_copy(ch):
        return dv_msg.at[par, ch], dv_recv.at[chip], msg_ss.at[4], msg_rs.at[2], 2 * ch + par

    def dk_copy(ch):
        return dk_msg.at[par, ch], dk_recv.at[chip], msg_ss.at[5], msg_rs.at[3], 2 * ch + par

    gc = Gather(c_all, 144, 80, cg_rz, cg_rp, cg_ss, None)
    with scope("send_c"):
        c_all[par, chip, pl.ds(0, BLK), :] = c_ref[...]
        for i in range(4):
            c_all[par, chip, pl.ds(BLK, 16), pl.ds(128 * i, 128)] = rt_ref[pl.ds(16 * i, 16), :]
        gc.begin()
    with scope("send_q"):
        def send_q(i):
            start(*q_copy(i))
            start(*do_copy(i))

        late = z >= nz // 2

        def lay_do(i):
            rows = pl.ds(pl.multiple_of(i * 32, 32), 32)
            do_ref[:, rows, :] = heads_first(do_raw[rows])

        loop(0, BLK // 32, lay_do)

        @pl.when(jnp.logical_not(late))
        def _():
            loop(0, n_chip, send_q)

    with scope("init"):
        dkr[...] = jnp.zeros_like(dkr)
        dv[...] = jnp.zeros_like(dv)
        for i in range(n_piece):
            w_copy(i).wait()

            def lay_w(r):
                w = heads_first(w_stage[i % 2, pl.ds(pl.multiple_of(r * 32, 32), 32)])
                rows = pl.ds(pl.multiple_of(i % (n_piece // 2) * BLK + r * 32, 32), 32)
                for h in range(n_chip):
                    w_big[rows, pl.ds(h * 256 + 128 * (i // (n_piece // 2)), 128)] = w[h]

            loop(0, BLK // 32, lay_w)
            if i + 2 < n_piece:
                w_copy(i + 2).start()
        wt_cat[...] = jnp.transpose(w_big[:, pl.ds(pl.multiple_of(chip * 256, 256), 256)].astype(F32)).astype(BF)
        qt[pl.ds(192, 64), :] = jnp.zeros((64, SUP), BF)

    def latent_of(ch):
        return jnp.concatenate([c_all[0, ch, pl.ds(0, BLK), :], c_all[1, ch, pl.ds(0, BLK), :]], axis=0)

    def up_project(ch):
        base = pl.multiple_of(ch * SUP, SUP)
        lat = latent_of(ch)
        kv = mm(lat, w_big[:, pl.ds(pl.multiple_of(chip * 256, 256), 256)]).astype(BF)
        kvt = mm(wt_cat[...], lat, NT).astype(BF)
        kr[pl.ds(base, SUP), pl.ds(0, 128)] = kv[:, :128]
        v[pl.ds(base, SUP), :] = kv[:, 128:]
        kt[pl.ds(0, 128), pl.ds(base, SUP)] = kvt[:128]
        vt[:, pl.ds(base, SUP)] = kvt[128:]
        for q in range(2):
            rt = jnp.concatenate([c_all[q, ch, pl.ds(BLK, 16), pl.ds(128 * i, 128)] for i in range(4)], axis=0)
            kt[pl.ds(128, 64), pl.ds(base + q * BLK, BLK)] = rt
            r = jnp.transpose(rt.astype(F32))
            kr[pl.ds(base + q * BLK, BLK), pl.ds(128, 128)] = jnp.concatenate(
                [r, jnp.zeros_like(r)], axis=1).astype(BF)

    diff = lax.broadcasted_iota(jnp.int32, (SUP, SUP), 0) - lax.broadcasted_iota(jnp.int32, (SUP, SUP), 1)

    def load_q(s):
        for i in range(2):
            qt[pl.ds(0, 192), pl.ds(i * BLK, BLK)] = q_recv[2 * s + i]
            dof[pl.ds(i * BLK, BLK), :] = do_recv[2 * s + i]

    def store_row(s):
        a = s // 2
        return (a + 1) * (a + s % 2) * CH

    def forward(s):
        ch = sup_chip(s)
        arrived(q_recv.at[pl.ds(2 * s, 2)], q_rs.at[s])
        arrived(do_recv.at[pl.ds(2 * s, 2)], do_rs.at[s])
        load_q(s)
        dot_[...] = jnp.transpose(dof[...].astype(F32))
        n_ch = s // 2 + 1

        def score(j, m8):
            for t in range(CH // SUP):
                r0 = pl.multiple_of(j * CH + t * SUP, SUP)
                st = mm(kr[pl.ds(r0, SUP), :], qt[...])
                st = jnp.where(diff <= ch * SUP - r0, st, NEG)
                s_buf[pl.ds(r0, SUP), :] = st
                m8 = jnp.maximum(m8, jnp.max(st.reshape(SUP // 8, 8, SUP), axis=0))
            return m8

        m8 = lax.fori_loop(0, n_ch, score, jnp.full((8, SUP), NEG, F32))
        m2 = jnp.max(m8, axis=0, keepdims=True) * c1
        ot[...] = jnp.zeros_like(ot)

        def values(j, l8):
            base = pl.multiple_of(j * CH, CH)
            for t in range(CH // SUP):
                p = jnp.exp2(s_buf[pl.ds(base + t * SUP, SUP), :] * c1 - m2)
                l8 = l8 + jnp.sum(p.reshape(SUP // 8, 8, SUP), axis=0)
                p_buf[pl.ds(t * SUP, SUP), :] = p.astype(BF)
            ot[...] += mm(vt[:, pl.ds(base, CH)], p_buf[...])
            return l8

        l8 = lax.fori_loop(0, n_ch, values, jnp.zeros((8, SUP), F32))
        l = jnp.sum(l8, axis=0, keepdims=True)
        o = ot[...] / l
        lse2 = m2 + jnp.log2(l)
        delta_s[s] = jnp.sum(o * dot_[...], axis=0, keepdims=True)
        o_rows = jnp.transpose(o)
        for i in range(2):
            o_send[2 * s + i] = o_rows[i * BLK:(i + 1) * BLK].astype(BF)
        for i in range(2):
            start(*o_copy(s, i))
        row0 = store_row(s)

        def values_grad(j):
            base = pl.multiple_of(j * CH, CH)
            for t in range(CH // SUP):
                rows = pl.ds(base + t * SUP, SUP)
                p = jnp.exp2(s_buf[rows, :] * c1 - lse2).astype(BF)
                p_store[pl.ds(pl.multiple_of(row0 + base + t * SUP, SUP), SUP), :] = p
                dv[rows, :] += mm(p, dof[...])

        loop(0, n_ch, values_grad)

    def backward(s):
        load_q(s)
        dqt[...] = jnp.zeros_like(dqt)
        row0 = store_row(s)
        delta = delta_s[s]

        def keys_grad(j):
            base = pl.multiple_of(j * CH, CH)
            for t in range(CH // SUP):
                rows = pl.ds(base + t * SUP, SUP)
                dp = mm(v[rows, :], dof[...], NT)
                p = p_store[pl.ds(pl.multiple_of(row0 + base + t * SUP, SUP), SUP), :].astype(F32)
                ds_buf[pl.ds(t * SUP, SUP), :] = (p * (dp - delta) * scale).astype(BF)
            for t in range(CH // SUP):
                rows = pl.ds(base + t * SUP, SUP)
                dkr[rows, :] += mm(ds_buf[pl.ds(t * SUP, SUP), :], qt[...], NT)
            dqt[...] += mm(kt[:, pl.ds(base, CH)], ds_buf[...])

        loop(0, s // 2 + 1, keys_grad)
        for i in range(2):
            dq_send[2 * s + i] = dqt[:, pl.ds(i * BLK, BLK)].astype(BF)
        for i in range(2):
            start(*dq_copy(s, i))

    def ready_c(zq):
        gc.pairs(zq)
        loop(zq * PLANE, (zq + 1) * PLANE, up_project)

    def col_ready(zq):
        @pl.when(z != zq)
        def _():
            gc.from_z(zq)

    def step_c(k):
        if k < nz:
            col_ready(k)
        if 0 <= k - 1 < nz:
            gc.xy(k - 1)
        if 0 <= k - 2 < nz:
            gc.diag(k - 2)
            ready_c(k - 2)

    for k in range(nz + 2):
        with scope(f"c{k}"):
            step_c(k)
            if k < 2:
                @pl.when(late)
                def _():
                    loop(k * n_chip // 2, (k + 1) * n_chip // 2, send_q)

        if k >= 2:
            with scope(f"fwd{k - 2}"):
                loop(2 * (k - 2), 2 * (k - 2) + 2, forward)

    def head_dw(k, lo, hi, grads):
        def add(ch):
            base = pl.multiple_of(ch * SUP, SUP)
            g = jnp.transpose(grads(pl.ds(base, SUP))).astype(BF)
            dwt[k] += mm(g, latent_of(ch))

        loop(lo, hi, add)

    def dw_exchange(k):
        dw_msg[k] = jnp.transpose(dwt[k]).reshape(2, SUP, 128)
        c = remote(dw_msg.at[k, 1 - par], dw_part.at[k], pair_s.at[k], pair_r.at[k], partner)
        c.start()
        return c

    def dw_begin(k, c):
        c.wait_recv()
        dw_all[k, par, chip] = dw_msg[k, par] + dw_part[k]

    def dw_out_copy(k, q, h):
        dst = dwk_out if k == 0 else dwv_out
        return pltpu.make_async_copy(dw_all.at[k, q, h], dst.at[pl.ds(q * SUP, SUP), h, 0], dw_sem.at[k])

    def put_dw(k):
        def put(zq):
            for q in range(2):
                loop(zq * PLANE, (zq + 1) * PLANE, lambda h: dw_out_copy(k, q, h).start())

        return put

    dwt[...] = jnp.zeros_like(dwt)
    gv = Gather(dw_all.at[1], SUP, 128, v_rz, v_rp, v_ss, put_dw(1))
    gk = Gather(dw_all.at[0], SUP, 128, k_rz, k_rp, k_ss, put_dw(0))
    with scope("dv"):
        def dv_out(ch):
            for q in range(2):
                dv_msg[q, ch] = dv[pl.ds(pl.multiple_of(ch * SUP, SUP) + q * BLK, BLK), :].astype(BF)

        loop(0, n_chip, dv_out)
        pair_dv = remote(dv_msg.at[1 - par], dv_part, pair_s.at[2], pair_r.at[2], partner)
        pair_dv.start()
        head_dw(1, 0, n_chip, lambda rows: dv[rows, :])
        pair_dwv = dw_exchange(1)
        pair_dv.wait_recv()

        def dv_add(ch):
            dv_msg[par, ch] = (dv_msg[par, ch].astype(F32) + dv_part[ch].astype(F32)).astype(BF)

        loop(0, n_chip, dv_add)
        dw_begin(1, pair_dwv)
        gv.begin()

        def dv_send(i):
            start(*dv_copy(lax.rem(chip + i, n_chip)))

        loop(0, n_chip, dv_send)

    pair_dk = [remote(dk_msg.at[1 - par, pl.ds(PLANE * g, PLANE)], dk_part.at[pl.ds(PLANE * g, PLANE)],
                      pair_s.at[3 + g], pair_r.at[3 + g], partner) for g in range(nz)]

    def dk_out(g):
        def put(ch):
            for q in range(2):
                rows = pl.ds(pl.multiple_of(ch * SUP, SUP) + q * BLK, BLK)
                dk_msg[q, ch, pl.ds(0, BLK), :] = dkr[rows, pl.ds(0, 128)].astype(BF)
                dk_msg[q, ch, pl.ds(BLK, 64), :] = pack_rope(dkr[rows, pl.ds(128, 128)][:, :64]).astype(BF)

        loop(PLANE * g, PLANE * (g + 1), put)
        pair_dk[g].start()
        head_dw(0, PLANE * g, PLANE * (g + 1), lambda rows: dkr[rows, pl.ds(0, 128)])

    def dk_add(g):
        pair_dk[g].wait_recv()

        def put(ch):
            dk_msg[par, ch] = (dk_msg[par, ch].astype(F32) + dk_part[ch].astype(F32)).astype(BF)

        loop(PLANE * g, PLANE * (g + 1), put)

    for g in reversed(range(nz)):
        for s in (2 * g + 1, 2 * g):
            with scope(f"bwd{s}"):
                backward(s)
        if g + 1 < nz:
            with scope(f"dks{g + 1}"):
                dk_add(g + 1)
        with scope(f"dko{g}"):
            dk_out(g)
        if g == 1:
            with scope("vz1"):
                gv.at(1, gv.from_z)

    with scope("dwk"):
        pair_dwk = dw_exchange(0)
        dw_begin(0, pair_dwk)
        gk.begin()
    with scope("dks0"):
        dk_add(0)
    with scope("vz"):
        for d in range(2, nz):
            gv.at(d, gv.from_z)
    with scope("vxy0"):
        gv.at(0, gv.xy)
    for d in range(nz):
        if d + 1 < nz:
            with scope(f"vxy{d + 1}"):
                gv.at(d + 1, gv.xy)
        with scope(f"vd{d}"):
            gv.at(d, gv.last)
            loop(d * n_chip // nz, (d + 1) * n_chip // nz, lambda i: start(*dk_copy(lax.rem(chip + i, n_chip))))
        if d == 0:
            with scope("ofin"):
                arrived(o_out, msg_rs.at[0])

                def lay_o(i):
                    rows = pl.ds(pl.multiple_of(i * 32, 32), 32)
                    o_fin[rows] = heads_first(o_out[:, rows, :])

                loop(0, BLK // 32, lay_o)

    def latent_grad():
        with scope("dc"):
            arrived(dv_recv, msg_rs.at[2])
            arrived(dk_recv, msg_rs.at[3])
            dkv = jnp.concatenate([g for h in range(n_chip) for g in (dk_recv[h, pl.ds(0, BLK), :], dv_recv[h])], axis=1)
            dc_fin[...] = mm(dkv, w_big[...], NT).astype(BF)
            dr = dk_recv[0, pl.ds(BLK, 64), :].astype(F32)
            for h in range(1, n_chip):
                dr = dr + dk_recv[h, pl.ds(BLK, 64), :].astype(F32)
            dr_fin[...] = jnp.transpose(jnp.concatenate([dr[:, :64], dr[:, 64:]], axis=0)).astype(BF)

    gk.steps("k", latent_grad)

    with scope("drain"):
        arrived(dq_out, msg_rs.at[1])
        outs = [pltpu.make_async_copy(buf, dst, out_sem.at[i]) for i, (buf, dst) in enumerate(
            ((dq_out, dq_hbm), (o_fin, o_hbm), (dc_fin, dc_hbm), (dr_fin, dr_hbm)))]
        for c in outs:
            c.start()
        for g in (gc, gv, gk):
            g.finish()
        for c in [pair_dv, pair_dwv, pair_dwk] + pair_dk:
            c.wait_send()
        for k, buf in enumerate((q_recv, do_recv, o_out, dq_out)):
            @pl.when(owner_core == par)
            def _():
                arrived(buf.at[pl.ds(0, n_chip - 1)], msg_ss.at[k])

            @pl.when(owner_core != par)
            def _():
                arrived(buf, msg_ss.at[k])
        for k, buf in enumerate((dv_recv, dk_recv)):
            arrived(buf.at[pl.ds(0, n_chip - 1)], msg_ss.at[4 + k])
        for k in range(2):
            arrived(dw_all.at[k], dw_sem.at[k])
        for c in outs:
            c.wait()


def copy_kernel(*refs):
    n = len(RESULT_PIECES)
    src, dst, buf, (sem_in, sem_out) = refs[:n], refs[n:2 * n], refs[2 * n:3 * n], refs[3 * n:]
    ins, outs = [], []
    for a, b, c, pieces in zip(src, dst, buf, RESULT_PIECES):
        size = a.shape[0] // pieces
        for i in range(pieces):
            rows = pl.ds(i * size, size)
            ins.append(pltpu.make_async_copy(a.at[rows], c.at[rows], sem_in.at[len(ins)]))
            outs.append(pltpu.make_async_copy(c.at[rows], b.at[rows], sem_out.at[len(outs)]))
    for c in ins:
        c.start()
    for c, d in zip(ins, outs):
        c.wait()
        d.start()
    for d in outs:
        d.wait()


RESULT_PIECES = (1, 1, 1, 1, 4, 4)


def copy_results(*arrays):
    hbm = pl.BlockSpec(memory_space=pl.ANY)
    shapes = tuple(jax.ShapeDtypeStruct(a.shape, a.dtype) for a in arrays)
    dma = pltpu.SemaphoreType.DMA((sum(RESULT_PIECES),))
    return pl.pallas_call(
        copy_kernel, out_shape=shapes, in_specs=[hbm] * len(arrays), out_specs=(hbm,) * len(arrays),
        scratch_shapes=[pltpu.VMEM(a.shape, a.dtype) for a in arrays] + [dma, dma],
    )(*arrays)


def solution(mesh):
    n_dev = mesh.shape["cp"]
    n_chip = n_dev // 2
    nz = n_chip // PLANE
    seq = n_dev * BLK
    seq_spec = P("cp")

    def local_step(queries, latent, key_rope, w_uk, w_uv, d_out):
        vm = pl.BlockSpec(memory_space=pltpu.VMEM)
        hbm = pl.BlockSpec(memory_space=pl.ANY)
        dma = pltpu.SemaphoreType.DMA
        gather_sems = [dma((4, nz)), dma((nz,)), dma((2,))]
        o, dq, dc, dr, dwk, dwv = pl.pallas_call(
            functools.partial(kernel, nz, queries.shape[-1]),
            out_shape=(jax.ShapeDtypeStruct((BLK, n_chip, 128), BF),
                       jax.ShapeDtypeStruct((n_chip, 192, BLK), BF),
                       jax.ShapeDtypeStruct((BLK, 512), BF),
                       jax.ShapeDtypeStruct((64, BLK), BF),
                       jax.ShapeDtypeStruct((512, n_chip, 1, 128), F32),
                       jax.ShapeDtypeStruct((512, n_chip, 1, 128), F32)),
            in_specs=[vm] * 4 + [hbm] * 2,
            out_specs=(hbm,) * 6,
            scratch_shapes=[
                pltpu.VMEM((n_chip, BLK, 128), BF),
                pltpu.VMEM((n_chip, 192, BLK), BF),
                pltpu.VMEM((n_chip, BLK, 128), BF),
                pltpu.VMEM((n_chip, 192, 128), BF),
                pltpu.VMEM((BLK, n_chip, 128), BF),
                pltpu.VMEM((BLK, 512), BF),
                pltpu.VMEM((64, BLK), BF),
                pltpu.VMEM((n_chip, BLK, 128), BF),
                pltpu.VMEM((512, n_chip * 256), BF),
                pltpu.VMEM((2, BLK, n_chip, 128), BF),
                pltpu.VMEM((256, 512), BF),
                pltpu.VMEM((n_chip, 192, BLK), BF),
                pltpu.VMEM((n_chip, BLK, 128), BF),
                pltpu.VMEM((2, n_chip, 144, 512), BF),
                pltpu.VMEM((seq, 256), BF),
                pltpu.VMEM((seq, 128), BF),
                pltpu.VMEM((192, seq), BF),
                pltpu.VMEM((128, seq), BF),
                pltpu.VMEM((seq, SUP), F32),
                pltpu.VMEM((CH, SUP), BF),
                pltpu.VMEM((nz * (nz + 1) * CH, SUP), BF),
                pltpu.VMEM((CH, SUP), BF),
                pltpu.VMEM((seq, 256), F32),
                pltpu.VMEM((seq, 128), F32),
                pltpu.VMEM((256, SUP), BF),
                pltpu.VMEM((SUP, 128), BF),
                pltpu.VMEM((128, SUP), F32),
                pltpu.VMEM((128, SUP), F32),
                pltpu.VMEM((192, SUP), F32),
                pltpu.VMEM((8, SUP), F32),
                pltpu.VMEM((n_chip // 2, 1, SUP), F32),
                pltpu.VMEM((n_chip, BLK, 128), BF),
                pltpu.VMEM((n_chip, 192, BLK), BF),
                pltpu.VMEM((2, n_chip, BLK, 128), BF),
                pltpu.VMEM((n_chip, BLK, 128), BF),
                pltpu.VMEM((2, n_chip, 192, 128), BF),
                pltpu.VMEM((n_chip, 192, 128), BF),
                pltpu.VMEM((2, 128, 512), F32),
                pltpu.VMEM((2, 2, SUP, 128), F32),
                pltpu.VMEM((2, SUP, 128), F32),
                pltpu.VMEM((2, 2, n_chip, SUP, 128), F32),
            ] + [dma((6,)), dma((4,)), dma((n_chip // 2,)), dma((n_chip // 2,))] + [dma((3 + nz,)), dma((3 + nz,)), dma((2,)), dma((4,)), dma((2,))] + gather_sems * 3,
            compiler_params=pltpu.CompilerParams(
                collective_id=0, has_side_effects=True, vmem_limit_bytes=62 * 1024 * 1024),
        )(queries.transpose(1, 2, 0), d_out, latent, key_rope.T, w_uk, w_uv)
        o, dq, dc, dr, dwk, dwv = copy_results(
            o, dq, dc, dr, dwk.reshape(512, n_chip, 128), dwv.reshape(512, n_chip, 128))
        return o, dq.transpose(2, 0, 1), dc, dr.T, dwk, dwv

    return jax.shard_map(local_step, mesh=mesh,
                         in_specs=(seq_spec, seq_spec, seq_spec, P(), P(), seq_spec),
                         out_specs=(seq_spec, seq_spec, seq_spec, seq_spec, P(), P()),
                         check_vma=False)
```

```python
import functools
import math

import jax
import jax.numpy as jnp
from jax import lax
from jax.experimental import pallas as pl
from jax.experimental.pallas import tpu as pltpu
from jax.sharding import PartitionSpec as P

MESH = pl.DeviceIdType.MESH
NX, NY = 2, 2
PLANE = NX * NY
BLK = 128
SUP = 256
CH = SUP * PLANE
NEG = -1e30
NT = (((1,), (1,)), ((), ()))
NN = (((1,), (0,)), ((), ()))
BF, F32 = jnp.bfloat16, jnp.float32


def mm(a, b, dims=NN):
    return lax.dot_general(a, b, dims, preferred_element_type=F32)


def pack_rope(x):
    return jnp.concatenate([x[:64], x[64:]], axis=1)


def kernel(nz, qk_dim, q_ref, do_raw, c_ref, rt_ref, wk_hbm, wv_hbm,
           o_hbm, dq_hbm, dc_hbm, dr_hbm, dwk_out, dwv_out,
           o_out, dq_out, dv_recv, dk_recv, o_fin, dc_fin, dr_fin, do_ref,
           w_big, w_stage, wt_cat, q_recv, do_recv, c_all, kr, v, kt, vt, s_buf, p_buf, p_store, ds_buf, dkr, dv,
           qt, dof, dot_, ot, dqt, lse, delta_s, o_send, dq_send, dv_msg, dv_part, dk_msg, dk_part,
           dwt, dw_msg, dw_part, dw_all,
           msg_ss, msg_rs, q_rs, do_rs, pair_s, pair_r, dw_sem, out_sem, w_sem,
           cg_rz, cg_rp, cg_ss, v_rz, v_rp, v_ss, k_rz, k_rp, k_ss):
    n_chip = PLANE * nz
    n_dev = 2 * n_chip
    n_sup = n_chip // 2
    me = lax.axis_index("cp")
    chip, par = me // 2, me % 2
    partner = 2 * chip + (1 - par)
    x, y, z = chip % NX, (chip // NX) % NY, chip // PLANE
    scale = 1.0 / math.sqrt(qk_dim)
    c1 = scale * math.log2(math.e)
    scope = jax.named_scope

    def chip_at(zq, yq, xq):
        return (zq * NY + yq) * NX + xq

    def col_chip(col, zq):
        return chip_at(zq, 1 - y if col >= 2 else y, 1 - x if col % 2 else x)

    def remote(src, dst, ssem, rsem, dev):
        return pltpu.make_async_remote_copy(src_ref=src, dst_ref=dst, send_sem=ssem, recv_sem=rsem,
                                            device_id=(dev,), device_id_type=MESH)

    def start(src, dst, ssem, rsem, dev):
        @pl.when(dev == me)
        def _():
            pltpu.make_async_copy(src, dst, rsem).start()

        @pl.when(dev != me)
        def _():
            remote(src, dst, ssem, rsem, dev).start()

    def arrived(dst, rsem):
        pltpu.make_async_copy(dst, dst, rsem).wait()

    def loop(lo, hi, f):
        def body(i, carry):
            f(i)
            return carry

        lax.fori_loop(lo, hi, body, 0)

    n_piece = 8

    def w_copy(i):
        src = wk_hbm if i < n_piece // 2 else wv_hbm
        return pltpu.make_async_copy(src.at[pl.ds(i % (n_piece // 2) * BLK, BLK)], w_stage.at[i % 2], w_sem.at[i % 2])

    for i in range(2):
        w_copy(i).start()

    def heads_first(x):
        return jnp.transpose(x, (1, 0, 2))

    with scope("barrier"):
        barrier = pltpu.get_barrier_semaphore()
        loop(1, n_dev, lambda i: pl.semaphore_signal(
            barrier, inc=1, device_id=(lax.rem(me + i, n_dev),), device_id_type=MESH))
        pl.semaphore_wait(barrier, n_dev - 1)

    class Gather:
        def __init__(self, buf, rows, split, rz, rp, ss, ready):
            self.buf, self.rows, self.split = buf, rows, split
            self.rz, self.rp, self.ss, self.ready = rz, rp, ss, ready
            self.dev_x = 2 * chip_at(z, y, 1 - x) + par
            self.dev_y = 2 * chip_at(z, 1 - y, x) + par

        def blk(self, col, zq):
            return self.buf.at[par, col_chip(col, zq)]

        def along_z(self, zq, to):
            b = self.blk(0, zq)
            return remote(b, b, self.ss.at[0], self.rz.at[0, zq], 2 * chip_at(to, y, x) + par)

        def to_x(self, col, zq):
            b = self.blk(col, zq)
            return remote(b, b, self.ss.at[0], self.rz.at[1, zq], self.dev_x)

        def to_y(self, col, zq):
            b = self.blk(col, zq)
            return remote(b, b, self.ss.at[0], self.rz.at[2, zq], self.dev_y)

        def part_y(self, col, zq):
            b = self.blk(col, zq).at[pl.ds(0, self.split)]
            return remote(b, b, self.ss.at[0], self.rz.at[3, zq], self.dev_y)

        def part_x(self, col, zq):
            b = self.blk(col, zq).at[pl.ds(self.split, self.rows - self.split)]
            return remote(b, b, self.ss.at[0], self.rz.at[3, zq], self.dev_x)

        def pair(self, col, zq):
            b = self.blk(col, zq)
            return remote(b, b, self.ss.at[1], self.rp.at[zq], partner)

        def own_col(self, zq):
            self.to_x(0, zq).start()
            self.to_y(0, zq).start()
            self.pair(0, zq).start()

        def xy(self, zq):
            self.to_x(1, zq).wait_recv()
            self.part_y(1, zq).start()
            self.pair(1, zq).start()
            self.to_y(2, zq).wait_recv()
            self.part_x(2, zq).start()
            self.pair(2, zq).start()

        def diag(self, zq):
            arrived(self.blk(3, zq), self.rz.at[3, zq])
            self.pair(3, zq).start()

        def pairs(self, zq):
            arrived(self.buf.at[1 - par, pl.ds(zq * PLANE, PLANE)], self.rp.at[zq])

        def begin(self):
            for d in range(1, nz):
                @pl.when(z + d < nz)
                def _():
                    self.along_z(z, z + d).start()

                @pl.when(z - d >= 0)
                def _():
                    self.along_z(z, z - d).start()

            self.own_col(z)

        def from_z(self, zq):
            self.along_z(zq, z).wait_recv()
            self.own_col(zq)

        def at(self, d, f):
            if d == 0:
                f(z)
                return

            @pl.when(z - d >= 0)
            def _():
                f(z - d)

            @pl.when(z + d < nz)
            def _():
                f(z + d)

        def last(self, zq):
            self.diag(zq)
            self.pairs(zq)
            self.ready(zq)

        def steps(self, tag, before_last):
            for d in range(1, nz):
                with scope(f"{tag}z{d}"):
                    self.at(d, self.from_z)
                with scope(f"{tag}xy{d - 1}"):
                    self.at(d - 1, self.xy)
                if d >= 2:
                    with scope(f"{tag}d{d - 2}"):
                        self.at(d - 2, self.last)
            with scope(f"{tag}xy{nz - 1}"):
                self.at(nz - 1, self.xy)
            for d in range(max(nz - 2, 0), nz):
                if d == nz - 1:
                    before_last()
                with scope(f"{tag}d{d}"):
                    self.at(d, self.last)

        def finish(self):
            arrived(self.buf.at[0, pl.ds(0, n_chip - 1)], self.ss.at[0])
            arrived(self.buf.at[0], self.ss.at[1])

    owner_core = lax.rem((chip + 1) // 2, 2)
    q_slot = 2 * (chip // 2) + par

    def sup_chip(s):
        return 2 * s + lax.rem(s + par, 2)

    def q_copy(i):
        head = lax.rem(chip + i, n_chip)
        return q_ref.at[head], q_recv.at[q_slot], msg_ss.at[0], q_rs.at[q_slot // 2], 2 * head + owner_core

    def do_copy(i):
        head = lax.rem(chip + i, n_chip)
        return do_ref.at[head], do_recv.at[q_slot], msg_ss.at[1], do_rs.at[q_slot // 2], 2 * head + owner_core

    def o_copy(s, i):
        return o_send.at[2 * s + i], o_out.at[chip], msg_ss.at[2], msg_rs.at[0], 2 * sup_chip(s) + i

    def dq_copy(s, i):
        return dq_send.at[2 * s + i], dq_out.at[chip], msg_ss.at[3], msg_rs.at[1], 2 * sup_chip(s) + i

    def dv_copy(ch):
        return dv_msg.at[par, ch], dv_recv.at[chip], msg_ss.at[4], msg_rs.at[2], 2 * ch + par

    def dk_copy(ch):
        return dk_msg.at[par, ch], dk_recv.at[chip], msg_ss.at[5], msg_rs.at[3], 2 * ch + par

    gc = Gather(c_all, 144, 80, cg_rz, cg_rp, cg_ss, None)
    with scope("send_c"):
        c_all[par, chip, pl.ds(0, BLK), :] = c_ref[...]
        for i in range(4):
            c_all[par, chip, pl.ds(BLK, 16), pl.ds(128 * i, 128)] = rt_ref[pl.ds(16 * i, 16), :]
        gc.begin()
    with scope("send_q"):
        def send_q(i):
            start(*q_copy(i))
            start(*do_copy(i))

        late = z >= nz // 2

        def lay_do(i):
            rows = pl.ds(pl.multiple_of(i * 32, 32), 32)
            do_ref[:, rows, :] = heads_first(do_raw[rows])

        loop(0, BLK // 32, lay_do)

        @pl.when(jnp.logical_not(late))
        def _():
            loop(0, n_chip, send_q)

    with scope("init"):
        dkr[...] = jnp.zeros_like(dkr)
        dv[...] = jnp.zeros_like(dv)
        for i in range(n_piece):
            w_copy(i).wait()

            def lay_w(r):
                w = heads_first(w_stage[i % 2, pl.ds(pl.multiple_of(r * 32, 32), 32)])
                rows = pl.ds(pl.multiple_of(i % (n_piece // 2) * BLK + r * 32, 32), 32)
                for h in range(n_chip):
                    w_big[rows, pl.ds(h * 256 + 128 * (i // (n_piece // 2)), 128)] = w[h]

            loop(0, BLK // 32, lay_w)
            if i + 2 < n_piece:
                w_copy(i + 2).start()
        wt_cat[...] = jnp.transpose(w_big[:, pl.ds(pl.multiple_of(chip * 256, 256), 256)].astype(F32)).astype(BF)
        qt[pl.ds(192, 64), :] = jnp.zeros((64, SUP), BF)

    def latent_of(ch):
        return jnp.concatenate([c_all[0, ch, pl.ds(0, BLK), :], c_all[1, ch, pl.ds(0, BLK), :]], axis=0)

    def up_project(ch):
        base = pl.multiple_of(ch * SUP, SUP)
        lat = latent_of(ch)
        kv = mm(lat, w_big[:, pl.ds(pl.multiple_of(chip * 256, 256), 256)]).astype(BF)
        kvt = mm(wt_cat[...], lat, NT).astype(BF)
        kr[pl.ds(base, SUP), pl.ds(0, 128)] = kv[:, :128]
        v[pl.ds(base, SUP), :] = kv[:, 128:]
        kt[pl.ds(0, 128), pl.ds(base, SUP)] = kvt[:128]
        vt[:, pl.ds(base, SUP)] = kvt[128:]
        for q in range(2):
            rt = jnp.concatenate([c_all[q, ch, pl.ds(BLK, 16), pl.ds(128 * i, 128)] for i in range(4)], axis=0)
            kt[pl.ds(128, 64), pl.ds(base + q * BLK, BLK)] = rt
            r = jnp.transpose(rt.astype(F32))
            kr[pl.ds(base + q * BLK, BLK), pl.ds(128, 128)] = jnp.concatenate(
                [r, jnp.zeros_like(r)], axis=1).astype(BF)

    diff = lax.broadcasted_iota(jnp.int32, (SUP, SUP), 0) - lax.broadcasted_iota(jnp.int32, (SUP, SUP), 1)

    def load_q(s):
        for i in range(2):
            qt[pl.ds(0, 192), pl.ds(i * BLK, BLK)] = q_recv[2 * s + i]
            dof[pl.ds(i * BLK, BLK), :] = do_recv[2 * s + i]

    def store_row(s):
        a = s // 2
        return (a + 1) * (a + s % 2) * CH

    def forward(s):
        ch = sup_chip(s)
        arrived(q_recv.at[pl.ds(2 * s, 2)], q_rs.at[s])
        arrived(do_recv.at[pl.ds(2 * s, 2)], do_rs.at[s])
        load_q(s)
        dot_[...] = jnp.transpose(dof[...].astype(F32))
        n_ch = s // 2 + 1

        def score(j, m8):
            for t in range(CH // SUP):
                r0 = pl.multiple_of(j * CH + t * SUP, SUP)
                st = mm(kr[pl.ds(r0, SUP), :], qt[...])
                st = jnp.where(diff <= ch * SUP - r0, st, NEG)
                s_buf[pl.ds(r0, SUP), :] = st
                m8 = jnp.maximum(m8, jnp.max(st.reshape(SUP // 8, 8, SUP), axis=0))
            return m8

        m8 = lax.fori_loop(0, n_ch, score, jnp.full((8, SUP), NEG, F32))
        m2 = jnp.max(m8, axis=0, keepdims=True) * c1
        ot[...] = jnp.zeros_like(ot)

        def values(j, l8):
            base = pl.multiple_of(j * CH, CH)
            for t in range(CH // SUP):
                p = jnp.exp2(s_buf[pl.ds(base + t * SUP, SUP), :] * c1 - m2)
                l8 = l8 + jnp.sum(p.reshape(SUP // 8, 8, SUP), axis=0)
                p_buf[pl.ds(t * SUP, SUP), :] = p.astype(BF)
            ot[...] += mm(vt[:, pl.ds(base, CH)], p_buf[...])
            return l8

        l8 = lax.fori_loop(0, n_ch, values, jnp.zeros((8, SUP), F32))
        l = jnp.sum(l8, axis=0, keepdims=True)
        o = ot[...] / l
        lse2 = m2 + jnp.log2(l)
        delta_s[s] = jnp.sum(o * dot_[...], axis=0, keepdims=True)
        o_rows = jnp.transpose(o)
        for i in range(2):
            o_send[2 * s + i] = o_rows[i * BLK:(i + 1) * BLK].astype(BF)
        for i in range(2):
            start(*o_copy(s, i))
        row0 = store_row(s)

        def values_grad(j):
            base = pl.multiple_of(j * CH, CH)
            for t in range(CH // SUP):
                rows = pl.ds(base + t * SUP, SUP)
                p = jnp.exp2(s_buf[rows, :] * c1 - lse2).astype(BF)
                p_store[pl.ds(pl.multiple_of(row0 + base + t * SUP, SUP), SUP), :] = p
                dv[rows, :] += mm(p, dof[...])

        loop(0, n_ch, values_grad)

    def send_dq(s):
        for i in range(2):
            start(*dq_copy(s, i))

    def backward(s):
        load_q(s)
        dqt[...] = jnp.zeros_like(dqt)
        row0 = store_row(s)
        delta = delta_s[s]

        def keys_grad(j):
            base = pl.multiple_of(j * CH, CH)
            for t in range(CH // SUP):
                rows = pl.ds(base + t * SUP, SUP)
                dp = mm(v[rows, :], dof[...], NT)
                p = p_store[pl.ds(pl.multiple_of(row0 + base + t * SUP, SUP), SUP), :].astype(F32)
                ds_buf[pl.ds(t * SUP, SUP), :] = (p * (dp - delta) * scale).astype(BF)
            for t in range(CH // SUP):
                rows = pl.ds(base + t * SUP, SUP)
                dkr[rows, :] += mm(ds_buf[pl.ds(t * SUP, SUP), :], qt[...], NT)
            dqt[...] += mm(kt[:, pl.ds(base, CH)], ds_buf[...])

        loop(0, s // 2 + 1, keys_grad)
        for i in range(2):
            dq_send[2 * s + i] = dqt[:, pl.ds(i * BLK, BLK)].astype(BF)
        if s >= n_sup // 2:
            send_dq(s)

    def ready_c(zq):
        gc.pairs(zq)
        loop(zq * PLANE, (zq + 1) * PLANE, up_project)

    def col_ready(zq):
        @pl.when(z != zq)
        def _():
            gc.from_z(zq)

    def step_c(k):
        if k < nz:
            col_ready(k)
        if 0 <= k - 1 < nz:
            gc.xy(k - 1)
        if 0 <= k - 2 < nz:
            gc.diag(k - 2)
            ready_c(k - 2)

    for k in range(nz + 2):
        with scope(f"c{k}"):
            step_c(k)
            if k < 2:
                @pl.when(late)
                def _():
                    loop(k * n_chip // 2, (k + 1) * n_chip // 2, send_q)

        if k >= 2:
            with scope(f"fwd{k - 2}"):
                loop(2 * (k - 2), 2 * (k - 2) + 2, forward)

    def head_dw(k, lo, hi, grads):
        def add(ch):
            base = pl.multiple_of(ch * SUP, SUP)
            g = jnp.transpose(grads(pl.ds(base, SUP))).astype(BF)
            dwt[k] += mm(g, latent_of(ch))

        loop(lo, hi, add)

    def dw_exchange(k):
        dw_msg[k] = jnp.transpose(dwt[k]).reshape(2, SUP, 128)
        c = remote(dw_msg.at[k, 1 - par], dw_part.at[k], pair_s.at[k], pair_r.at[k], partner)
        c.start()
        return c

    def dw_begin(k, c):
        c.wait_recv()
        dw_all[k, par, chip] = dw_msg[k, par] + dw_part[k]

    def dw_out_copy(k, q, h):
        dst = dwk_out if k == 0 else dwv_out
        return pltpu.make_async_copy(dw_all.at[k, q, h], dst.at[pl.ds(q * SUP, SUP), h, 0], dw_sem.at[k])

    def put_dw(k):
        def put(zq):
            for q in range(2):
                loop(zq * PLANE, (zq + 1) * PLANE, lambda h: dw_out_copy(k, q, h).start())

        return put

    dwt[...] = jnp.zeros_like(dwt)
    gv = Gather(dw_all.at[1], SUP, 128, v_rz, v_rp, v_ss, put_dw(1))
    gk = Gather(dw_all.at[0], SUP, 128, k_rz, k_rp, k_ss, put_dw(0))
    with scope("dv"):
        def dv_out(ch):
            for q in range(2):
                dv_msg[q, ch] = dv[pl.ds(pl.multiple_of(ch * SUP, SUP) + q * BLK, BLK), :].astype(BF)

        loop(0, n_chip, dv_out)
        pair_dv = remote(dv_msg.at[1 - par], dv_part, pair_s.at[2], pair_r.at[2], partner)
        pair_dv.start()
        head_dw(1, 0, n_chip, lambda rows: dv[rows, :])
        pair_dwv = dw_exchange(1)
        pair_dv.wait_recv()

        def dv_add(ch):
            dv_msg[par, ch] = (dv_msg[par, ch].astype(F32) + dv_part[ch].astype(F32)).astype(BF)

        loop(0, n_chip, dv_add)
        dw_begin(1, pair_dwv)
        gv.begin()

        def dv_send(i):
            start(*dv_copy(lax.rem(chip + i, n_chip)))

        loop(0, n_chip, dv_send)

    pair_dk = [remote(dk_msg.at[1 - par, pl.ds(PLANE * g, PLANE)], dk_part.at[pl.ds(PLANE * g, PLANE)],
                      pair_s.at[3 + g], pair_r.at[3 + g], partner) for g in range(nz)]

    def dk_out(g):
        def put(ch):
            for q in range(2):
                rows = pl.ds(pl.multiple_of(ch * SUP, SUP) + q * BLK, BLK)
                dk_msg[q, ch, pl.ds(0, BLK), :] = dkr[rows, pl.ds(0, 128)].astype(BF)
                dk_msg[q, ch, pl.ds(BLK, 64), :] = pack_rope(dkr[rows, pl.ds(128, 128)][:, :64]).astype(BF)

        loop(PLANE * g, PLANE * (g + 1), put)
        pair_dk[g].start()
        head_dw(0, PLANE * g, PLANE * (g + 1), lambda rows: dkr[rows, pl.ds(0, 128)])

    def dk_add(g):
        pair_dk[g].wait_recv()

        def put(ch):
            dk_msg[par, ch] = (dk_msg[par, ch].astype(F32) + dk_part[ch].astype(F32)).astype(BF)

        loop(PLANE * g, PLANE * (g + 1), put)

    for g in reversed(range(nz)):
        for s in (2 * g + 1, 2 * g):
            with scope(f"bwd{s}"):
                backward(s)
        if g + 1 < nz:
            with scope(f"dks{g + 1}"):
                dk_add(g + 1)
        with scope(f"dko{g}"):
            dk_out(g)
        if g == 1:
            with scope("vz1"):
                gv.at(1, gv.from_z)

    with scope("dwk"):
        pair_dwk = dw_exchange(0)
        dw_begin(0, pair_dwk)
        gk.begin()
    with scope("dks0"):
        dk_add(0)
    with scope("vz"):
        for d in range(2, nz):
            gv.at(d, gv.from_z)
        for s in reversed(range(n_sup // 2)):
            send_dq(s)
    with scope("vxy0"):
        gv.at(0, gv.xy)
    for d in range(nz):
        if d + 1 < nz:
            with scope(f"vxy{d + 1}"):
                gv.at(d + 1, gv.xy)
        with scope(f"vd{d}"):
            gv.at(d, gv.last)
            loop(d * n_chip // nz, (d + 1) * n_chip // nz, lambda i: start(*dk_copy(lax.rem(chip + i, n_chip))))
        if d == 0:
            with scope("ofin"):
                arrived(o_out, msg_rs.at[0])

                def lay_o(i):
                    rows = pl.ds(pl.multiple_of(i * 32, 32), 32)
                    o_fin[rows] = heads_first(o_out[:, rows, :])

                loop(0, BLK // 32, lay_o)

    def latent_grad():
        with scope("dc"):
            arrived(dv_recv, msg_rs.at[2])
            arrived(dk_recv, msg_rs.at[3])
            dkv = jnp.concatenate([g for h in range(n_chip) for g in (dk_recv[h, pl.ds(0, BLK), :], dv_recv[h])], axis=1)
            dc_fin[...] = mm(dkv, w_big[...], NT).astype(BF)
            dr = dk_recv[0, pl.ds(BLK, 64), :].astype(F32)
            for h in range(1, n_chip):
                dr = dr + dk_recv[h, pl.ds(BLK, 64), :].astype(F32)
            dr_fin[...] = jnp.transpose(jnp.concatenate([dr[:, :64], dr[:, 64:]], axis=0)).astype(BF)

    gk.steps("k", latent_grad)

    with scope("drain"):
        arrived(dq_out, msg_rs.at[1])
        outs = [pltpu.make_async_copy(buf, dst, out_sem.at[i]) for i, (buf, dst) in enumerate(
            ((dq_out, dq_hbm), (o_fin, o_hbm), (dc_fin, dc_hbm), (dr_fin, dr_hbm)))]
        for c in outs:
            c.start()
        for g in (gc, gv, gk):
            g.finish()
        for c in [pair_dv, pair_dwv, pair_dwk] + pair_dk:
            c.wait_send()
        for k, buf in enumerate((q_recv, do_recv, o_out, dq_out)):
            @pl.when(owner_core == par)
            def _():
                arrived(buf.at[pl.ds(0, n_chip - 1)], msg_ss.at[k])

            @pl.when(owner_core != par)
            def _():
                arrived(buf, msg_ss.at[k])
        for k, buf in enumerate((dv_recv, dk_recv)):
            arrived(buf.at[pl.ds(0, n_chip - 1)], msg_ss.at[4 + k])
        for k in range(2):
            arrived(dw_all.at[k], dw_sem.at[k])
        for c in outs:
            c.wait()


def copy_kernel(*refs):
    n = len(RESULT_PIECES)
    src, dst, buf, (sem_in, sem_out) = refs[:n], refs[n:2 * n], refs[2 * n:3 * n], refs[3 * n:]
    ins, outs = [], []
    for a, b, c, pieces in zip(src, dst, buf, RESULT_PIECES):
        size = a.shape[0] // pieces
        for i in range(pieces):
            rows = pl.ds(i * size, size)
            ins.append(pltpu.make_async_copy(a.at[rows], c.at[rows], sem_in.at[len(ins)]))
            outs.append(pltpu.make_async_copy(c.at[rows], b.at[rows], sem_out.at[len(outs)]))
    for c in ins:
        c.start()
    for c, d in zip(ins, outs):
        c.wait()
        d.start()
    for d in outs:
        d.wait()


RESULT_PIECES = (1, 1, 1, 1, 4, 4)


def copy_results(*arrays):
    hbm = pl.BlockSpec(memory_space=pl.ANY)
    shapes = tuple(jax.ShapeDtypeStruct(a.shape, a.dtype) for a in arrays)
    dma = pltpu.SemaphoreType.DMA((sum(RESULT_PIECES),))
    return pl.pallas_call(
        copy_kernel, out_shape=shapes, in_specs=[hbm] * len(arrays), out_specs=(hbm,) * len(arrays),
        scratch_shapes=[pltpu.VMEM(a.shape, a.dtype) for a in arrays] + [dma, dma],
    )(*arrays)


def solution(mesh):
    n_dev = mesh.shape["cp"]
    n_chip = n_dev // 2
    nz = n_chip // PLANE
    seq = n_dev * BLK
    seq_spec = P("cp")

    def local_step(queries, latent, key_rope, w_uk, w_uv, d_out):
        vm = pl.BlockSpec(memory_space=pltpu.VMEM)
        hbm = pl.BlockSpec(memory_space=pl.ANY)
        dma = pltpu.SemaphoreType.DMA
        gather_sems = [dma((4, nz)), dma((nz,)), dma((2,))]
        o, dq, dc, dr, dwk, dwv = pl.pallas_call(
            functools.partial(kernel, nz, queries.shape[-1]),
            out_shape=(jax.ShapeDtypeStruct((BLK, n_chip, 128), BF),
                       jax.ShapeDtypeStruct((n_chip, 192, BLK), BF),
                       jax.ShapeDtypeStruct((BLK, 512), BF),
                       jax.ShapeDtypeStruct((64, BLK), BF),
                       jax.ShapeDtypeStruct((512, n_chip, 1, 128), F32),
                       jax.ShapeDtypeStruct((512, n_chip, 1, 128), F32)),
            in_specs=[vm] * 4 + [hbm] * 2,
            out_specs=(hbm,) * 6,
            scratch_shapes=[
                pltpu.VMEM((n_chip, BLK, 128), BF),
                pltpu.VMEM((n_chip, 192, BLK), BF),
                pltpu.VMEM((n_chip, BLK, 128), BF),
                pltpu.VMEM((n_chip, 192, 128), BF),
                pltpu.VMEM((BLK, n_chip, 128), BF),
                pltpu.VMEM((BLK, 512), BF),
                pltpu.VMEM((64, BLK), BF),
                pltpu.VMEM((n_chip, BLK, 128), BF),
                pltpu.VMEM((512, n_chip * 256), BF),
                pltpu.VMEM((2, BLK, n_chip, 128), BF),
                pltpu.VMEM((256, 512), BF),
                pltpu.VMEM((n_chip, 192, BLK), BF),
                pltpu.VMEM((n_chip, BLK, 128), BF),
                pltpu.VMEM((2, n_chip, 144, 512), BF),
                pltpu.VMEM((seq, 256), BF),
                pltpu.VMEM((seq, 128), BF),
                pltpu.VMEM((192, seq), BF),
                pltpu.VMEM((128, seq), BF),
                pltpu.VMEM((seq, SUP), F32),
                pltpu.VMEM((CH, SUP), BF),
                pltpu.VMEM((nz * (nz + 1) * CH, SUP), BF),
                pltpu.VMEM((CH, SUP), BF),
                pltpu.VMEM((seq, 256), F32),
                pltpu.VMEM((seq, 128), F32),
                pltpu.VMEM((256, SUP), BF),
                pltpu.VMEM((SUP, 128), BF),
                pltpu.VMEM((128, SUP), F32),
                pltpu.VMEM((128, SUP), F32),
                pltpu.VMEM((192, SUP), F32),
                pltpu.VMEM((8, SUP), F32),
                pltpu.VMEM((n_chip // 2, 1, SUP), F32),
                pltpu.VMEM((n_chip, BLK, 128), BF),
                pltpu.VMEM((n_chip, 192, BLK), BF),
                pltpu.VMEM((2, n_chip, BLK, 128), BF),
                pltpu.VMEM((n_chip, BLK, 128), BF),
                pltpu.VMEM((2, n_chip, 192, 128), BF),
                pltpu.VMEM((n_chip, 192, 128), BF),
                pltpu.VMEM((2, 128, 512), F32),
                pltpu.VMEM((2, 2, SUP, 128), F32),
                pltpu.VMEM((2, SUP, 128), F32),
                pltpu.VMEM((2, 2, n_chip, SUP, 128), F32),
            ] + [dma((6,)), dma((4,)), dma((n_chip // 2,)), dma((n_chip // 2,))] + [dma((3 + nz,)), dma((3 + nz,)), dma((2,)), dma((4,)), dma((2,))] + gather_sems * 3,
            compiler_params=pltpu.CompilerParams(
                collective_id=0, has_side_effects=True, vmem_limit_bytes=62 * 1024 * 1024),
        )(queries.transpose(1, 2, 0), d_out, latent, key_rope.T, w_uk, w_uv)
        o, dq, dc, dr, dwk, dwv = copy_results(
            o, dq, dc, dr, dwk.reshape(512, n_chip, 128), dwv.reshape(512, n_chip, 128))
        return o, dq.transpose(2, 0, 1), dc, dr.T, dwk, dwv

    return jax.shard_map(local_step, mesh=mesh,
                         in_specs=(seq_spec, seq_spec, seq_spec, P(), P(), seq_spec),
                         out_specs=(seq_spec, seq_spec, seq_spec, seq_spec, P(), P()),
                         check_vma=False)
```

```python
import functools
import math

import jax
import jax.numpy as jnp
from jax import lax
from jax.experimental import pallas as pl
from jax.experimental.pallas import tpu as pltpu
from jax.sharding import PartitionSpec as P

MESH = pl.DeviceIdType.MESH
NX, NY = 2, 2
PLANE = NX * NY
BLK = 128
SUP = 256
CH = SUP * PLANE
NEG = -1e30
NT = (((1,), (1,)), ((), ()))
NN = (((1,), (0,)), ((), ()))
BF, F32 = jnp.bfloat16, jnp.float32


def mm(a, b, dims=NN):
    return lax.dot_general(a, b, dims, preferred_element_type=F32)


def pack_rope(x):
    return jnp.concatenate([x[:64], x[64:]], axis=1)


def kernel(nz, qk_dim, q_ref, do_raw, c_ref, rt_ref, wk_hbm, wv_hbm,
           o_hbm, dq_hbm, dc_hbm, dr_hbm, dwk_out, dwv_out,
           o_out, dq_out, dv_recv, dk_recv, o_fin, dc_fin, dr_fin, do_ref,
           w_big, w_stage, wt_cat, q_recv, do_recv, c_all, kr, v, kt, vt, s_buf, p_buf, p_store, ds_buf, dkr, dv,
           qt, dof, dot_, ot, dqt, lse, delta_s, o_send, dq_send, dv_msg, dv_part, dk_msg, dk_part,
           dwt, dw_msg, dw_part, dw_all,
           msg_ss, msg_rs, q_rs, do_rs, pair_s, pair_r, dw_sem, out_sem, w_sem,
           cg_rz, cg_rp, cg_ss, v_rz, v_rp, v_ss, k_rz, k_rp, k_ss):
    n_chip = PLANE * nz
    n_dev = 2 * n_chip
    n_sup = n_chip // 2
    me = lax.axis_index("cp")
    chip, par = me // 2, me % 2
    partner = 2 * chip + (1 - par)
    x, y, z = chip % NX, (chip // NX) % NY, chip // PLANE
    scale = 1.0 / math.sqrt(qk_dim)
    c1 = scale * math.log2(math.e)
    scope = jax.named_scope

    def chip_at(zq, yq, xq):
        return (zq * NY + yq) * NX + xq

    def col_chip(col, zq):
        return chip_at(zq, 1 - y if col >= 2 else y, 1 - x if col % 2 else x)

    def remote(src, dst, ssem, rsem, dev):
        return pltpu.make_async_remote_copy(src_ref=src, dst_ref=dst, send_sem=ssem, recv_sem=rsem,
                                            device_id=(dev,), device_id_type=MESH)

    def start(src, dst, ssem, rsem, dev):
        @pl.when(dev == me)
        def _():
            pltpu.make_async_copy(src, dst, rsem).start()

        @pl.when(dev != me)
        def _():
            remote(src, dst, ssem, rsem, dev).start()

    def arrived(dst, rsem):
        pltpu.make_async_copy(dst, dst, rsem).wait()

    def loop(lo, hi, f):
        def body(i, carry):
            f(i)
            return carry

        lax.fori_loop(lo, hi, body, 0)

    n_piece = 8

    def w_copy(i):
        src = wk_hbm if i < n_piece // 2 else wv_hbm
        return pltpu.make_async_copy(src.at[pl.ds(i % (n_piece // 2) * BLK, BLK)], w_stage.at[i % 2], w_sem.at[i % 2])

    for i in range(2):
        w_copy(i).start()

    def heads_first(x):
        return jnp.transpose(x, (1, 0, 2))

    with scope("barrier"):
        barrier = pltpu.get_barrier_semaphore()
        loop(1, n_dev, lambda i: pl.semaphore_signal(
            barrier, inc=1, device_id=(lax.rem(me + i, n_dev),), device_id_type=MESH))
        pl.semaphore_wait(barrier, n_dev - 1)

    class Gather:
        def __init__(self, buf, rows, split, rz, rp, ss, ready):
            self.buf, self.rows, self.split = buf, rows, split
            self.rz, self.rp, self.ss, self.ready = rz, rp, ss, ready
            self.dev_x = 2 * chip_at(z, y, 1 - x) + par
            self.dev_y = 2 * chip_at(z, 1 - y, x) + par

        def blk(self, col, zq):
            return self.buf.at[par, col_chip(col, zq)]

        def along_z(self, zq, to):
            b = self.blk(0, zq)
            return remote(b, b, self.ss.at[0], self.rz.at[0, zq], 2 * chip_at(to, y, x) + par)

        def to_x(self, col, zq):
            b = self.blk(col, zq)
            return remote(b, b, self.ss.at[0], self.rz.at[1, zq], self.dev_x)

        def to_y(self, col, zq):
            b = self.blk(col, zq)
            return remote(b, b, self.ss.at[0], self.rz.at[2, zq], self.dev_y)

        def part_y(self, col, zq):
            b = self.blk(col, zq).at[pl.ds(0, self.split)]
            return remote(b, b, self.ss.at[0], self.rz.at[3, zq], self.dev_y)

        def part_x(self, col, zq):
            b = self.blk(col, zq).at[pl.ds(self.split, self.rows - self.split)]
            return remote(b, b, self.ss.at[0], self.rz.at[3, zq], self.dev_x)

        def pair(self, col, zq):
            b = self.blk(col, zq)
            return remote(b, b, self.ss.at[1], self.rp.at[zq], partner)

        def own_col(self, zq):
            self.to_x(0, zq).start()
            self.to_y(0, zq).start()
            self.pair(0, zq).start()

        def xy(self, zq):
            self.to_x(1, zq).wait_recv()
            self.part_y(1, zq).start()
            self.pair(1, zq).start()
            self.to_y(2, zq).wait_recv()
            self.part_x(2, zq).start()
            self.pair(2, zq).start()

        def diag(self, zq):
            arrived(self.blk(3, zq), self.rz.at[3, zq])
            self.pair(3, zq).start()

        def pairs(self, zq):
            arrived(self.buf.at[1 - par, pl.ds(zq * PLANE, PLANE)], self.rp.at[zq])

        def begin(self):
            for d in range(1, nz):
                @pl.when(z + d < nz)
                def _():
                    self.along_z(z, z + d).start()

                @pl.when(z - d >= 0)
                def _():
                    self.along_z(z, z - d).start()

            self.own_col(z)

        def from_z(self, zq):
            self.along_z(zq, z).wait_recv()
            self.own_col(zq)

        def at(self, d, f):
            if d == 0:
                f(z)
                return

            @pl.when(z - d >= 0)
            def _():
                f(z - d)

            @pl.when(z + d < nz)
            def _():
                f(z + d)

        def last(self, zq):
            self.diag(zq)
            self.pairs(zq)
            self.ready(zq)

        def steps(self, tag, before_last):
            for d in range(1, nz):
                with scope(f"{tag}z{d}"):
                    self.at(d, self.from_z)
                with scope(f"{tag}xy{d - 1}"):
                    self.at(d - 1, self.xy)
                if d >= 2:
                    with scope(f"{tag}d{d - 2}"):
                        self.at(d - 2, self.last)
            with scope(f"{tag}xy{nz - 1}"):
                self.at(nz - 1, self.xy)
            for d in range(max(nz - 2, 0), nz):
                if d == nz - 1:
                    before_last()
                with scope(f"{tag}d{d}"):
                    self.at(d, self.last)

        def finish(self):
            arrived(self.buf.at[0, pl.ds(0, n_chip - 1)], self.ss.at[0])
            arrived(self.buf.at[0], self.ss.at[1])

    owner_core = lax.rem((chip + 1) // 2, 2)
    q_slot = 2 * (chip // 2) + par

    def sup_chip(s):
        return 2 * s + lax.rem(s + par, 2)

    def q_copy(i):
        head = lax.rem(chip + i, n_chip)
        return q_ref.at[head], q_recv.at[q_slot], msg_ss.at[0], q_rs.at[q_slot // 2], 2 * head + owner_core

    def do_copy(i):
        head = lax.rem(chip + i, n_chip)
        return do_ref.at[head], do_recv.at[q_slot], msg_ss.at[1], do_rs.at[q_slot // 2], 2 * head + owner_core

    def o_copy(s, i):
        return o_send.at[2 * s + i], o_out.at[chip], msg_ss.at[2], msg_rs.at[0], 2 * sup_chip(s) + i

    def dq_copy(s, i):
        return dq_send.at[2 * s + i], dq_out.at[chip], msg_ss.at[3], msg_rs.at[1], 2 * sup_chip(s) + i

    def dv_copy(ch):
        return dv_msg.at[par, ch], dv_recv.at[chip], msg_ss.at[4], msg_rs.at[2], 2 * ch + par

    def dk_copy(ch):
        return dk_msg.at[par, ch], dk_recv.at[chip], msg_ss.at[5], msg_rs.at[3], 2 * ch + par

    gc = Gather(c_all, 144, 80, cg_rz, cg_rp, cg_ss, None)
    with scope("send_c"):
        c_all[par, chip, pl.ds(0, BLK), :] = c_ref[...]
        for i in range(4):
            c_all[par, chip, pl.ds(BLK, 16), pl.ds(128 * i, 128)] = rt_ref[pl.ds(16 * i, 16), :]
        gc.begin()
    with scope("send_q"):
        def send_q(i):
            start(*q_copy(i))
            start(*do_copy(i))

        late = z >= nz // 2

        def lay_do(i):
            rows = pl.ds(pl.multiple_of(i * 32, 32), 32)
            do_ref[:, rows, :] = heads_first(do_raw[rows])

        loop(0, BLK // 32, lay_do)

        @pl.when(jnp.logical_not(late))
        def _():
            loop(0, n_chip, send_q)

    with scope("init"):
        dkr[...] = jnp.zeros_like(dkr)
        dv[...] = jnp.zeros_like(dv)
        for i in range(n_piece):
            w_copy(i).wait()

            def lay_w(r):
                w = heads_first(w_stage[i % 2, pl.ds(pl.multiple_of(r * 32, 32), 32)])
                rows = pl.ds(pl.multiple_of(i % (n_piece // 2) * BLK + r * 32, 32), 32)
                for h in range(n_chip):
                    w_big[rows, pl.ds(h * 256 + 128 * (i // (n_piece // 2)), 128)] = w[h]

            loop(0, BLK // 32, lay_w)
            if i + 2 < n_piece:
                w_copy(i + 2).start()
        wt_cat[...] = jnp.transpose(w_big[:, pl.ds(pl.multiple_of(chip * 256, 256), 256)].astype(F32)).astype(BF)
        qt[pl.ds(192, 64), :] = jnp.zeros((64, SUP), BF)

    def latent_of(ch):
        return jnp.concatenate([c_all[0, ch, pl.ds(0, BLK), :], c_all[1, ch, pl.ds(0, BLK), :]], axis=0)

    def up_project(ch):
        base = pl.multiple_of(ch * SUP, SUP)
        lat = latent_of(ch)
        kv = mm(lat, w_big[:, pl.ds(pl.multiple_of(chip * 256, 256), 256)]).astype(BF)
        kvt = mm(wt_cat[...], lat, NT).astype(BF)
        kr[pl.ds(base, SUP), pl.ds(0, 128)] = kv[:, :128]
        v[pl.ds(base, SUP), :] = kv[:, 128:]
        kt[pl.ds(0, 128), pl.ds(base, SUP)] = kvt[:128]
        vt[:, pl.ds(base, SUP)] = kvt[128:]
        for q in range(2):
            rt = jnp.concatenate([c_all[q, ch, pl.ds(BLK, 16), pl.ds(128 * i, 128)] for i in range(4)], axis=0)
            kt[pl.ds(128, 64), pl.ds(base + q * BLK, BLK)] = rt
            r = jnp.transpose(rt.astype(F32))
            kr[pl.ds(base + q * BLK, BLK), pl.ds(128, 128)] = jnp.concatenate(
                [r, jnp.zeros_like(r)], axis=1).astype(BF)

    diff = lax.broadcasted_iota(jnp.int32, (SUP, SUP), 0) - lax.broadcasted_iota(jnp.int32, (SUP, SUP), 1)

    def load_q(s):
        for i in range(2):
            qt[pl.ds(0, 192), pl.ds(i * BLK, BLK)] = q_recv[2 * s + i]
            dof[pl.ds(i * BLK, BLK), :] = do_recv[2 * s + i]

    def store_row(s):
        a = s // 2
        return (a + 1) * (a + s % 2) * CH

    def forward(s):
        ch = sup_chip(s)
        arrived(q_recv.at[pl.ds(2 * s, 2)], q_rs.at[s])
        arrived(do_recv.at[pl.ds(2 * s, 2)], do_rs.at[s])
        load_q(s)
        dot_[...] = jnp.transpose(dof[...].astype(F32))
        n_ch = s // 2 + 1

        def score(j, m8):
            for t in range(CH // SUP):
                r0 = pl.multiple_of(j * CH + t * SUP, SUP)
                st = mm(kr[pl.ds(r0, SUP), :], qt[...])
                st = jnp.where(diff <= ch * SUP - r0, st, NEG)
                s_buf[pl.ds(r0, SUP), :] = st
                m8 = jnp.maximum(m8, jnp.max(st.reshape(SUP // 8, 8, SUP), axis=0))
            return m8

        m8 = lax.fori_loop(0, n_ch, score, jnp.full((8, SUP), NEG, F32))
        m2 = jnp.max(m8, axis=0, keepdims=True) * c1
        ot[...] = jnp.zeros_like(ot)

        def values(j, l8):
            base = pl.multiple_of(j * CH, CH)
            for t in range(CH // SUP):
                p = jnp.exp2(s_buf[pl.ds(base + t * SUP, SUP), :] * c1 - m2)
                l8 = l8 + jnp.sum(p.reshape(SUP // 8, 8, SUP), axis=0)
                p_buf[pl.ds(t * SUP, SUP), :] = p.astype(BF)
            ot[...] += mm(vt[:, pl.ds(base, CH)], p_buf[...])
            return l8

        l8 = lax.fori_loop(0, n_ch, values, jnp.zeros((8, SUP), F32))
        l = jnp.sum(l8, axis=0, keepdims=True)
        o = ot[...] / l
        lse2 = m2 + jnp.log2(l)
        delta_s[s] = jnp.sum(o * dot_[...], axis=0, keepdims=True)
        o_rows = jnp.transpose(o)
        for i in range(2):
            o_send[2 * s + i] = o_rows[i * BLK:(i + 1) * BLK].astype(BF)
        for i in range(2):
            start(*o_copy(s, i))
        row0 = store_row(s)

        def values_grad(j):
            base = pl.multiple_of(j * CH, CH)
            for t in range(CH // SUP):
                rows = pl.ds(base + t * SUP, SUP)
                p = jnp.exp2(s_buf[rows, :] * c1 - lse2).astype(BF)
                p_store[pl.ds(pl.multiple_of(row0 + base + t * SUP, SUP), SUP), :] = p
                dv[rows, :] += mm(p, dof[...])

        loop(0, n_ch, values_grad)

    def send_dq(s):
        for i in range(2):
            start(*dq_copy(s, i))

    def backward(s):
        load_q(s)
        dqt[...] = jnp.zeros_like(dqt)
        row0 = store_row(s)
        delta = delta_s[s]

        def keys_grad(j):
            base = pl.multiple_of(j * CH, CH)
            for t in range(CH // SUP):
                rows = pl.ds(base + t * SUP, SUP)
                dp = mm(v[rows, :], dof[...], NT)
                p = p_store[pl.ds(pl.multiple_of(row0 + base + t * SUP, SUP), SUP), :].astype(F32)
                ds_buf[pl.ds(t * SUP, SUP), :] = (p * (dp - delta) * scale).astype(BF)
            for t in range(CH // SUP):
                rows = pl.ds(base + t * SUP, SUP)
                dkr[rows, :] += mm(ds_buf[pl.ds(t * SUP, SUP), :], qt[...], NT)
            dqt[...] += mm(kt[:, pl.ds(base, CH)], ds_buf[...])

        loop(0, s // 2 + 1, keys_grad)
        for i in range(2):
            dq_send[2 * s + i] = dqt[:, pl.ds(i * BLK, BLK)].astype(BF)
        if s >= n_sup // 2:
            send_dq(s)

    def ready_c(zq):
        gc.pairs(zq)
        loop(zq * PLANE, (zq + 1) * PLANE, up_project)

    def col_ready(zq):
        @pl.when(z != zq)
        def _():
            gc.from_z(zq)

    def step_c(k):
        if k < nz:
            col_ready(k)
        if 0 <= k - 1 < nz:
            gc.xy(k - 1)
        if 0 <= k - 2 < nz:
            gc.diag(k - 2)
            ready_c(k - 2)

    for k in range(nz + 2):
        with scope(f"c{k}"):
            step_c(k)
            if k < 2:
                @pl.when(late)
                def _():
                    loop(k * n_chip // 2, (k + 1) * n_chip // 2, send_q)

        if k >= 2:
            with scope(f"fwd{k - 2}"):
                loop(2 * (k - 2), 2 * (k - 2) + 2, forward)

    def head_dw(k, lo, hi, grads):
        def add(ch):
            base = pl.multiple_of(ch * SUP, SUP)
            g = jnp.transpose(grads(pl.ds(base, SUP))).astype(BF)
            dwt[k] += mm(g, latent_of(ch))

        loop(lo, hi, add)

    def dw_exchange(k):
        dw_msg[k] = jnp.transpose(dwt[k]).reshape(2, SUP, 128)
        c = remote(dw_msg.at[k, 1 - par], dw_part.at[k], pair_s.at[k], pair_r.at[k], partner)
        c.start()
        return c

    def dw_begin(k, c):
        c.wait_recv()
        dw_all[k, par, chip] = dw_msg[k, par] + dw_part[k]

    def dw_out_copy(k, q, h):
        dst = dwk_out if k == 0 else dwv_out
        return pltpu.make_async_copy(dw_all.at[k, q, h], dst.at[pl.ds(q * SUP, SUP), h, 0], dw_sem.at[k])

    def put_dw(k):
        def put(zq):
            for q in range(2):
                loop(zq * PLANE, (zq + 1) * PLANE, lambda h: dw_out_copy(k, q, h).start())

        return put

    dwt[...] = jnp.zeros_like(dwt)
    gv = Gather(dw_all.at[1], SUP, 128, v_rz, v_rp, v_ss, put_dw(1))
    gk = Gather(dw_all.at[0], SUP, 128, k_rz, k_rp, k_ss, put_dw(0))
    with scope("dv"):
        def dv_out(ch):
            for q in range(2):
                dv_msg[q, ch] = dv[pl.ds(pl.multiple_of(ch * SUP, SUP) + q * BLK, BLK), :].astype(BF)

        loop(0, n_chip, dv_out)
        pair_dv = remote(dv_msg.at[1 - par], dv_part, pair_s.at[2], pair_r.at[2], partner)
        pair_dv.start()
        head_dw(1, 0, n_chip, lambda rows: dv[rows, :])
        pair_dwv = dw_exchange(1)
        pair_dv.wait_recv()

        def dv_add(ch):
            dv_msg[par, ch] = (dv_msg[par, ch].astype(F32) + dv_part[ch].astype(F32)).astype(BF)

        loop(0, n_chip, dv_add)
        dw_begin(1, pair_dwv)
        gv.begin()

        def dv_send(i):
            start(*dv_copy(lax.rem(chip + i, n_chip)))

        loop(0, n_chip, dv_send)

    pair_dk = [remote(dk_msg.at[1 - par, pl.ds(PLANE * g, PLANE)], dk_part.at[pl.ds(PLANE * g, PLANE)],
                      pair_s.at[3 + g], pair_r.at[3 + g], partner) for g in range(nz)]

    def dk_out(g):
        def put(ch):
            for q in range(2):
                rows = pl.ds(pl.multiple_of(ch * SUP, SUP) + q * BLK, BLK)
                dk_msg[q, ch, pl.ds(0, BLK), :] = dkr[rows, pl.ds(0, 128)].astype(BF)
                dk_msg[q, ch, pl.ds(BLK, 64), :] = pack_rope(dkr[rows, pl.ds(128, 128)][:, :64]).astype(BF)

        loop(PLANE * g, PLANE * (g + 1), put)
        pair_dk[g].start()
        head_dw(0, PLANE * g, PLANE * (g + 1), lambda rows: dkr[rows, pl.ds(0, 128)])

    def dk_add(g):
        pair_dk[g].wait_recv()

        def put(ch):
            dk_msg[par, ch] = (dk_msg[par, ch].astype(F32) + dk_part[ch].astype(F32)).astype(BF)

        loop(PLANE * g, PLANE * (g + 1), put)

    for g in reversed(range(nz)):
        for s in (2 * g + 1, 2 * g):
            with scope(f"bwd{s}"):
                backward(s)
        if g + 1 < nz:
            with scope(f"dks{g + 1}"):
                dk_add(g + 1)
        with scope(f"dko{g}"):
            dk_out(g)
        if g == nz - 2:
            with scope("vz1"):
                gv.at(0, gv.xy)
                gv.at(1, gv.from_z)

    with scope("dwk"):
        pair_dwk = dw_exchange(0)
        dw_begin(0, pair_dwk)
        gk.begin()
    with scope("dks0"):
        dk_add(0)
    with scope("vz"):
        for d in range(2, nz):
            gv.at(d, gv.from_z)
        for s in reversed(range(n_sup // 2)):
            send_dq(s)
    for d in range(nz):
        if d + 1 < nz:
            with scope(f"vxy{d + 1}"):
                gv.at(d + 1, gv.xy)
        with scope(f"vd{d}"):
            gv.at(d, gv.last)
            loop(d * n_chip // nz, (d + 1) * n_chip // nz, lambda i: start(*dk_copy(lax.rem(chip + i, n_chip))))
        if d == 0:
            with scope("ofin"):
                arrived(o_out, msg_rs.at[0])

                def lay_o(i):
                    rows = pl.ds(pl.multiple_of(i * 32, 32), 32)
                    o_fin[rows] = heads_first(o_out[:, rows, :])

                loop(0, BLK // 32, lay_o)

    def latent_grad():
        with scope("dc"):
            arrived(dv_recv, msg_rs.at[2])
            arrived(dk_recv, msg_rs.at[3])
            dkv = jnp.concatenate([g for h in range(n_chip) for g in (dk_recv[h, pl.ds(0, BLK), :], dv_recv[h])], axis=1)
            dc_fin[...] = mm(dkv, w_big[...], NT).astype(BF)
            dr = dk_recv[0, pl.ds(BLK, 64), :].astype(F32)
            for h in range(1, n_chip):
                dr = dr + dk_recv[h, pl.ds(BLK, 64), :].astype(F32)
            dr_fin[...] = jnp.transpose(jnp.concatenate([dr[:, :64], dr[:, 64:]], axis=0)).astype(BF)

    gk.steps("k", latent_grad)

    with scope("drain"):
        arrived(dq_out, msg_rs.at[1])
        outs = [pltpu.make_async_copy(buf, dst, out_sem.at[i]) for i, (buf, dst) in enumerate(
            ((dq_out, dq_hbm), (o_fin, o_hbm), (dc_fin, dc_hbm), (dr_fin, dr_hbm)))]
        for c in outs:
            c.start()
        for g in (gc, gv, gk):
            g.finish()
        for c in [pair_dv, pair_dwv, pair_dwk] + pair_dk:
            c.wait_send()
        for k, buf in enumerate((q_recv, do_recv, o_out, dq_out)):
            @pl.when(owner_core == par)
            def _():
                arrived(buf.at[pl.ds(0, n_chip - 1)], msg_ss.at[k])

            @pl.when(owner_core != par)
            def _():
                arrived(buf, msg_ss.at[k])
        for k, buf in enumerate((dv_recv, dk_recv)):
            arrived(buf.at[pl.ds(0, n_chip - 1)], msg_ss.at[4 + k])
        for k in range(2):
            arrived(dw_all.at[k], dw_sem.at[k])
        for c in outs:
            c.wait()


def copy_kernel(*refs):
    n = len(RESULT_PIECES)
    src, dst, buf, (sem_in, sem_out) = refs[:n], refs[n:2 * n], refs[2 * n:3 * n], refs[3 * n:]
    ins, outs = [], []
    for a, b, c, pieces in zip(src, dst, buf, RESULT_PIECES):
        size = a.shape[0] // pieces
        for i in range(pieces):
            rows = pl.ds(i * size, size)
            ins.append(pltpu.make_async_copy(a.at[rows], c.at[rows], sem_in.at[len(ins)]))
            outs.append(pltpu.make_async_copy(c.at[rows], b.at[rows], sem_out.at[len(outs)]))
    for c in ins:
        c.start()
    for c, d in zip(ins, outs):
        c.wait()
        d.start()
    for d in outs:
        d.wait()


RESULT_PIECES = (1, 2, 1, 1, 8, 8)


def copy_results(*arrays):
    hbm = pl.BlockSpec(memory_space=pl.ANY)
    shapes = tuple(jax.ShapeDtypeStruct(a.shape, a.dtype) for a in arrays)
    dma = pltpu.SemaphoreType.DMA((sum(RESULT_PIECES),))
    return pl.pallas_call(
        copy_kernel, out_shape=shapes, in_specs=[hbm] * len(arrays), out_specs=(hbm,) * len(arrays),
        scratch_shapes=[pltpu.VMEM(a.shape, a.dtype) for a in arrays] + [dma, dma],
    )(*arrays)


def solution(mesh):
    n_dev = mesh.shape["cp"]
    n_chip = n_dev // 2
    nz = n_chip // PLANE
    seq = n_dev * BLK
    seq_spec = P("cp")

    def local_step(queries, latent, key_rope, w_uk, w_uv, d_out):
        vm = pl.BlockSpec(memory_space=pltpu.VMEM)
        hbm = pl.BlockSpec(memory_space=pl.ANY)
        dma = pltpu.SemaphoreType.DMA
        gather_sems = [dma((4, nz)), dma((nz,)), dma((2,))]
        o, dq, dc, dr, dwk, dwv = pl.pallas_call(
            functools.partial(kernel, nz, queries.shape[-1]),
            out_shape=(jax.ShapeDtypeStruct((BLK, n_chip, 128), BF),
                       jax.ShapeDtypeStruct((n_chip, 192, BLK), BF),
                       jax.ShapeDtypeStruct((BLK, 512), BF),
                       jax.ShapeDtypeStruct((64, BLK), BF),
                       jax.ShapeDtypeStruct((512, n_chip, 1, 128), F32),
                       jax.ShapeDtypeStruct((512, n_chip, 1, 128), F32)),
            in_specs=[vm] * 4 + [hbm] * 2,
            out_specs=(hbm,) * 6,
            scratch_shapes=[
                pltpu.VMEM((n_chip, BLK, 128), BF),
                pltpu.VMEM((n_chip, 192, BLK), BF),
                pltpu.VMEM((n_chip, BLK, 128), BF),
                pltpu.VMEM((n_chip, 192, 128), BF),
                pltpu.VMEM((BLK, n_chip, 128), BF),
                pltpu.VMEM((BLK, 512), BF),
                pltpu.VMEM((64, BLK), BF),
                pltpu.VMEM((n_chip, BLK, 128), BF),
                pltpu.VMEM((512, n_chip * 256), BF),
                pltpu.VMEM((2, BLK, n_chip, 128), BF),
                pltpu.VMEM((256, 512), BF),
                pltpu.VMEM((n_chip, 192, BLK), BF),
                pltpu.VMEM((n_chip, BLK, 128), BF),
                pltpu.VMEM((2, n_chip, 144, 512), BF),
                pltpu.VMEM((seq, 256), BF),
                pltpu.VMEM((seq, 128), BF),
                pltpu.VMEM((192, seq), BF),
                pltpu.VMEM((128, seq), BF),
                pltpu.VMEM((seq, SUP), F32),
                pltpu.VMEM((CH, SUP), BF),
                pltpu.VMEM((nz * (nz + 1) * CH, SUP), BF),
                pltpu.VMEM((CH, SUP), BF),
                pltpu.VMEM((seq, 256), F32),
                pltpu.VMEM((seq, 128), F32),
                pltpu.VMEM((256, SUP), BF),
                pltpu.VMEM((SUP, 128), BF),
                pltpu.VMEM((128, SUP), F32),
                pltpu.VMEM((128, SUP), F32),
                pltpu.VMEM((192, SUP), F32),
                pltpu.VMEM((8, SUP), F32),
                pltpu.VMEM((n_chip // 2, 1, SUP), F32),
                pltpu.VMEM((n_chip, BLK, 128), BF),
                pltpu.VMEM((n_chip, 192, BLK), BF),
                pltpu.VMEM((2, n_chip, BLK, 128), BF),
                pltpu.VMEM((n_chip, BLK, 128), BF),
                pltpu.VMEM((2, n_chip, 192, 128), BF),
                pltpu.VMEM((n_chip, 192, 128), BF),
                pltpu.VMEM((2, 128, 512), F32),
                pltpu.VMEM((2, 2, SUP, 128), F32),
                pltpu.VMEM((2, SUP, 128), F32),
                pltpu.VMEM((2, 2, n_chip, SUP, 128), F32),
            ] + [dma((6,)), dma((4,)), dma((n_chip // 2,)), dma((n_chip // 2,))] + [dma((3 + nz,)), dma((3 + nz,)), dma((2,)), dma((4,)), dma((2,))] + gather_sems * 3,
            compiler_params=pltpu.CompilerParams(
                collective_id=0, has_side_effects=True, vmem_limit_bytes=62 * 1024 * 1024),
        )(queries.transpose(1, 2, 0), d_out, latent, key_rope.T, w_uk, w_uv)
        o, dq, dc, dr, dwk, dwv = copy_results(
            o, dq, dc, dr, dwk.reshape(512, n_chip, 128), dwv.reshape(512, n_chip, 128))
        return o, dq.transpose(2, 0, 1), dc, dr.T, dwk, dwv

    return jax.shard_map(local_step, mesh=mesh,
                         in_specs=(seq_spec, seq_spec, seq_spec, P(), P(), seq_spec),
                         out_specs=(seq_spec, seq_spec, seq_spec, seq_spec, P(), P()),
                         check_vma=False)
```

```python
import functools
import math

import jax
import jax.numpy as jnp
from jax import lax
from jax.experimental import pallas as pl
from jax.experimental.pallas import tpu as pltpu
from jax.sharding import PartitionSpec as P

MESH = pl.DeviceIdType.MESH
NX, NY = 2, 2
PLANE = NX * NY
BLK = 128
SUP = 256
CH = SUP * PLANE
NEG = -1e30
NT = (((1,), (1,)), ((), ()))
NN = (((1,), (0,)), ((), ()))
BF, F32 = jnp.bfloat16, jnp.float32


def mm(a, b, dims=NN):
    return lax.dot_general(a, b, dims, preferred_element_type=F32)


def pack_rope(x):
    return jnp.concatenate([x[:64], x[64:]], axis=1)


def kernel(nz, qk_dim, q_ref, do_raw, c_ref, rt_ref, wk_hbm, wv_hbm,
           o_hbm, dq_hbm, dc_hbm, dr_hbm, dwk_out, dwv_out,
           o_out, dq_out, dv_recv, dk_recv, o_fin, dc_fin, dr_fin, do_ref,
           w_big, w_stage, wt_cat, q_recv, do_recv, c_all, kr, v, kt, vt, s_buf, p_buf, p_store, ds_buf, dkr, dv,
           qt, dof, dot_, ot, dqt, lse, delta_s, o_send, dq_send, dv_msg, dv_part, dk_msg, dk_part,
           dwt, dw_msg, dw_part, dw_all,
           msg_ss, msg_rs, q_rs, do_rs, pair_s, pair_r, dw_sem, out_sem, w_sem,
           cg_rz, cg_rp, cg_ss, v_rz, v_rp, v_ss, k_rz, k_rp, k_ss):
    n_chip = PLANE * nz
    n_dev = 2 * n_chip
    n_sup = n_chip // 2
    me = lax.axis_index("cp")
    chip, par = me // 2, me % 2
    partner = 2 * chip + (1 - par)
    x, y, z = chip % NX, (chip // NX) % NY, chip // PLANE
    scale = 1.0 / math.sqrt(qk_dim)
    c1 = scale * math.log2(math.e)
    scope = jax.named_scope

    def chip_at(zq, yq, xq):
        return (zq * NY + yq) * NX + xq

    def col_chip(col, zq):
        return chip_at(zq, 1 - y if col >= 2 else y, 1 - x if col % 2 else x)

    def remote(src, dst, ssem, rsem, dev):
        return pltpu.make_async_remote_copy(src_ref=src, dst_ref=dst, send_sem=ssem, recv_sem=rsem,
                                            device_id=(dev,), device_id_type=MESH)

    def start(src, dst, ssem, rsem, dev):
        @pl.when(dev == me)
        def _():
            pltpu.make_async_copy(src, dst, rsem).start()

        @pl.when(dev != me)
        def _():
            remote(src, dst, ssem, rsem, dev).start()

    def arrived(dst, rsem):
        pltpu.make_async_copy(dst, dst, rsem).wait()

    def loop(lo, hi, f):
        def body(i, carry):
            f(i)
            return carry

        lax.fori_loop(lo, hi, body, 0)

    n_piece = 8

    def w_copy(i):
        src = wk_hbm if i < n_piece // 2 else wv_hbm
        return pltpu.make_async_copy(src.at[pl.ds(i % (n_piece // 2) * BLK, BLK)], w_stage.at[i % 2], w_sem.at[i % 2])

    for i in range(2):
        w_copy(i).start()

    def heads_first(x):
        return jnp.transpose(x, (1, 0, 2))

    with scope("barrier"):
        barrier = pltpu.get_barrier_semaphore()
        loop(1, n_dev, lambda i: pl.semaphore_signal(
            barrier, inc=1, device_id=(lax.rem(me + i, n_dev),), device_id_type=MESH))
        pl.semaphore_wait(barrier, n_dev - 1)

    class Gather:
        def __init__(self, buf, rows, split, rz, rp, ss, ready):
            self.buf, self.rows, self.split = buf, rows, split
            self.rz, self.rp, self.ss, self.ready = rz, rp, ss, ready
            self.dev_x = 2 * chip_at(z, y, 1 - x) + par
            self.dev_y = 2 * chip_at(z, 1 - y, x) + par

        def blk(self, col, zq):
            return self.buf.at[par, col_chip(col, zq)]

        def along_z(self, zq, to):
            b = self.blk(0, zq)
            return remote(b, b, self.ss.at[0], self.rz.at[0, zq], 2 * chip_at(to, y, x) + par)

        def to_x(self, col, zq):
            b = self.blk(col, zq)
            return remote(b, b, self.ss.at[0], self.rz.at[1, zq], self.dev_x)

        def to_y(self, col, zq):
            b = self.blk(col, zq)
            return remote(b, b, self.ss.at[0], self.rz.at[2, zq], self.dev_y)

        def part_y(self, col, zq):
            b = self.blk(col, zq).at[pl.ds(0, self.split)]
            return remote(b, b, self.ss.at[0], self.rz.at[3, zq], self.dev_y)

        def part_x(self, col, zq):
            b = self.blk(col, zq).at[pl.ds(self.split, self.rows - self.split)]
            return remote(b, b, self.ss.at[0], self.rz.at[3, zq], self.dev_x)

        def pair(self, col, zq):
            b = self.blk(col, zq)
            return remote(b, b, self.ss.at[1], self.rp.at[zq], partner)

        def own_col(self, zq):
            self.to_x(0, zq).start()
            self.to_y(0, zq).start()
            self.pair(0, zq).start()

        def xy(self, zq):
            self.to_x(1, zq).wait_recv()
            self.part_y(1, zq).start()
            self.pair(1, zq).start()
            self.to_y(2, zq).wait_recv()
            self.part_x(2, zq).start()
            self.pair(2, zq).start()

        def diag(self, zq):
            arrived(self.blk(3, zq), self.rz.at[3, zq])
            self.pair(3, zq).start()

        def pairs(self, zq):
            arrived(self.buf.at[1 - par, pl.ds(zq * PLANE, PLANE)], self.rp.at[zq])

        def begin(self):
            for d in range(1, nz):
                @pl.when(z + d < nz)
                def _():
                    self.along_z(z, z + d).start()

                @pl.when(z - d >= 0)
                def _():
                    self.along_z(z, z - d).start()

            self.own_col(z)

        def from_z(self, zq):
            self.along_z(zq, z).wait_recv()
            self.own_col(zq)

        def at(self, d, f):
            if d == 0:
                f(z)
                return

            @pl.when(z - d >= 0)
            def _():
                f(z - d)

            @pl.when(z + d < nz)
            def _():
                f(z + d)

        def last(self, zq):
            self.diag(zq)
            self.pairs(zq)
            self.ready(zq)

        def steps(self, tag, before_last):
            for d in range(1, nz):
                with scope(f"{tag}z{d}"):
                    self.at(d, self.from_z)
                with scope(f"{tag}xy{d - 1}"):
                    self.at(d - 1, self.xy)
                if d >= 2:
                    with scope(f"{tag}d{d - 2}"):
                        self.at(d - 2, self.last)
            with scope(f"{tag}xy{nz - 1}"):
                self.at(nz - 1, self.xy)
            for d in range(max(nz - 2, 0), nz):
                if d == nz - 1:
                    before_last()
                with scope(f"{tag}d{d}"):
                    self.at(d, self.last)

        def finish(self):
            arrived(self.buf.at[0, pl.ds(0, n_chip - 1)], self.ss.at[0])
            arrived(self.buf.at[0], self.ss.at[1])

    owner_core = lax.rem((chip + 1) // 2, 2)
    q_slot = 2 * (chip // 2) + par

    def sup_chip(s):
        return 2 * s + lax.rem(s + par, 2)

    def far_first(i):
        half = n_chip // 2
        return (1 - chip // half + i // half) % 2 * half + (chip + i) % half

    def q_copy(i):
        head = far_first(i)
        return q_ref.at[head], q_recv.at[q_slot], msg_ss.at[0], q_rs.at[q_slot // 2], 2 * head + owner_core

    def do_copy(i):
        head = far_first(i)
        return do_ref.at[head], do_recv.at[q_slot], msg_ss.at[1], do_rs.at[q_slot // 2], 2 * head + owner_core

    def o_copy(s, i):
        return o_send.at[2 * s + i], o_out.at[chip], msg_ss.at[2], msg_rs.at[0], 2 * sup_chip(s) + i

    def dq_copy(s, i):
        return dq_send.at[2 * s + i], dq_out.at[chip], msg_ss.at[3], msg_rs.at[1], 2 * sup_chip(s) + i

    def dv_copy(ch):
        return dv_msg.at[par, ch], dv_recv.at[chip], msg_ss.at[4], msg_rs.at[2], 2 * ch + par

    def dk_copy(ch):
        return dk_msg.at[par, ch], dk_recv.at[chip], msg_ss.at[5], msg_rs.at[3], 2 * ch + par

    gc = Gather(c_all, 144, 80, cg_rz, cg_rp, cg_ss, None)
    with scope("send_c"):
        c_all[par, chip, pl.ds(0, BLK), :] = c_ref[...]
        for i in range(4):
            c_all[par, chip, pl.ds(BLK, 16), pl.ds(128 * i, 128)] = rt_ref[pl.ds(16 * i, 16), :]
        gc.begin()
    with scope("send_q"):
        def send_q(i):
            start(*q_copy(i))
            start(*do_copy(i))

        late = z >= nz // 2

        def lay_do(i):
            rows = pl.ds(pl.multiple_of(i * 32, 32), 32)
            do_ref[:, rows, :] = heads_first(do_raw[rows])

        loop(0, BLK // 32, lay_do)

        @pl.when(jnp.logical_not(late))
        def _():
            loop(0, n_chip, send_q)

    with scope("init"):
        dkr[...] = jnp.zeros_like(dkr)
        dv[...] = jnp.zeros_like(dv)
        for i in range(n_piece):
            w_copy(i).wait()

            def lay_w(r):
                w = heads_first(w_stage[i % 2, pl.ds(pl.multiple_of(r * 32, 32), 32)])
                rows = pl.ds(pl.multiple_of(i % (n_piece // 2) * BLK + r * 32, 32), 32)
                for h in range(n_chip):
                    w_big[rows, pl.ds(h * 256 + 128 * (i // (n_piece // 2)), 128)] = w[h]

            loop(0, BLK // 32, lay_w)
            if i + 2 < n_piece:
                w_copy(i + 2).start()
        wt_cat[...] = jnp.transpose(w_big[:, pl.ds(pl.multiple_of(chip * 256, 256), 256)].astype(F32)).astype(BF)
        qt[pl.ds(192, 64), :] = jnp.zeros((64, SUP), BF)

    def latent_of(ch):
        return jnp.concatenate([c_all[0, ch, pl.ds(0, BLK), :], c_all[1, ch, pl.ds(0, BLK), :]], axis=0)

    def up_project(ch):
        base = pl.multiple_of(ch * SUP, SUP)
        lat = latent_of(ch)
        kv = mm(lat, w_big[:, pl.ds(pl.multiple_of(chip * 256, 256), 256)]).astype(BF)
        kvt = mm(wt_cat[...], lat, NT).astype(BF)
        kr[pl.ds(base, SUP), pl.ds(0, 128)] = kv[:, :128]
        v[pl.ds(base, SUP), :] = kv[:, 128:]
        kt[pl.ds(0, 128), pl.ds(base, SUP)] = kvt[:128]
        vt[:, pl.ds(base, SUP)] = kvt[128:]
        for q in range(2):
            rt = jnp.concatenate([c_all[q, ch, pl.ds(BLK, 16), pl.ds(128 * i, 128)] for i in range(4)], axis=0)
            kt[pl.ds(128, 64), pl.ds(base + q * BLK, BLK)] = rt
            r = jnp.transpose(rt.astype(F32))
            kr[pl.ds(base + q * BLK, BLK), pl.ds(128, 128)] = jnp.concatenate(
                [r, jnp.zeros_like(r)], axis=1).astype(BF)

    diff = lax.broadcasted_iota(jnp.int32, (SUP, SUP), 0) - lax.broadcasted_iota(jnp.int32, (SUP, SUP), 1)

    def load_q(s):
        for i in range(2):
            qt[pl.ds(0, 192), pl.ds(i * BLK, BLK)] = q_recv[2 * s + i]
            dof[pl.ds(i * BLK, BLK), :] = do_recv[2 * s + i]

    def store_row(s):
        a = s // 2
        return (a + 1) * (a + s % 2) * CH

    def forward(s):
        ch = sup_chip(s)
        arrived(q_recv.at[pl.ds(2 * s, 2)], q_rs.at[s])
        arrived(do_recv.at[pl.ds(2 * s, 2)], do_rs.at[s])
        load_q(s)
        dot_[...] = jnp.transpose(dof[...].astype(F32))
        n_ch = s // 2 + 1

        def score(j, m8):
            for t in range(CH // SUP):
                r0 = pl.multiple_of(j * CH + t * SUP, SUP)
                st = mm(kr[pl.ds(r0, SUP), :], qt[...])
                st = jnp.where(diff <= ch * SUP - r0, st, NEG)
                s_buf[pl.ds(r0, SUP), :] = st
                m8 = jnp.maximum(m8, jnp.max(st.reshape(SUP // 8, 8, SUP), axis=0))
            return m8

        m8 = lax.fori_loop(0, n_ch, score, jnp.full((8, SUP), NEG, F32))
        m2 = jnp.max(m8, axis=0, keepdims=True) * c1
        ot[...] = jnp.zeros_like(ot)

        def values(j, l8):
            base = pl.multiple_of(j * CH, CH)
            for t in range(CH // SUP):
                p = jnp.exp2(s_buf[pl.ds(base + t * SUP, SUP), :] * c1 - m2)
                l8 = l8 + jnp.sum(p.reshape(SUP // 8, 8, SUP), axis=0)
                p_buf[pl.ds(t * SUP, SUP), :] = p.astype(BF)
            ot[...] += mm(vt[:, pl.ds(base, CH)], p_buf[...])
            return l8

        l8 = lax.fori_loop(0, n_ch, values, jnp.zeros((8, SUP), F32))
        l = jnp.sum(l8, axis=0, keepdims=True)
        o = ot[...] / l
        lse2 = m2 + jnp.log2(l)
        delta_s[s] = jnp.sum(o * dot_[...], axis=0, keepdims=True)
        o_rows = jnp.transpose(o)
        for i in range(2):
            o_send[2 * s + i] = o_rows[i * BLK:(i + 1) * BLK].astype(BF)
        for i in range(2):
            start(*o_copy(s, i))
        row0 = store_row(s)

        def values_grad(j):
            base = pl.multiple_of(j * CH, CH)
            for t in range(CH // SUP):
                rows = pl.ds(base + t * SUP, SUP)
                p = jnp.exp2(s_buf[rows, :] * c1 - lse2).astype(BF)
                p_store[pl.ds(pl.multiple_of(row0 + base + t * SUP, SUP), SUP), :] = p
                dv[rows, :] += mm(p, dof[...])

        loop(0, n_ch, values_grad)

    def send_dq(s):
        for i in range(2):
            start(*dq_copy(s, i))

    def backward(s):
        load_q(s)
        dqt[...] = jnp.zeros_like(dqt)
        row0 = store_row(s)
        delta = delta_s[s]

        def keys_grad(j):
            base = pl.multiple_of(j * CH, CH)
            for t in range(CH // SUP):
                rows = pl.ds(base + t * SUP, SUP)
                dp = mm(v[rows, :], dof[...], NT)
                p = p_store[pl.ds(pl.multiple_of(row0 + base + t * SUP, SUP), SUP), :].astype(F32)
                ds_buf[pl.ds(t * SUP, SUP), :] = (p * (dp - delta) * scale).astype(BF)
            for t in range(CH // SUP):
                rows = pl.ds(base + t * SUP, SUP)
                dkr[rows, :] += mm(ds_buf[pl.ds(t * SUP, SUP), :], qt[...], NT)
            dqt[...] += mm(kt[:, pl.ds(base, CH)], ds_buf[...])

        loop(0, s // 2 + 1, keys_grad)
        for i in range(2):
            dq_send[2 * s + i] = dqt[:, pl.ds(i * BLK, BLK)].astype(BF)
        if s >= n_sup // 2:
            send_dq(s)

    def ready_c(zq):
        gc.pairs(zq)
        loop(zq * PLANE, (zq + 1) * PLANE, up_project)

    def col_ready(zq):
        @pl.when(z != zq)
        def _():
            gc.from_z(zq)

    def step_c(k):
        if k < nz:
            col_ready(k)
        if 0 <= k - 1 < nz:
            gc.xy(k - 1)
        if 0 <= k - 2 < nz:
            gc.diag(k - 2)
            ready_c(k - 2)

    for k in range(nz + 2):
        with scope(f"c{k}"):
            step_c(k)
            if k < 2:
                @pl.when(late)
                def _():
                    loop(k * n_chip // 2, (k + 1) * n_chip // 2, send_q)

        if k >= 2:
            with scope(f"fwd{k - 2}"):
                loop(2 * (k - 2), 2 * (k - 2) + 2, forward)

    def head_dw(k, lo, hi, grads):
        def add(ch):
            base = pl.multiple_of(ch * SUP, SUP)
            g = jnp.transpose(grads(pl.ds(base, SUP))).astype(BF)
            dwt[k] += mm(g, latent_of(ch))

        loop(lo, hi, add)

    def dw_exchange(k):
        dw_msg[k] = jnp.transpose(dwt[k]).reshape(2, SUP, 128)
        c = remote(dw_msg.at[k, 1 - par], dw_part.at[k], pair_s.at[k], pair_r.at[k], partner)
        c.start()
        return c

    def dw_begin(k, c):
        c.wait_recv()
        dw_all[k, par, chip] = dw_msg[k, par] + dw_part[k]

    def dw_out_copy(k, q, h):
        dst = dwk_out if k == 0 else dwv_out
        return pltpu.make_async_copy(dw_all.at[k, q, h], dst.at[pl.ds(q * SUP, SUP), h, 0], dw_sem.at[k])

    def put_dw(k):
        def put(zq):
            for q in range(2):
                loop(zq * PLANE, (zq + 1) * PLANE, lambda h: dw_out_copy(k, q, h).start())

        return put

    dwt[...] = jnp.zeros_like(dwt)
    gv = Gather(dw_all.at[1], SUP, 128, v_rz, v_rp, v_ss, put_dw(1))
    gk = Gather(dw_all.at[0], SUP, 128, k_rz, k_rp, k_ss, put_dw(0))
    with scope("dv"):
        def dv_out(ch):
            for q in range(2):
                dv_msg[q, ch] = dv[pl.ds(pl.multiple_of(ch * SUP, SUP) + q * BLK, BLK), :].astype(BF)

        loop(0, n_chip, dv_out)
        pair_dv = remote(dv_msg.at[1 - par], dv_part, pair_s.at[2], pair_r.at[2], partner)
        pair_dv.start()
        head_dw(1, 0, n_chip, lambda rows: dv[rows, :])
        pair_dwv = dw_exchange(1)
        pair_dv.wait_recv()

        def dv_add(ch):
            dv_msg[par, ch] = (dv_msg[par, ch].astype(F32) + dv_part[ch].astype(F32)).astype(BF)

        loop(0, n_chip, dv_add)
        dw_begin(1, pair_dwv)
        gv.begin()

        def dv_send(i):
            start(*dv_copy(lax.rem(chip + i, n_chip)))

        loop(0, n_chip, dv_send)

    pair_dk = [remote(dk_msg.at[1 - par, pl.ds(PLANE * g, PLANE)], dk_part.at[pl.ds(PLANE * g, PLANE)],
                      pair_s.at[3 + g], pair_r.at[3 + g], partner) for g in range(nz)]

    def dk_out(g):
        def put(ch):
            for q in range(2):
                rows = pl.ds(pl.multiple_of(ch * SUP, SUP) + q * BLK, BLK)
                dk_msg[q, ch, pl.ds(0, BLK), :] = dkr[rows, pl.ds(0, 128)].astype(BF)
                dk_msg[q, ch, pl.ds(BLK, 64), :] = pack_rope(dkr[rows, pl.ds(128, 128)][:, :64]).astype(BF)

        loop(PLANE * g, PLANE * (g + 1), put)
        pair_dk[g].start()
        head_dw(0, PLANE * g, PLANE * (g + 1), lambda rows: dkr[rows, pl.ds(0, 128)])

    def dk_add(g):
        pair_dk[g].wait_recv()

        def put(ch):
            dk_msg[par, ch] = (dk_msg[par, ch].astype(F32) + dk_part[ch].astype(F32)).astype(BF)

        loop(PLANE * g, PLANE * (g + 1), put)

    for g in reversed(range(nz)):
        for s in (2 * g + 1, 2 * g):
            with scope(f"bwd{s}"):
                backward(s)
        if g + 1 < nz:
            with scope(f"dks{g + 1}"):
                dk_add(g + 1)
        with scope(f"dko{g}"):
            dk_out(g)
        if g == nz - 2:
            with scope("vz1"):
                gv.at(0, gv.xy)
                gv.at(1, gv.from_z)

    with scope("dwk"):
        pair_dwk = dw_exchange(0)
        dw_begin(0, pair_dwk)
        gk.begin()
    with scope("dks0"):
        dk_add(0)
    with scope("vz"):
        for d in range(2, nz):
            gv.at(d, gv.from_z)
        for s in reversed(range(n_sup // 2)):
            send_dq(s)
    for d in range(nz):
        if d + 1 < nz:
            with scope(f"vxy{d + 1}"):
                gv.at(d + 1, gv.xy)
        with scope(f"vd{d}"):
            gv.at(d, gv.last)
            loop(d * n_chip // nz, (d + 1) * n_chip // nz, lambda i: start(*dk_copy(lax.rem(chip + i, n_chip))))
        if d == 0:
            with scope("ofin"):
                arrived(o_out, msg_rs.at[0])

                def lay_o(i):
                    rows = pl.ds(pl.multiple_of(i * 32, 32), 32)
                    o_fin[rows] = heads_first(o_out[:, rows, :])

                loop(0, BLK // 32, lay_o)

    def latent_grad():
        with scope("dc"):
            arrived(dv_recv, msg_rs.at[2])
            arrived(dk_recv, msg_rs.at[3])
            dkv = jnp.concatenate([g for h in range(n_chip) for g in (dk_recv[h, pl.ds(0, BLK), :], dv_recv[h])], axis=1)
            dc_fin[...] = mm(dkv, w_big[...], NT).astype(BF)
            dr = dk_recv[0, pl.ds(BLK, 64), :].astype(F32)
            for h in range(1, n_chip):
                dr = dr + dk_recv[h, pl.ds(BLK, 64), :].astype(F32)
            dr_fin[...] = jnp.transpose(jnp.concatenate([dr[:, :64], dr[:, 64:]], axis=0)).astype(BF)

    gk.steps("k", latent_grad)

    with scope("drain"):
        arrived(dq_out, msg_rs.at[1])
        outs = [pltpu.make_async_copy(buf, dst, out_sem.at[i]) for i, (buf, dst) in enumerate(
            ((dq_out, dq_hbm), (o_fin, o_hbm), (dc_fin, dc_hbm), (dr_fin, dr_hbm)))]
        for c in outs:
            c.start()
        for g in (gc, gv, gk):
            g.finish()
        for c in [pair_dv, pair_dwv, pair_dwk] + pair_dk:
            c.wait_send()
        for k, buf in enumerate((q_recv, do_recv, o_out, dq_out)):
            @pl.when(owner_core == par)
            def _():
                arrived(buf.at[pl.ds(0, n_chip - 1)], msg_ss.at[k])

            @pl.when(owner_core != par)
            def _():
                arrived(buf, msg_ss.at[k])
        for k, buf in enumerate((dv_recv, dk_recv)):
            arrived(buf.at[pl.ds(0, n_chip - 1)], msg_ss.at[4 + k])
        for k in range(2):
            arrived(dw_all.at[k], dw_sem.at[k])
        for c in outs:
            c.wait()


def copy_kernel(*refs):
    n = len(RESULT_PIECES)
    src, dst, buf, (sem_in, sem_out) = refs[:n], refs[n:2 * n], refs[2 * n:3 * n], refs[3 * n:]
    ins, outs = [], []
    for a, b, c, pieces in zip(src, dst, buf, RESULT_PIECES):
        size = a.shape[0] // pieces
        for i in range(pieces):
            rows = pl.ds(i * size, size)
            ins.append(pltpu.make_async_copy(a.at[rows], c.at[rows], sem_in.at[len(ins)]))
            outs.append(pltpu.make_async_copy(c.at[rows], b.at[rows], sem_out.at[len(outs)]))
    for c in ins:
        c.start()
    for c, d in zip(ins, outs):
        c.wait()
        d.start()
    for d in outs:
        d.wait()


RESULT_PIECES = (1, 2, 1, 1, 8, 8)


def copy_results(*arrays):
    hbm = pl.BlockSpec(memory_space=pl.ANY)
    shapes = tuple(jax.ShapeDtypeStruct(a.shape, a.dtype) for a in arrays)
    dma = pltpu.SemaphoreType.DMA((sum(RESULT_PIECES),))
    return pl.pallas_call(
        copy_kernel, out_shape=shapes, in_specs=[hbm] * len(arrays), out_specs=(hbm,) * len(arrays),
        scratch_shapes=[pltpu.VMEM(a.shape, a.dtype) for a in arrays] + [dma, dma],
    )(*arrays)


def solution(mesh):
    n_dev = mesh.shape["cp"]
    n_chip = n_dev // 2
    nz = n_chip // PLANE
    seq = n_dev * BLK
    seq_spec = P("cp")

    def local_step(queries, latent, key_rope, w_uk, w_uv, d_out):
        vm = pl.BlockSpec(memory_space=pltpu.VMEM)
        hbm = pl.BlockSpec(memory_space=pl.ANY)
        dma = pltpu.SemaphoreType.DMA
        gather_sems = [dma((4, nz)), dma((nz,)), dma((2,))]
        o, dq, dc, dr, dwk, dwv = pl.pallas_call(
            functools.partial(kernel, nz, queries.shape[-1]),
            out_shape=(jax.ShapeDtypeStruct((BLK, n_chip, 128), BF),
                       jax.ShapeDtypeStruct((n_chip, 192, BLK), BF),
                       jax.ShapeDtypeStruct((BLK, 512), BF),
                       jax.ShapeDtypeStruct((64, BLK), BF),
                       jax.ShapeDtypeStruct((512, n_chip, 1, 128), F32),
                       jax.ShapeDtypeStruct((512, n_chip, 1, 128), F32)),
            in_specs=[vm] * 4 + [hbm] * 2,
            out_specs=(hbm,) * 6,
            scratch_shapes=[
                pltpu.VMEM((n_chip, BLK, 128), BF),
                pltpu.VMEM((n_chip, 192, BLK), BF),
                pltpu.VMEM((n_chip, BLK, 128), BF),
                pltpu.VMEM((n_chip, 192, 128), BF),
                pltpu.VMEM((BLK, n_chip, 128), BF),
                pltpu.VMEM((BLK, 512), BF),
                pltpu.VMEM((64, BLK), BF),
                pltpu.VMEM((n_chip, BLK, 128), BF),
                pltpu.VMEM((512, n_chip * 256), BF),
                pltpu.VMEM((2, BLK, n_chip, 128), BF),
                pltpu.VMEM((256, 512), BF),
                pltpu.VMEM((n_chip, 192, BLK), BF),
                pltpu.VMEM((n_chip, BLK, 128), BF),
                pltpu.VMEM((2, n_chip, 144, 512), BF),
                pltpu.VMEM((seq, 256), BF),
                pltpu.VMEM((seq, 128), BF),
                pltpu.VMEM((192, seq), BF),
                pltpu.VMEM((128, seq), BF),
                pltpu.VMEM((seq, SUP), F32),
                pltpu.VMEM((CH, SUP), BF),
                pltpu.VMEM((nz * (nz + 1) * CH, SUP), BF),
                pltpu.VMEM((CH, SUP), BF),
                pltpu.VMEM((seq, 256), F32),
                pltpu.VMEM((seq, 128), F32),
                pltpu.VMEM((256, SUP), BF),
                pltpu.VMEM((SUP, 128), BF),
                pltpu.VMEM((128, SUP), F32),
                pltpu.VMEM((128, SUP), F32),
                pltpu.VMEM((192, SUP), F32),
                pltpu.VMEM((8, SUP), F32),
                pltpu.VMEM((n_chip // 2, 1, SUP), F32),
                pltpu.VMEM((n_chip, BLK, 128), BF),
                pltpu.VMEM((n_chip, 192, BLK), BF),
                pltpu.VMEM((2, n_chip, BLK, 128), BF),
                pltpu.VMEM((n_chip, BLK, 128), BF),
                pltpu.VMEM((2, n_chip, 192, 128), BF),
                pltpu.VMEM((n_chip, 192, 128), BF),
                pltpu.VMEM((2, 128, 512), F32),
                pltpu.VMEM((2, 2, SUP, 128), F32),
                pltpu.VMEM((2, SUP, 128), F32),
                pltpu.VMEM((2, 2, n_chip, SUP, 128), F32),
            ] + [dma((6,)), dma((4,)), dma((n_chip // 2,)), dma((n_chip // 2,))] + [dma((3 + nz,)), dma((3 + nz,)), dma((2,)), dma((4,)), dma((2,))] + gather_sems * 3,
            compiler_params=pltpu.CompilerParams(
                collective_id=0, has_side_effects=True, vmem_limit_bytes=62 * 1024 * 1024),
        )(queries.transpose(1, 2, 0), d_out, latent, key_rope.T, w_uk, w_uv)
        o, dq, dc, dr, dwk, dwv = copy_results(
            o, dq, dc, dr, dwk.reshape(512, n_chip, 128), dwv.reshape(512, n_chip, 128))
        return o, dq.transpose(2, 0, 1), dc, dr.T, dwk, dwv

    return jax.shard_map(local_step, mesh=mesh,
                         in_specs=(seq_spec, seq_spec, seq_spec, P(), P(), seq_spec),
                         out_specs=(seq_spec, seq_spec, seq_spec, seq_spec, P(), P()),
                         check_vma=False)
```

```python
import functools
import math

import jax
import jax.numpy as jnp
from jax import lax
from jax.experimental import pallas as pl
from jax.experimental.pallas import tpu as pltpu
from jax.sharding import PartitionSpec as P

MESH = pl.DeviceIdType.MESH
NX, NY = 2, 2
PLANE = NX * NY
BLK = 128
SUP = 256
CH = SUP * PLANE
NEG = -1e30
NT = (((1,), (1,)), ((), ()))
NN = (((1,), (0,)), ((), ()))
BF, F32 = jnp.bfloat16, jnp.float32


def mm(a, b, dims=NN):
    return lax.dot_general(a, b, dims, preferred_element_type=F32)


def pack_rope(x):
    return jnp.concatenate([x[:64], x[64:]], axis=1)


def kernel(nz, qk_dim, q_ref, do_raw, c_ref, rt_ref, wk_hbm, wv_hbm,
           o_hbm, dq_hbm, dc_hbm, dr_hbm, dwk_out, dwv_out,
           o_out, dq_out, dv_recv, dk_recv, o_fin, dc_fin, dr_fin, do_ref,
           w_big, w_stage, wt_cat, q_recv, do_recv, c_all, kr, v, kt, vt, s_buf, p_buf, p_store, ds_buf, dkr, dv,
           qt, dof, dot_, ot, dqt, lse, delta_s, o_send, dq_send, dv_msg, dv_part, dk_msg, dk_part,
           dwt, dw_msg, dw_part, dw_all,
           msg_ss, msg_rs, q_rs, do_rs, pair_s, pair_r, dw_sem, out_sem, w_sem,
           cg_rz, cg_rp, cg_ss, v_rz, v_rp, v_ss, k_rz, k_rp, k_ss):
    n_chip = PLANE * nz
    n_dev = 2 * n_chip
    n_sup = n_chip // 2
    me = lax.axis_index("cp")
    chip, par = me // 2, me % 2
    partner = 2 * chip + (1 - par)
    x, y, z = chip % NX, (chip // NX) % NY, chip // PLANE
    scale = 1.0 / math.sqrt(qk_dim)
    c1 = scale * math.log2(math.e)
    scope = jax.named_scope

    def chip_at(zq, yq, xq):
        return (zq * NY + yq) * NX + xq

    def col_chip(col, zq):
        return chip_at(zq, 1 - y if col >= 2 else y, 1 - x if col % 2 else x)

    def remote(src, dst, ssem, rsem, dev):
        return pltpu.make_async_remote_copy(src_ref=src, dst_ref=dst, send_sem=ssem, recv_sem=rsem,
                                            device_id=(dev,), device_id_type=MESH)

    def start(src, dst, ssem, rsem, dev):
        @pl.when(dev == me)
        def _():
            pltpu.make_async_copy(src, dst, rsem).start()

        @pl.when(dev != me)
        def _():
            remote(src, dst, ssem, rsem, dev).start()

    def arrived(dst, rsem):
        pltpu.make_async_copy(dst, dst, rsem).wait()

    def loop(lo, hi, f):
        def body(i, carry):
            f(i)
            return carry

        lax.fori_loop(lo, hi, body, 0)

    n_piece = 8

    def w_copy(i):
        src = wk_hbm if i < n_piece // 2 else wv_hbm
        return pltpu.make_async_copy(src.at[pl.ds(i % (n_piece // 2) * BLK, BLK)], w_stage.at[i % 2], w_sem.at[i % 2])

    for i in range(2):
        w_copy(i).start()

    def heads_first(x):
        return jnp.transpose(x, (1, 0, 2))

    with scope("barrier"):
        barrier = pltpu.get_barrier_semaphore()
        loop(1, n_dev, lambda i: pl.semaphore_signal(
            barrier, inc=1, device_id=(lax.rem(me + i, n_dev),), device_id_type=MESH))
        pl.semaphore_wait(barrier, n_dev - 1)

    class Gather:
        def __init__(self, buf, rows, split, rz, rp, ss, ready):
            self.buf, self.rows, self.split = buf, rows, split
            self.rz, self.rp, self.ss, self.ready = rz, rp, ss, ready
            self.dev_x = 2 * chip_at(z, y, 1 - x) + par
            self.dev_y = 2 * chip_at(z, 1 - y, x) + par

        def blk(self, col, zq):
            return self.buf.at[par, col_chip(col, zq)]

        def along_z(self, zq, to):
            b = self.blk(0, zq)
            return remote(b, b, self.ss.at[0], self.rz.at[0, zq], 2 * chip_at(to, y, x) + par)

        def to_x(self, col, zq):
            b = self.blk(col, zq)
            return remote(b, b, self.ss.at[0], self.rz.at[1, zq], self.dev_x)

        def to_y(self, col, zq):
            b = self.blk(col, zq)
            return remote(b, b, self.ss.at[0], self.rz.at[2, zq], self.dev_y)

        def part_y(self, col, zq):
            b = self.blk(col, zq).at[pl.ds(0, self.split)]
            return remote(b, b, self.ss.at[0], self.rz.at[3, zq], self.dev_y)

        def part_x(self, col, zq):
            b = self.blk(col, zq).at[pl.ds(self.split, self.rows - self.split)]
            return remote(b, b, self.ss.at[0], self.rz.at[3, zq], self.dev_x)

        def pair(self, col, zq):
            b = self.blk(col, zq)
            return remote(b, b, self.ss.at[1], self.rp.at[zq], partner)

        def own_col(self, zq):
            self.to_x(0, zq).start()
            self.to_y(0, zq).start()
            self.pair(0, zq).start()

        def xy(self, zq):
            self.to_x(1, zq).wait_recv()
            self.part_y(1, zq).start()
            self.pair(1, zq).start()
            self.to_y(2, zq).wait_recv()
            self.part_x(2, zq).start()
            self.pair(2, zq).start()

        def diag(self, zq):
            arrived(self.blk(3, zq), self.rz.at[3, zq])
            self.pair(3, zq).start()

        def pairs(self, zq):
            arrived(self.buf.at[1 - par, pl.ds(zq * PLANE, PLANE)], self.rp.at[zq])

        def begin(self):
            for d in range(1, nz):
                @pl.when(z + d < nz)
                def _():
                    self.along_z(z, z + d).start()

                @pl.when(z - d >= 0)
                def _():
                    self.along_z(z, z - d).start()

            self.own_col(z)

        def from_z(self, zq):
            self.along_z(zq, z).wait_recv()
            self.own_col(zq)

        def at(self, d, f):
            if d == 0:
                f(z)
                return

            @pl.when(z - d >= 0)
            def _():
                f(z - d)

            @pl.when(z + d < nz)
            def _():
                f(z + d)

        def last(self, zq):
            self.diag(zq)
            self.pairs(zq)
            self.ready(zq)

        def steps(self, tag, before_last):
            for d in range(1, nz):
                with scope(f"{tag}z{d}"):
                    self.at(d, self.from_z)
                with scope(f"{tag}xy{d - 1}"):
                    self.at(d - 1, self.xy)
                if d >= 2:
                    with scope(f"{tag}d{d - 2}"):
                        self.at(d - 2, self.last)
            with scope(f"{tag}xy{nz - 1}"):
                self.at(nz - 1, self.xy)
            for d in range(max(nz - 2, 0), nz):
                if d == nz - 1:
                    before_last()
                with scope(f"{tag}d{d}"):
                    self.at(d, self.last)

        def finish(self):
            arrived(self.buf.at[0, pl.ds(0, n_chip - 1)], self.ss.at[0])
            arrived(self.buf.at[0], self.ss.at[1])

    owner_core = lax.rem((chip + 1) // 2, 2)
    q_slot = 2 * (chip // 2) + par

    def sup_chip(s):
        return 2 * s + lax.rem(s + par, 2)

    def q_copy(i):
        head = lax.rem(chip + i, n_chip)
        return q_ref.at[head], q_recv.at[q_slot], msg_ss.at[0], q_rs.at[q_slot // 2], 2 * head + owner_core

    def do_copy(i):
        head = lax.rem(chip + i, n_chip)
        return do_ref.at[head], do_recv.at[q_slot], msg_ss.at[1], do_rs.at[q_slot // 2], 2 * head + owner_core

    def o_copy(s, i):
        return o_send.at[2 * s + i], o_out.at[chip], msg_ss.at[2], msg_rs.at[0], 2 * sup_chip(s) + i

    def dq_copy(s, i):
        return dq_send.at[2 * s + i], dq_out.at[chip], msg_ss.at[3], msg_rs.at[1], 2 * sup_chip(s) + i

    def dv_copy(ch):
        return dv_msg.at[par, ch], dv_recv.at[chip], msg_ss.at[4], msg_rs.at[2], 2 * ch + par

    def dk_copy(ch):
        return dk_msg.at[par, ch], dk_recv.at[chip], msg_ss.at[5], msg_rs.at[3], 2 * ch + par

    gc = Gather(c_all, 144, 80, cg_rz, cg_rp, cg_ss, None)
    with scope("send_c"):
        c_all[par, chip, pl.ds(0, BLK), :] = c_ref[...]
        for i in range(4):
            c_all[par, chip, pl.ds(BLK, 16), pl.ds(128 * i, 128)] = rt_ref[pl.ds(16 * i, 16), :]
        gc.begin()
    with scope("send_q"):
        def send_q(i):
            start(*q_copy(i))
            start(*do_copy(i))

        late = z >= nz // 2

        def lay_do(i):
            rows = pl.ds(pl.multiple_of(i * 32, 32), 32)
            do_ref[:, rows, :] = heads_first(do_raw[rows])

        loop(0, BLK // 32, lay_do)

        @pl.when(jnp.logical_not(late))
        def _():
            loop(0, n_chip, send_q)

    with scope("init"):
        dkr[...] = jnp.zeros_like(dkr)
        dv[...] = jnp.zeros_like(dv)
        for i in range(n_piece):
            w_copy(i).wait()

            def lay_w(r):
                w = heads_first(w_stage[i % 2, pl.ds(pl.multiple_of(r * 32, 32), 32)])
                rows = pl.ds(pl.multiple_of(i % (n_piece // 2) * BLK + r * 32, 32), 32)
                for h in range(n_chip):
                    w_big[rows, pl.ds(h * 256 + 128 * (i // (n_piece // 2)), 128)] = w[h]

            loop(0, BLK // 32, lay_w)
            if i + 2 < n_piece:
                w_copy(i + 2).start()
        wt_cat[...] = jnp.transpose(w_big[:, pl.ds(pl.multiple_of(chip * 256, 256), 256)].astype(F32)).astype(BF)
        qt[pl.ds(192, 64), :] = jnp.zeros((64, SUP), BF)

    def latent_of(ch):
        return jnp.concatenate([c_all[0, ch, pl.ds(0, BLK), :], c_all[1, ch, pl.ds(0, BLK), :]], axis=0)

    def up_project(ch):
        base = pl.multiple_of(ch * SUP, SUP)
        lat = latent_of(ch)
        kv = mm(lat, w_big[:, pl.ds(pl.multiple_of(chip * 256, 256), 256)]).astype(BF)
        kvt = mm(wt_cat[...], lat, NT).astype(BF)
        kr[pl.ds(base, SUP), pl.ds(0, 128)] = kv[:, :128]
        v[pl.ds(base, SUP), :] = kv[:, 128:]
        kt[pl.ds(0, 128), pl.ds(base, SUP)] = kvt[:128]
        vt[:, pl.ds(base, SUP)] = kvt[128:]
        for q in range(2):
            rt = jnp.concatenate([c_all[q, ch, pl.ds(BLK, 16), pl.ds(128 * i, 128)] for i in range(4)], axis=0)
            kt[pl.ds(128, 64), pl.ds(base + q * BLK, BLK)] = rt
            r = jnp.transpose(rt.astype(F32))
            kr[pl.ds(base + q * BLK, BLK), pl.ds(128, 128)] = jnp.concatenate(
                [r, jnp.zeros_like(r)], axis=1).astype(BF)

    diff = lax.broadcasted_iota(jnp.int32, (SUP, SUP), 0) - lax.broadcasted_iota(jnp.int32, (SUP, SUP), 1)

    def load_q(s):
        for i in range(2):
            qt[pl.ds(0, 192), pl.ds(i * BLK, BLK)] = q_recv[2 * s + i]
            dof[pl.ds(i * BLK, BLK), :] = do_recv[2 * s + i]

    def store_row(s):
        a = s // 2
        return (a + 1) * (a + s % 2) * CH

    def forward(s):
        ch = sup_chip(s)
        arrived(q_recv.at[pl.ds(2 * s, 2)], q_rs.at[s])
        arrived(do_recv.at[pl.ds(2 * s, 2)], do_rs.at[s])
        load_q(s)
        dot_[...] = jnp.transpose(dof[...].astype(F32))
        n_ch = s // 2 + 1

        def score(j, m8):
            for t in range(CH // SUP):
                r0 = pl.multiple_of(j * CH + t * SUP, SUP)
                st = mm(kr[pl.ds(r0, SUP), :], qt[...])
                st = jnp.where(diff <= ch * SUP - r0, st, NEG)
                s_buf[pl.ds(r0, SUP), :] = st
                m8 = jnp.maximum(m8, jnp.max(st.reshape(SUP // 8, 8, SUP), axis=0))
            return m8

        m8 = lax.fori_loop(0, n_ch, score, jnp.full((8, SUP), NEG, F32))
        m2 = jnp.max(m8, axis=0, keepdims=True) * c1
        ot[...] = jnp.zeros_like(ot)

        def values(j, l8):
            base = pl.multiple_of(j * CH, CH)
            for t in range(CH // SUP):
                p = jnp.exp2(s_buf[pl.ds(base + t * SUP, SUP), :] * c1 - m2)
                l8 = l8 + jnp.sum(p.reshape(SUP // 8, 8, SUP), axis=0)
                p_buf[pl.ds(t * SUP, SUP), :] = p.astype(BF)
            ot[...] += mm(vt[:, pl.ds(base, CH)], p_buf[...])
            return l8

        l8 = lax.fori_loop(0, n_ch, values, jnp.zeros((8, SUP), F32))
        l = jnp.sum(l8, axis=0, keepdims=True)
        o = ot[...] / l
        lse2 = m2 + jnp.log2(l)
        delta_s[s] = jnp.sum(o * dot_[...], axis=0, keepdims=True)
        o_rows = jnp.transpose(o)
        for i in range(2):
            o_send[2 * s + i] = o_rows[i * BLK:(i + 1) * BLK].astype(BF)
        for i in range(2):
            start(*o_copy(s, i))
        row0 = store_row(s)

        def values_grad(j):
            base = pl.multiple_of(j * CH, CH)
            for t in range(CH // SUP):
                rows = pl.ds(base + t * SUP, SUP)
                p = jnp.exp2(s_buf[rows, :] * c1 - lse2).astype(BF)
                p_store[pl.ds(pl.multiple_of(row0 + base + t * SUP, SUP), SUP), :] = p
                dv[rows, :] += mm(p, dof[...])

        loop(0, n_ch, values_grad)

    def send_dq(s):
        for i in range(2):
            start(*dq_copy(s, i))

    def backward(s):
        load_q(s)
        dqt[...] = jnp.zeros_like(dqt)
        row0 = store_row(s)
        delta = delta_s[s]

        def keys_grad(j):
            base = pl.multiple_of(j * CH, CH)
            for t in range(CH // SUP):
                rows = pl.ds(base + t * SUP, SUP)
                dp = mm(v[rows, :], dof[...], NT)
                p = p_store[pl.ds(pl.multiple_of(row0 + base + t * SUP, SUP), SUP), :].astype(F32)
                ds_buf[pl.ds(t * SUP, SUP), :] = (p * (dp - delta) * scale).astype(BF)
            for t in range(CH // SUP):
                rows = pl.ds(base + t * SUP, SUP)
                dkr[rows, :] += mm(ds_buf[pl.ds(t * SUP, SUP), :], qt[...], NT)
            dqt[...] += mm(kt[:, pl.ds(base, CH)], ds_buf[...])

        loop(0, s // 2 + 1, keys_grad)
        for i in range(2):
            dq_send[2 * s + i] = dqt[:, pl.ds(i * BLK, BLK)].astype(BF)
        if s >= n_sup // 2:
            send_dq(s)

    def ready_c(zq):
        gc.pairs(zq)
        loop(zq * PLANE, (zq + 1) * PLANE, up_project)

    def col_ready(zq):
        @pl.when(z != zq)
        def _():
            gc.from_z(zq)

    def step_c(k):
        if k < nz:
            col_ready(k)
        if 0 <= k - 1 < nz:
            gc.xy(k - 1)
        if 0 <= k - 2 < nz:
            gc.diag(k - 2)
            ready_c(k - 2)

    for k in range(nz + 2):
        with scope(f"c{k}"):
            step_c(k)
            if k < 2:
                @pl.when(late)
                def _():
                    loop(k * n_chip // 2, (k + 1) * n_chip // 2, send_q)

        if k >= 2:
            with scope(f"fwd{k - 2}"):
                loop(2 * (k - 2), 2 * (k - 2) + 2, forward)

    def head_dw(k, lo, hi, grads):
        def add(ch):
            base = pl.multiple_of(ch * SUP, SUP)
            g = jnp.transpose(grads(pl.ds(base, SUP))).astype(BF)
            dwt[k] += mm(g, latent_of(ch))

        loop(lo, hi, add)

    def dw_exchange(k):
        dw_msg[k] = jnp.transpose(dwt[k]).reshape(2, SUP, 128)
        c = remote(dw_msg.at[k, 1 - par], dw_part.at[k], pair_s.at[k], pair_r.at[k], partner)
        c.start()
        return c

    def dw_begin(k, c):
        c.wait_recv()
        dw_all[k, par, chip] = dw_msg[k, par] + dw_part[k]

    def dw_out_copy(k, q, h):
        dst = dwk_out if k == 0 else dwv_out
        return pltpu.make_async_copy(dw_all.at[k, q, h], dst.at[pl.ds(q * SUP, SUP), h, 0], dw_sem.at[k])

    def put_dw(k):
        def put(zq):
            for q in range(2):
                loop(zq * PLANE, (zq + 1) * PLANE, lambda h: dw_out_copy(k, q, h).start())

        return put

    dwt[...] = jnp.zeros_like(dwt)
    gv = Gather(dw_all.at[1], SUP, 128, v_rz, v_rp, v_ss, put_dw(1))
    gk = Gather(dw_all.at[0], SUP, 128, k_rz, k_rp, k_ss, put_dw(0))
    with scope("dv"):
        def dv_out(ch):
            for q in range(2):
                dv_msg[q, ch] = dv[pl.ds(pl.multiple_of(ch * SUP, SUP) + q * BLK, BLK), :].astype(BF)

        loop(0, n_chip, dv_out)
        pair_dv = remote(dv_msg.at[1 - par], dv_part, pair_s.at[2], pair_r.at[2], partner)
        pair_dv.start()
        head_dw(1, 0, n_chip, lambda rows: dv[rows, :])
        pair_dwv = dw_exchange(1)
        pair_dv.wait_recv()

        def dv_add(ch):
            dv_msg[par, ch] = (dv_msg[par, ch].astype(F32) + dv_part[ch].astype(F32)).astype(BF)

        loop(0, n_chip, dv_add)
        dw_begin(1, pair_dwv)
        gv.begin()

        def dv_send(i):
            start(*dv_copy(lax.rem(chip + i, n_chip)))

        loop(0, n_chip, dv_send)

    pair_dk = [remote(dk_msg.at[1 - par, pl.ds(PLANE * g, PLANE)], dk_part.at[pl.ds(PLANE * g, PLANE)],
                      pair_s.at[3 + g], pair_r.at[3 + g], partner) for g in range(nz)]

    def dk_out(g):
        def put(ch):
            for q in range(2):
                rows = pl.ds(pl.multiple_of(ch * SUP, SUP) + q * BLK, BLK)
                dk_msg[q, ch, pl.ds(0, BLK), :] = dkr[rows, pl.ds(0, 128)].astype(BF)
                dk_msg[q, ch, pl.ds(BLK, 64), :] = pack_rope(dkr[rows, pl.ds(128, 128)][:, :64]).astype(BF)

        loop(PLANE * g, PLANE * (g + 1), put)
        pair_dk[g].start()
        head_dw(0, PLANE * g, PLANE * (g + 1), lambda rows: dkr[rows, pl.ds(0, 128)])

    def dk_add(g):
        pair_dk[g].wait_recv()

        def put(ch):
            dk_msg[par, ch] = (dk_msg[par, ch].astype(F32) + dk_part[ch].astype(F32)).astype(BF)

        loop(PLANE * g, PLANE * (g + 1), put)

    for g in reversed(range(nz)):
        for s in (2 * g + 1, 2 * g):
            with scope(f"bwd{s}"):
                backward(s)
        if g + 1 < nz:
            with scope(f"dks{g + 1}"):
                dk_add(g + 1)
        with scope(f"dko{g}"):
            dk_out(g)
        if g == 1:
            with scope("vz1"):
                gv.at(1, gv.from_z)

    with scope("dwk"):
        pair_dwk = dw_exchange(0)
        dw_begin(0, pair_dwk)
        gk.begin()
    with scope("dks0"):
        dk_add(0)
    with scope("vz"):
        for d in range(2, nz):
            gv.at(d, gv.from_z)
    with scope("vxy0"):
        gv.at(0, gv.xy)
    for d in range(nz):
        if d + 1 < nz:
            with scope(f"vxy{d + 1}"):
                gv.at(d + 1, gv.xy)
        with scope(f"vd{d}"):
            gv.at(d, gv.last)
            loop(d * n_chip // nz, (d + 1) * n_chip // nz, lambda i: start(*dk_copy(lax.rem(chip + i, n_chip))))
        if d == 0:
            for s in reversed(range(n_sup // 2)):
                send_dq(s)
            with scope("ofin"):
                arrived(o_out, msg_rs.at[0])

                def lay_o(i):
                    rows = pl.ds(pl.multiple_of(i * 32, 32), 32)
                    o_fin[rows] = heads_first(o_out[:, rows, :])

                loop(0, BLK // 32, lay_o)

    def latent_grad():
        with scope("dc"):
            arrived(dv_recv, msg_rs.at[2])
            arrived(dk_recv, msg_rs.at[3])
            dkv = jnp.concatenate([g for h in range(n_chip) for g in (dk_recv[h, pl.ds(0, BLK), :], dv_recv[h])], axis=1)
            dc_fin[...] = mm(dkv, w_big[...], NT).astype(BF)
            dr = dk_recv[0, pl.ds(BLK, 64), :].astype(F32)
            for h in range(1, n_chip):
                dr = dr + dk_recv[h, pl.ds(BLK, 64), :].astype(F32)
            dr_fin[...] = jnp.transpose(jnp.concatenate([dr[:, :64], dr[:, 64:]], axis=0)).astype(BF)

    gk.steps("k", latent_grad)

    with scope("drain"):
        arrived(dq_out, msg_rs.at[1])
        outs = [pltpu.make_async_copy(buf, dst, out_sem.at[i]) for i, (buf, dst) in enumerate(
            ((dq_out, dq_hbm), (o_fin, o_hbm), (dc_fin, dc_hbm), (dr_fin, dr_hbm)))]
        for c in outs:
            c.start()
        for g in (gc, gv, gk):
            g.finish()
        for c in [pair_dv, pair_dwv, pair_dwk] + pair_dk:
            c.wait_send()
        for k, buf in enumerate((q_recv, do_recv, o_out, dq_out)):
            @pl.when(owner_core == par)
            def _():
                arrived(buf.at[pl.ds(0, n_chip - 1)], msg_ss.at[k])

            @pl.when(owner_core != par)
            def _():
                arrived(buf, msg_ss.at[k])
        for k, buf in enumerate((dv_recv, dk_recv)):
            arrived(buf.at[pl.ds(0, n_chip - 1)], msg_ss.at[4 + k])
        for k in range(2):
            arrived(dw_all.at[k], dw_sem.at[k])
        for c in outs:
            c.wait()


def copy_kernel(*refs):
    n = len(RESULT_PIECES)
    src, dst, buf, (sem_in, sem_out) = refs[:n], refs[n:2 * n], refs[2 * n:3 * n], refs[3 * n:]
    ins, outs = [], []
    for a, b, c, pieces in zip(src, dst, buf, RESULT_PIECES):
        size = a.shape[0] // pieces
        for i in range(pieces):
            rows = pl.ds(i * size, size)
            ins.append(pltpu.make_async_copy(a.at[rows], c.at[rows], sem_in.at[len(ins)]))
            outs.append(pltpu.make_async_copy(c.at[rows], b.at[rows], sem_out.at[len(outs)]))
    for c in ins:
        c.start()
    for c, d in zip(ins, outs):
        c.wait()
        d.start()
    for d in outs:
        d.wait()


RESULT_PIECES = (1, 1, 1, 1, 4, 4)


def copy_results(*arrays):
    hbm = pl.BlockSpec(memory_space=pl.ANY)
    shapes = tuple(jax.ShapeDtypeStruct(a.shape, a.dtype) for a in arrays)
    dma = pltpu.SemaphoreType.DMA((sum(RESULT_PIECES),))
    return pl.pallas_call(
        copy_kernel, out_shape=shapes, in_specs=[hbm] * len(arrays), out_specs=(hbm,) * len(arrays),
        scratch_shapes=[pltpu.VMEM(a.shape, a.dtype) for a in arrays] + [dma, dma],
    )(*arrays)


def solution(mesh):
    n_dev = mesh.shape["cp"]
    n_chip = n_dev // 2
    nz = n_chip // PLANE
    seq = n_dev * BLK
    seq_spec = P("cp")

    def local_step(queries, latent, key_rope, w_uk, w_uv, d_out):
        vm = pl.BlockSpec(memory_space=pltpu.VMEM)
        hbm = pl.BlockSpec(memory_space=pl.ANY)
        dma = pltpu.SemaphoreType.DMA
        gather_sems = [dma((4, nz)), dma((nz,)), dma((2,))]
        o, dq, dc, dr, dwk, dwv = pl.pallas_call(
            functools.partial(kernel, nz, queries.shape[-1]),
            out_shape=(jax.ShapeDtypeStruct((BLK, n_chip, 128), BF),
                       jax.ShapeDtypeStruct((n_chip, 192, BLK), BF),
                       jax.ShapeDtypeStruct((BLK, 512), BF),
                       jax.ShapeDtypeStruct((64, BLK), BF),
                       jax.ShapeDtypeStruct((512, n_chip, 1, 128), F32),
                       jax.ShapeDtypeStruct((512, n_chip, 1, 128), F32)),
            in_specs=[vm] * 4 + [hbm] * 2,
            out_specs=(hbm,) * 6,
            scratch_shapes=[
                pltpu.VMEM((n_chip, BLK, 128), BF),
                pltpu.VMEM((n_chip, 192, BLK), BF),
                pltpu.VMEM((n_chip, BLK, 128), BF),
                pltpu.VMEM((n_chip, 192, 128), BF),
                pltpu.VMEM((BLK, n_chip, 128), BF),
                pltpu.VMEM((BLK, 512), BF),
                pltpu.VMEM((64, BLK), BF),
                pltpu.VMEM((n_chip, BLK, 128), BF),
                pltpu.VMEM((512, n_chip * 256), BF),
                pltpu.VMEM((2, BLK, n_chip, 128), BF),
                pltpu.VMEM((256, 512), BF),
                pltpu.VMEM((n_chip, 192, BLK), BF),
                pltpu.VMEM((n_chip, BLK, 128), BF),
                pltpu.VMEM((2, n_chip, 144, 512), BF),
                pltpu.VMEM((seq, 256), BF),
                pltpu.VMEM((seq, 128), BF),
                pltpu.VMEM((192, seq), BF),
                pltpu.VMEM((128, seq), BF),
                pltpu.VMEM((seq, SUP), F32),
                pltpu.VMEM((CH, SUP), BF),
                pltpu.VMEM((nz * (nz + 1) * CH, SUP), BF),
                pltpu.VMEM((CH, SUP), BF),
                pltpu.VMEM((seq, 256), F32),
                pltpu.VMEM((seq, 128), F32),
                pltpu.VMEM((256, SUP), BF),
                pltpu.VMEM((SUP, 128), BF),
                pltpu.VMEM((128, SUP), F32),
                pltpu.VMEM((128, SUP), F32),
                pltpu.VMEM((192, SUP), F32),
                pltpu.VMEM((8, SUP), F32),
                pltpu.VMEM((n_chip // 2, 1, SUP), F32),
                pltpu.VMEM((n_chip, BLK, 128), BF),
                pltpu.VMEM((n_chip, 192, BLK), BF),
                pltpu.VMEM((2, n_chip, BLK, 128), BF),
                pltpu.VMEM((n_chip, BLK, 128), BF),
                pltpu.VMEM((2, n_chip, 192, 128), BF),
                pltpu.VMEM((n_chip, 192, 128), BF),
                pltpu.VMEM((2, 128, 512), F32),
                pltpu.VMEM((2, 2, SUP, 128), F32),
                pltpu.VMEM((2, SUP, 128), F32),
                pltpu.VMEM((2, 2, n_chip, SUP, 128), F32),
            ] + [dma((6,)), dma((4,)), dma((n_chip // 2,)), dma((n_chip // 2,))] + [dma((3 + nz,)), dma((3 + nz,)), dma((2,)), dma((4,)), dma((2,))] + gather_sems * 3,
            compiler_params=pltpu.CompilerParams(
                collective_id=0, has_side_effects=True, vmem_limit_bytes=62 * 1024 * 1024),
        )(queries.transpose(1, 2, 0), d_out, latent, key_rope.T, w_uk, w_uv)
        o, dq, dc, dr, dwk, dwv = copy_results(
            o, dq, dc, dr, dwk.reshape(512, n_chip, 128), dwv.reshape(512, n_chip, 128))
        return o, dq.transpose(2, 0, 1), dc, dr.T, dwk, dwv

    return jax.shard_map(local_step, mesh=mesh,
                         in_specs=(seq_spec, seq_spec, seq_spec, P(), P(), seq_spec),
                         out_specs=(seq_spec, seq_spec, seq_spec, seq_spec, P(), P()),
                         check_vma=False)
```
